256 devices in a mesh: gx: 4 (over z_hi), gy: 8 (over x, core), gz: 8 (over z_lo, y).
Axes of the slice: x: 4, y: 4, z: 8 (z_hi: 4, z_lo: 2; z = z_hi * 2 + z_lo), core: 2. Of those that a mesh axis runs over, the one named last changes fastest.
Arguments:
- state: float32 [7, 64, 128, 1024], P(None, 'gx', 'gy', 'gz'), may hold values from -1 to 4, as said below
- solver_owner: int32 [8, 8, 8], P('gy', 'gz'), may hold values from 0 to 15, as said below
- phi_prev: float32 [16, 8, 128, 1024], P('gx', None, 'gy', 'gz'), may hold values from -1.2 to 1.2
Outputs:
- new_state: float32 [7, 64, 128, 1024], P(None, 'gx', 'gy', 'gz')
- density_solver: float32 [16, 8, 128, 1024], P('gx', None, 'gy', 'gz')
- residual: float32 [64, 128, 1024], P('gx', 'gy', 'gz')
The draws below stay inside these ranges and needn't reach their ends.
Inputs may be any that keep to these rules, and one draw needn't show every extreme that they name: `state`: field 0 lies in [1, 2], fields 1 to 3 in [-1, 1], field 4 in [2, 4], field 5 in [1, 2], field 6 in [0, 1]. `solver_owner`: entry b of line (j, k) is owner * 4 + slot, the owner being the gx index holding box b in the solver ownership. Codes within a line are distinct, so an owner holds at most 4 boxes of a line, and in every line some owner holds exactly 4.
All inputs are finite; a program needn't handle non-finite values.
Results may differ from the reference program's by a relative error of at most 0.00012.
Values sent between devices are 32-bit elements; how exact they have to be, the bound alone decides.
A program may use at most 64 MiB of HBM per device.

```python
import jax
import jax.numpy as jnp
from jax import lax

CY = 16
CZ = 128
SLOTS = 4
BX = 8
LINES_Y = 8
LINES_Z = 8
BOXES = 8
CODES = 16
NX = 64
NY = 128
NZ = 1024


def draw_state(key, part):
    keys = jax.random.split(key, 6)
    shape = (NX, NY, NZ)
    density = jnp.exp(jax.random.uniform(keys[0], shape, jnp.float32) * jnp.log(2.0))
    momenta = jnp.clip(0.4 * jax.random.normal(keys[2], (3,) + shape, jnp.float32), -1.0, 1.0)
    energy = jax.random.uniform(keys[3], shape, jnp.float32, 2.0, 4.0)
    internal = jax.random.uniform(keys[4], shape, jnp.float32, 1.0, 2.0)
    tracer = jax.random.uniform(keys[5], shape, jnp.float32)
    stacked = jnp.concatenate([density[None], momenta, energy[None], internal[None], tracer[None]], 0)
    return stacked.astype(jnp.float32)


def owner_line(key):
    keys = jax.random.split(key, 3)
    fullest = jax.random.randint(keys[0], (), 0, CODES // SLOTS)
    index = jnp.arange(CODES, dtype=jnp.int32)
    scores = jax.random.randint(keys[1], (CODES,), 0, 1 << 20) * CODES + index
    scores = jnp.where(index // SLOTS == fullest, index - CODES, scores)
    order = jnp.argsort(scores, stable=True).astype(jnp.int32)
    chosen = order[:BOXES]
    placing = jax.random.permutation(keys[2], BOXES)
    return jnp.zeros((BOXES,), jnp.int32).at[placing].set(chosen)


def draw_solver_owner(key, part):
    keys = jax.random.split(key, LINES_Y * LINES_Z)
    lines = jax.vmap(owner_line)(keys)
    return lines.reshape(LINES_Y, LINES_Z, BOXES).astype(jnp.int32)


def levels(rng, extent, pieces, low, largest):
    def one(axis_at, shards_of):
        draws = jax.random.uniform(jax.random.fold_in(jax.random.fold_in(rng, 6), axis_at), (shards_of,), jnp.float32, low / len(pieces), largest / len(pieces))
        return jnp.repeat(jnp.exp(draws), extent[axis_at] // shards_of).reshape((-1,) + (1,) * (len(extent) - axis_at - 1))

    loudness = one(*pieces[0])
    for cut in pieces[1:]:
        loudness = loudness * one(*cut)
    return loudness


def scatter_about(own_key, shape, scale, reach, cuts=(), kind=jnp.bfloat16):
    loudness = levels(own_key, shape, cuts, -0.22, 0.18) if cuts else 1.0
    entries = jax.random.normal(own_key, shape, jnp.float32) * scale * loudness
    return jnp.minimum(jnp.maximum(entries, -reach), reach).astype(kind)


def setup_inputs(seed: int = 0) -> dict:
    key_list = jax.random.split(jax.random.key(seed), 4)
    state = draw_state(jax.random.fold_in(key_list[3], 71), 0)
    solver_owner = draw_solver_owner(jax.random.fold_in(key_list[3], 71), 0)
    phi_prev = scatter_about(key_list[2], (CODES, BX, NY, NZ), 0.2, 1.2, ((0, 4), (2, 8), (3, 8)), jnp.float32)
    return {"state": state, "solver_owner": solver_owner, "phi_prev": phi_prev}


GAMMA = 5.0 / 3.0
DTH = 0.04
FOURPIG = 2.0

def wave_speed(q, d):
    dens = jnp.maximum(q[0], 0.25)
    vel = q[d] / dens
    press = (GAMMA - 1.0) * jnp.maximum(q[5], 0.1)
    return jnp.abs(vel) + jnp.sqrt(GAMMA * press / dens)

def physical_flux(v, d):
    dens = jnp.maximum(v[0], 0.25)
    vel = v[d] / dens
    press = (GAMMA - 1.0) * jnp.maximum(v[5], 0.1)
    comps = [v[d]]
    for k in (1, 2, 3):
        term = v[k] * vel
        if k == d:
            term = term + press
        comps.append(term)
    comps.append((v[4] + press) * vel)
    comps.append(v[5] * vel)
    comps.append(v[6] * vel)
    return jnp.stack(comps, 0)

def tendency(padded):
    total = None
    for d in (1, 2, 3):
        line = padded
        for e in (1, 2, 3):
            if e != d:
                line = lax.slice_in_dim(line, 2, line.shape[e] - 2, axis=e)
        count = line.shape[d] - 3
        left_far = lax.slice_in_dim(line, 0, count, axis=d)
        left = lax.slice_in_dim(line, 1, count + 1, axis=d)
        right = lax.slice_in_dim(line, 2, count + 2, axis=d)
        right_far = lax.slice_in_dim(line, 3, count + 3, axis=d)
        edge = 7.0 / 12.0 * (left + right) - 1.0 / 12.0 * (left_far + right_far)
        edge = jnp.clip(edge, jnp.minimum(left, right), jnp.maximum(left, right))
        speed = wave_speed(line, d)
        fastest = jnp.maximum(lax.slice_in_dim(speed, 1, count + 1, axis=d - 1), lax.slice_in_dim(speed, 2, count + 2, axis=d - 1))
        flux = physical_flux(edge, d) - 0.5 * fastest[None] * (right - left)
        change = lax.slice_in_dim(flux, 1, count, axis=d) - lax.slice_in_dim(flux, 0, count - 1, axis=d)
        total = change if total is None else total + change
    return -total

def wrapped(q):
    return jnp.pad(q, ((0, 0), (2, 2), (2, 2), (2, 2)), mode='wrap')

def reference(state, solver_owner, phi_prev):
    first = state + DTH * tendency(wrapped(state))
    new_state = 0.5 * state + 0.5 * (first + DTH * tendency(wrapped(first)))
    density = new_state[0]
    onehot = (solver_owner[..., None] == jnp.arange(CODES, dtype=jnp.int32)).astype(jnp.float32)
    boxes = density.reshape(BOXES, BX, LINES_Y, CY, LINES_Z, CZ).astype(jnp.float32)
    density_solver = jnp.einsum('jkbc,bxjykz->cxjykz', onehot, boxes, precision=lax.Precision.HIGHEST).reshape(CODES, BX, NY, NZ)
    slots_phi = phi_prev.reshape(CODES, BX, LINES_Y, CY, LINES_Z, CZ).astype(jnp.float32)
    potential = jnp.einsum('jkbc,cxjykz->bxjykz', onehot, slots_phi, precision=lax.Precision.HIGHEST).reshape(NX, NY, NZ)
    beside_all = jnp.zeros_like(potential)
    for axis in (0, 1, 2):
        beside_all = beside_all + jnp.roll(potential, 1, axis) + jnp.roll(potential, -1, axis)
    laplace = beside_all - 6.0 * potential
    mean = jnp.sum(density) / (NX * NY * NZ)
    residual = FOURPIG * (density - mean) - laplace
    return (new_state, density_solver, residual)
```

```python
import functools

import jax
import jax.numpy as jnp
from jax import lax
from jax.experimental import pallas as pl
from jax.experimental.pallas import tpu as pltpu
from jax.sharding import PartitionSpec as P

MESH = pl.DeviceIdType.MESH
GAMMA = 5.0 / 3.0
DTH = 0.04
FOURPIG = 2.0
NF = 7
CX, CY, CZ = 16, 16, 128
PITCH, BASE = 24, 8
ROWS = CX * PITCH + 8
HALF = 8
SLOTS = 4


def pressure(q5):
    return (GAMMA - 1.0) * jnp.maximum(q5, 0.1)


def speeds(get, dirs):
    inv = 1.0 / jnp.maximum(get(0), 0.25)
    sound = jnp.sqrt(GAMMA * pressure(get(5)) * inv)
    return [jnp.abs(get(d)) * inv + sound for d in dirs]


def interface_flux(get, speed_l, speed_r, d):
    def edge(k):
        a, b, c, e = get(k)
        v = 7.0 / 12.0 * (b + c) - 1.0 / 12.0 * (a + e)
        v = jnp.minimum(jnp.maximum(v, jnp.minimum(b, c)), jnp.maximum(b, c))
        return v, c - b

    half = 0.5 * jnp.maximum(speed_l, speed_r)
    e0, j0 = edge(0)
    ed, jd = edge(d)
    e5, j5 = edge(5)
    vel = ed / jnp.maximum(e0, 0.25)
    press = pressure(e5)
    out = [ed - half * j0]
    for k in (1, 2, 3):
        if k == d:
            out.append(ed * vel + press - half * jd)
        else:
            ek, jk = edge(k)
            out.append(ek * vel - half * jk)
    e4, j4 = edge(4)
    out.append((e4 + press) * vel - half * j4)
    out.append(e5 * vel - half * j5)
    e6, j6 = edge(6)
    out.append(e6 * vel - half * j6)
    return out


def lanes(shape=(CY, CZ)):
    return lax.broadcasted_iota(jnp.int32, shape, 1)


def rows_of(i):
    start = i * PITCH + BASE
    if not isinstance(i, int):
        start = pl.multiple_of(start, 8)
    return pl.ds(start, CY)


def z_shifted(q):
    return (pltpu.roll(q, 1, 1), q, pltpu.roll(q, CZ - 1, 1), pltpu.roll(q, CZ - 2, 1))


def each(n, body, unroll=1):
    def step(i, c):
        body(i)
        return c

    lax.fori_loop(0, n, step, 0, unroll=unroll)


def pack_z(load, count, dst):
    lane = lanes()

    def body(i, acc):
        here = (lane >= 8 * i) & (lane < 8 * i + 8)
        shift = lax.rem(8 * i + 4, CZ)
        return tuple(jnp.where(here, pltpu.roll(load(k, i), shift, 1), acc[k]) for k in range(count))

    acc = lax.fori_loop(0, CX, body, tuple(jnp.zeros((CY, CZ), jnp.float32) for _ in range(count)))
    for k in range(count):
        dst[k] = acc[k]


def kernel(n_gx, n_gy, n_gz, owner, state, phi_in, new_out, den_out, res_out,
           q1, q2, phi, sx, sy, sz, dd, fb, fym, tz, nst,
           xh, ysend, yrecv, zpack, zrecv,
           pb, pot, pin, pfirst, gl, gr, go, dsol,
           pxr, pys, pyr, pzs, pzr, res,
           m0, m1, m2, my, mz, mx,
           lsem, osem, hs, hr, ps, pr, ds_, dr, fs, fr, ms, mr):
    gx, gy, gz = lax.axis_index("gx"), lax.axis_index("gy"), lax.axis_index("gz")

    def at(axis, pos, n, off):
        return {axis: lax.rem(pos + (off + n), n)}

    x_lo, x_hi = at("gx", gx, n_gx, -1), at("gx", gx, n_gx, 1)
    y_lo, y_hi = at("gy", gy, n_gy, -1), at("gy", gy, n_gy, 1)
    z_lo, z_hi = at("gz", gz, n_gz, -1), at("gz", gz, n_gz, 1)

    def remote(src, dst, send, recv, dev):
        c = pltpu.make_async_remote_copy(src_ref=src, dst_ref=dst, send_sem=send, recv_sem=recv,
                                         device_id=dev, device_id_type=MESH)
        c.start()
        return c

    loads = {}
    for i in (0, 1, 14, 15, 2, 3, 4, 5, 6, 7, 8, 9, 10, 11, 12, 13):
        c = pltpu.make_async_copy(state.at[:, i], q1.at[:, rows_of(i)], lsem.at[i])
        c.start()
        loads[i] = c
    phi_load = pltpu.make_async_copy(phi_in, phi, lsem.at[CX])
    phi_load.start()

    barrier = pltpu.get_barrier_semaphore()
    peers = [at("gx", gx, n_gx, o) for o in range(1, n_gx)]
    peers += [at("gy", gy, n_gy, o) for o in range(1, n_gy)]
    peers += [at("gz", gz, n_gz, o) for o in range(1, n_gz)]
    for dev in peers:
        pl.semaphore_signal(barrier, inc=1, device_id=dev, device_id_type=MESH)
    pl.semaphore_wait(barrier, len(peers))

    pending = []

    def send_x(q, r):
        cs = []
        for j in (0, 1):
            cs.append(remote(q.at[:, rows_of(14 + j)], xh.at[r, 0, j], hs.at[r, j], hr.at[r, j], x_hi))
            cs.append(remote(q.at[:, rows_of(j)], xh.at[r, 1, j], hs.at[r, 2 + j], hr.at[r, 2 + j], x_lo))
        return cs

    def send_y(q, r):
        for k in range(NF):
            for j in (0, 1):
                ysend[r, 0, k, j] = q[k, pl.ds(BASE + j, CX, stride=PITCH), :]
                ysend[r, 1, k, j] = q[k, pl.ds(BASE + 14 + j, CX, stride=PITCH), :]
        return [remote(ysend.at[r, 1], yrecv.at[r, 0], hs.at[r, 4], hr.at[r, 4], y_hi),
                remote(ysend.at[r, 0], yrecv.at[r, 1], hs.at[r, 5], hr.at[r, 5], y_lo)]

    def send_z(q, r):
        pack_z(lambda k, i: q[k, rows_of(i), :], NF, zpack.at[r])
        return [remote(zpack.at[r], zrecv.at[r, 0], hs.at[r, 6], hr.at[r, 6], z_hi),
                remote(zpack.at[r], zrecv.at[r, 1], hs.at[r, 7], hr.at[r, 7], z_lo)]

    def interior(q):
        def speed_body(i):
            s = speeds(lambda k: q[k, rows_of(i), :], (1, 2, 3))
            sx[i] = s[0]
            sy[rows_of(i), :] = s[1]
            sz[i] = s[2]

        each(CX, speed_body)
        lane = lanes()
        inner = (lane >= 2) & (lane < CZ - 2)

        def z_body(i):
            s = sz[i]
            f = interface_flux(lambda k: z_shifted(q[k, rows_of(i), :]), s, pltpu.roll(s, CZ - 1, 1), 3)
            for k in range(NF):
                dd[k, i] = jnp.where(inner, pltpu.roll(f[k], 1, 1) - f[k], 0.0)

        each(CX, z_body)

        def x_flux(i):
            return interface_flux(lambda k: tuple(q[k, rows_of(i + o), :] for o in (-1, 0, 1, 2)), sx[i], sx[i + 1], 1)

        f = x_flux(1)
        for k in range(NF):
            fb[0, k] = f[k]

        def x_body(i, prev):
            f = x_flux(i)
            for k in range(NF):
                dd[k, i] = dd[k, i] + (prev[k] - f[k])
            return tuple(f)

        f = lax.fori_loop(2, 14, x_body, tuple(f))
        for k in range(NF):
            fb[1, k] = f[k]

    def yz_part(q, r, finish):
        lane = lanes()
        sub = lane & 7
        low = sub < 4

        def z_edge(get):
            s, = speeds(get, (3,))
            f = interface_flux(lambda k: z_shifted(get(k)), s, pltpu.roll(s, CZ - 1, 1), 3)
            return [pltpu.roll(f[k], 1, 1) - f[k] for k in range(NF)]

        left = z_edge(lambda k: jnp.where(low, zrecv[r, 0, k], zpack[r, k]))
        for k in range(NF):
            tz[k] = left[k]
        right = z_edge(lambda k: jnp.where(low, zpack[r, k], zrecv[r, 1, k]))
        for k in range(NF):
            tz[k] = jnp.where(low, right[k], tz[k])

        for k in range(NF):
            for j in (0, 1):
                q[k, pl.ds(BASE - 2 + j, CX, stride=PITCH), :] = yrecv[r, 0, k, j]
                q[k, pl.ds(BASE + CY + j, CX, stride=PITCH), :] = yrecv[r, 1, k, j]
        sy[pl.ds(BASE + CY, CX, stride=PITCH), :] = speeds(lambda k: yrecv[r, 1, k, 0], (2,))[0]
        s_l, = speeds(lambda k: yrecv[r, 0, k, 1], (2,))
        s_r, = speeds(lambda k: ysend[r, 0, k, 0], (2,))
        f = interface_flux(
            lambda k: (yrecv[r, 0, k, 0], yrecv[r, 0, k, 1], ysend[r, 0, k, 0], ysend[r, 0, k, 1]), s_l, s_r, 2)
        for k in range(NF):
            fym[k] = f[k]

        outer = (lane < 2) | (lane >= CZ - 2)
        first_row = lax.broadcasted_iota(jnp.int32, (CY, CZ), 0) == 0

        def y_body(i, done):
            at_ = i * PITCH + BASE
            f = interface_flux(lambda k: tuple(q[k, pl.ds(at_ + o, CY), :] for o in (-1, 0, 1, 2)),
                               sy[pl.ds(at_, CY), :], sy[pl.ds(at_ + 1, CY), :], 2)
            shift = lax.rem(CZ - 4 - 8 * i + CZ, CZ)
            t = []
            for k in range(NF):
                lower = jnp.where(first_row, fym[k, pl.ds(i, 1), :], pltpu.roll(f[k], 1, 0))
                edge = jnp.where(outer, pltpu.roll(tz[k], shift, 1), 0.0)
                t.append(dd[k, i] + ((lower - f[k]) + edge))
            if done:
                finish(i, t)
            else:
                for k in range(NF):
                    dd[k, i] = t[k]

        for i in (0, 14):
            def body(j, i=i):
                y_body(i + j, False)
            each(2, body)

        def body(j):
            y_body(2 + j, True)
        each(12, body)

    def x_part(q, r, finish):
        def get(i):
            if i < 0:
                return lambda k: xh[r, 0, i + 2, k]
            if i >= CX:
                return lambda k: xh[r, 1, i - CX, k]
            return lambda k: q[k, rows_of(i), :]

        def speed(i):
            return sx[i] if 0 <= i < CX else speeds(get(i), (1,))[0]

        def flux(i):
            g = [get(i + o) for o in (-1, 0, 1, 2)]
            return interface_flux(lambda k: tuple(h(k) for h in g), speed(i), speed(i + 1), 1)

        a = flux(-1)
        b = flux(0)
        finish(0, [dd[k, 0] + (a[k] - b[k]) for k in range(NF)])
        finish(1, [dd[k, 1] + (b[k] - fb[0, k]) for k in range(NF)])
        a = flux(14)
        finish(14, [dd[k, 14] + (fb[1, k] - a[k]) for k in range(NF)])
        b = flux(15)
        finish(15, [dd[k, 15] + (a[k] - b[k]) for k in range(NF)])

    def finish_first(i, t):
        for k in range(NF):
            q2[k, rows_of(i), :] = q1[k, rows_of(i), :] + DTH * t[k]

    def finish_new(i, t):
        for k in range(NF):
            nst[k, i] = 0.5 * q1[k, rows_of(i), :] + 0.5 * (q2[k, rows_of(i), :] + DTH * t[k])

    for i in (0, 1, 14, 15):
        loads[i].wait()
    xs = send_x(q1, 0)
    for i in range(2, 14):
        loads[i].wait()
    yzs = send_y(q1, 0) + send_z(q1, 0)
    pending += xs + yzs

    phi_load.wait()

    def is_code(box, slot):
        return jnp.where(owner[box] == gx * SLOTS + slot, 1.0, 0.0).astype(jnp.float32)

    masks = [[[is_code(lax.rem(gx + o, n_gx) * 2 + b, s) for s in range(SLOTS)] for b in (0, 1)] for o in range(4)]

    for o in (2, 1, 3, 0):
        def phi_body(j, o=o):
            rows = [phi[s, j] for s in range(SLOTS)]
            for b in (0, 1):
                m = masks[o][b]
                v = rows[0] * m[0]
                for s in range(1, SLOTS):
                    v = v + rows[s] * m[s]
                pb[o, b, j] = v
        each(HALF, phi_body)
    p1 = [remote(pb.at[2, 0], pfirst.at[0], ps.at[0], pr.at[0], x_hi),
          remote(pb.at[2, 1], pfirst.at[1], ps.at[1], pr.at[1], x_lo)]

    interior(q1)
    for c in yzs:
        c.wait_recv()
    yz_part(q1, 0, finish_first)
    for c in xs:
        c.wait_recv()
    x_part(q1, 0, finish_first)

    xs = send_x(q2, 1)
    yzs = send_y(q2, 1) + send_z(q2, 1)
    pending += xs + yzs

    p2 = [remote(pb.at[1, 1], pin.at[0, 1], ps.at[2], pr.at[2], x_hi),
          remote(pb.at[3, 0], pin.at[1, 0], ps.at[3], pr.at[3], x_lo)]
    for c in p1:
        c.wait_recv()

    def add_body(j):
        pb[1, 0, j] = pb[1, 0, j] + pfirst[0, j]
        pb[3, 1, j] = pb[3, 1, j] + pfirst[1, j]

    each(HALF, add_body)
    p2 += [remote(pb.at[1, 0], pin.at[0, 0], ps.at[4], pr.at[4], x_hi),
           remote(pb.at[3, 1], pin.at[1, 1], ps.at[5], pr.at[5], x_lo)]
    pending += p1 + p2

    interior(q2)
    for c in yzs:
        c.wait_recv()
    yz_part(q2, 1, finish_new)
    for c in xs:
        c.wait_recv()
    x_part(q2, 1, finish_new)

    def mass_body(i, acc):
        return acc + nst[0, i, 0:8, :] + nst[0, i, 8:16, :]

    m0[...] = lax.fori_loop(0, CX, mass_body, jnp.zeros((8, CZ), jnp.float32))

    d1 = [remote(nst.at[0, pl.ds(0, HALF)], gl.at[0], ds_.at[0], dr.at[0], x_hi),
          remote(nst.at[0, pl.ds(HALF, HALF)], gr.at[1], ds_.at[1], dr.at[1], x_lo),
          remote(nst.at[0, pl.ds(HALF, HALF)], gl.at[1], ds_.at[2], dr.at[2], x_hi),
          remote(nst.at[0, pl.ds(0, HALF)], gr.at[0], ds_.at[3], dr.at[3], x_lo)]
    out_state = pltpu.make_async_copy(nst, new_out, osem.at[0])
    out_state.start()

    def spread(src, dst, axis, pos, n, first):
        return [remote(src, dst.at[o - 1], ms.at[first + o - 1], mr.at[first + o - 1], at(axis, pos, n, o))
                for o in range(1, n)]

    m_y = spread(m0, my, "gy", gy, n_gy, 0)

    for c in p2:
        c.wait_recv()

    def pot_body(j):
        for b in (0, 1):
            pot[b * HALF + j] = pb[0, b, j] + (pin[0, b, j] + pin[1, b, j])

    each(HALF, pot_body)
    def row_body(i):
        pys[0, pl.ds(i, 1), :] = pot[i, 0:1, :]
        pys[1, pl.ds(i, 1), :] = pot[i, CY - 1:CY, :]

    each(CX, row_body)
    pack_z(lambda k, i: pot[i], 1, pzs)
    ph = [remote(pot.at[CX - 1], pxr.at[0], fs.at[0], fr.at[0], x_hi),
          remote(pot.at[0], pxr.at[1], fs.at[1], fr.at[1], x_lo),
          remote(pys.at[1], pyr.at[0], fs.at[2], fr.at[2], y_hi),
          remote(pys.at[0], pyr.at[1], fs.at[3], fr.at[3], y_lo),
          remote(pzs.at[0], pzr.at[0], fs.at[4], fr.at[4], z_hi),
          remote(pzs.at[0], pzr.at[1], fs.at[5], fr.at[5], z_lo)]
    pending += ph

    def gathered(copies, own, got, n, out):
        for c in copies:
            c.wait_recv()
        acc = own[...]
        for o in range(n - 1):
            acc = acc + got[o]
        out[...] = acc

    gathered(m_y, m0, my, n_gy, m1)
    m_z = spread(m1, mz, "gz", gz, n_gz, n_gy - 1)

    d1[0].wait_recv()
    d2 = [remote(gl.at[0], go.at[0], ds_.at[4], dr.at[4], x_hi)]
    d1[1].wait_recv()
    d2 += [remote(gr.at[1], go.at[1], ds_.at[5], dr.at[5], x_lo)]

    gathered(m_z, m1, mz, n_gz, m2)
    m_x = spread(m2, mx, "gx", gx, n_gx, n_gy + n_gz - 2)
    pending += m_y + m_z + m_x

    for c in ph:
        c.wait_recv()
    lane = lanes()
    row = lax.broadcasted_iota(jnp.int32, (CY, CZ), 0)
    halo = jnp.where((lane & 7) < 4, pzr[0, :, :], pzr[1, :, :])

    def lap(i, below, above):
        p = pot[i]
        h = pltpu.roll(halo, lax.rem(CZ - 4 - 8 * i + CZ, CZ), 1)
        z = pltpu.roll(jnp.where(lane == CZ - 1, h, p), 1, 1) + pltpu.roll(jnp.where(lane == 0, h, p), CZ - 1, 1)
        up = jnp.where(row == 0, pyr[0, pl.ds(i, 1), :], pltpu.roll(p, 1, 0))
        dn = jnp.where(row == CY - 1, pyr[1, pl.ds(i, 1), :], pltpu.roll(p, CY - 1, 0))
        res[i] = FOURPIG * nst[0, i] - (((below + above) + (up + dn) + z) - 6.0 * p)

    lap(0, pxr[0], pot[1])

    def lap_body(j):
        lap(j + 1, pot[j], pot[j + 2])
    each(CX - 2, lap_body)
    lap(CX - 1, pot[CX - 2], pxr[1])

    for c in m_x:
        c.wait_recv()
    total = m2[...]
    for o in range(n_gx - 1):
        total = total + mx[o]
    cells = float(CX * CY * CZ * n_gx * n_gy * n_gz)
    mean = jnp.sum(total) * (FOURPIG / cells)

    def mean_body(i):
        res[i] = res[i] - mean
    each(CX, mean_body)
    out_res = pltpu.make_async_copy(res, res_out, osem.at[1])
    out_res.start()

    for c in (d1[2], d1[3]):
        c.wait_recv()

    def is_box(o, b, s):
        return is_code(lax.rem(gx + o, n_gx) * 2 + b, s)

    near = [[(is_box(o, b, s)) for o in (0, 3, 1) for b in (0, 1)] for s in range(SLOTS)]

    def near_body(j):
        boxes = [nst[0, j], nst[0, HALF + j], gl[0, j], gl[1, j], gr[0, j], gr[1, j]]
        for s in range(SLOTS):
            v = boxes[0] * near[s][0]
            for t in range(1, 6):
                v = v + boxes[t] * near[s][t]
            dsol[s, j] = v
    each(HALF, near_body)
    far = [[is_box(2, b, s) for b in (0, 1)] for s in range(SLOTS)]
    for c in d2:
        c.wait_recv()

    def far_body(j):
        boxes = [go[0, j], go[1, j]]
        for s in range(SLOTS):
            dsol[s, j] = dsol[s, j] + (boxes[0] * far[s][0] + boxes[1] * far[s][1])
    each(HALF, far_body)
    out_den = pltpu.make_async_copy(dsol, den_out, osem.at[2])
    out_den.start()

    pending += d1 + d2
    for c in pending:
        c.wait_send()
    out_state.wait()
    out_res.wait()
    out_den.wait()


def solution(mesh):
    n_gx, n_gy, n_gz = mesh.shape["gx"], mesh.shape["gy"], mesh.shape["gz"]

    def on_device(state, solver_owner, phi_prev):
        f32 = jnp.float32
        V = lambda *s: pltpu.VMEM(s, f32)
        D = lambda *s: pltpu.SemaphoreType.DMA(s)
        n_mass = n_gx + n_gy + n_gz - 3
        anyspace = pl.BlockSpec(memory_space=pl.ANY)
        return pl.pallas_call(
            functools.partial(kernel, n_gx, n_gy, n_gz),
            out_shape=(
                jax.ShapeDtypeStruct(state.shape, f32),
                jax.ShapeDtypeStruct(phi_prev.shape, f32),
                jax.ShapeDtypeStruct(state.shape[1:], f32),
            ),
            in_specs=[pl.BlockSpec(memory_space=pltpu.SMEM), anyspace, anyspace],
            out_specs=(anyspace, anyspace, anyspace),
            scratch_shapes=[
                V(NF, ROWS, CZ), V(NF, ROWS, CZ), V(SLOTS, HALF, CY, CZ),
                V(CX, CY, CZ), V(ROWS, CZ), V(CX, CY, CZ), V(NF, CX, CY, CZ),
                V(2, NF, CY, CZ), V(NF, CX, CZ), V(NF, CY, CZ), V(NF, CX, CY, CZ),
                V(2, 2, 2, NF, CY, CZ), V(2, 2, NF, 2, CX, CZ), V(2, 2, NF, 2, CX, CZ),
                V(2, NF, CY, CZ), V(2, 2, NF, CY, CZ),
                V(4, 2, HALF, CY, CZ), V(CX, CY, CZ), V(2, 2, HALF, CY, CZ), V(2, HALF, CY, CZ),
                V(2, HALF, CY, CZ), V(2, HALF, CY, CZ), V(2, HALF, CY, CZ), V(SLOTS, HALF, CY, CZ),
                V(2, CY, CZ), V(2, CX, CZ), V(2, CX, CZ), V(1, CY, CZ), V(2, CY, CZ), V(CX, CY, CZ),
                V(8, CZ), V(8, CZ), V(8, CZ),
                V(n_gy - 1, 8, CZ), V(n_gz - 1, 8, CZ), V(n_gx - 1, 8, CZ),
                D(CX + 1), D(3), D(2, 8), D(2, 8), D(6), D(6), D(6), D(6), D(6), D(6), D(n_mass), D(n_mass),
            ],
            compiler_params=pltpu.CompilerParams(
                collective_id=0, has_side_effects=True, vmem_limit_bytes=32 * 1024 * 1024
            ),
            name="gas_step",
        )(solver_owner.reshape(-1), state, phi_prev)

    return jax.shard_map(
        on_device,
        mesh=mesh,
        in_specs=(P(None, "gx", "gy", "gz"), P("gy", "gz", None), P("gx", None, "gy", "gz")),
        out_specs=(P(None, "gx", "gy", "gz"), P("gx", None, "gy", "gz"), P("gx", "gy", "gz")),
        check_vma=False,
    )
```

```python
import functools

import jax
import jax.numpy as jnp
from jax import lax
from jax.experimental import pallas as pl
from jax.experimental.pallas import tpu as pltpu
from jax.sharding import PartitionSpec as P

MESH = pl.DeviceIdType.MESH
GAMMA = 5.0 / 3.0
DTH = 0.04
FOURPIG = 2.0
NF = 7
CX, CY, CZ = 16, 16, 128
PITCH, BASE = 24, 8
ROWS = CX * PITCH + 8
HALF = 8
SLOTS = 4
UN = 2


def pressure(q5):
    return (GAMMA - 1.0) * jnp.maximum(q5, 0.1)


def speeds(get, dirs):
    inv = 1.0 / jnp.maximum(get(0), 0.25)
    sound = jnp.sqrt(GAMMA * pressure(get(5)) * inv)
    return [jnp.abs(get(d)) * inv + sound for d in dirs]


def interface_flux(get, speed_l, speed_r, d):
    def edge(k):
        a, b, c, e = get(k)
        v = 7.0 / 12.0 * (b + c) - 1.0 / 12.0 * (a + e)
        v = jnp.minimum(jnp.maximum(v, jnp.minimum(b, c)), jnp.maximum(b, c))
        return v, c - b

    half = 0.5 * jnp.maximum(speed_l, speed_r)
    e0, j0 = edge(0)
    ed, jd = edge(d)
    e5, j5 = edge(5)
    vel = ed / jnp.maximum(e0, 0.25)
    press = pressure(e5)
    out = [ed - half * j0]
    for k in (1, 2, 3):
        if k == d:
            out.append(ed * vel + press - half * jd)
        else:
            ek, jk = edge(k)
            out.append(ek * vel - half * jk)
    e4, j4 = edge(4)
    out.append((e4 + press) * vel - half * j4)
    out.append(e5 * vel - half * j5)
    e6, j6 = edge(6)
    out.append(e6 * vel - half * j6)
    return out


def lanes(shape=(CY, CZ)):
    return lax.broadcasted_iota(jnp.int32, shape, 1)


def rows_of(i):
    start = i * PITCH + BASE
    if not isinstance(i, int):
        start = pl.multiple_of(start, 8)
    return pl.ds(start, CY)


def z_shifted(q):
    return (pltpu.roll(q, 1, 1), q, pltpu.roll(q, CZ - 1, 1), pltpu.roll(q, CZ - 2, 1))


def each(n, body, unroll=1):
    def step(i, c):
        body(i)
        return c

    lax.fori_loop(0, n, step, 0, unroll=unroll)


def pack_z(load, acc, slabs, unroll):
    lane = lanes()

    def put(i, acc, shift):
        here = (lane >= 8 * i) & (lane < 8 * i + 8)
        return tuple(jnp.where(here, pltpu.roll(load(k, i), shift, 1), a) for k, a in enumerate(acc))

    if isinstance(slabs, tuple):
        for i in slabs:
            acc = put(i, acc, (8 * i + 4) % CZ)
        return acc
    return lax.fori_loop(slabs.start, slabs.stop, lambda i, a: put(i, a, lax.rem(8 * i + 4, CZ)), acc, unroll=unroll)


def blank(count):
    return tuple(jnp.zeros((CY, CZ), jnp.float32) for _ in range(count))


def move_out(*refs):
    n = (len(refs) - 1) // 2
    sem = refs[-1]
    copies = [pltpu.make_async_copy(refs[i], refs[n + i], sem.at[i]) for i in range(n)]
    for c in copies:
        c.start()
    for c in copies:
        c.wait()


def kernel(n_gx, n_gy, n_gz, owner_in, state, phi_in, nst, dsol, res,
           owner_ref, q1, q2, phi, sx, sy, sz, dd, fb, fym, tz,
           xh, ysend, yrecv, zpack, zsend, zrecv,
           pb, pot, pin, pfirst, gl, gr, go,
           pxr, pys, pyr, pzs, pzr,
           m0, m1, m2, mx, my, mz,
           lsem, hs, hr, ps, pr, ds_, dr, fs, fr, ms, mr):
    gx, gy, gz = lax.axis_index("gx"), lax.axis_index("gy"), lax.axis_index("gz")

    def at(axis, pos, n, off):
        return {axis: lax.rem(pos + (off + n), n)}

    x_lo, x_hi = at("gx", gx, n_gx, -1), at("gx", gx, n_gx, 1)
    y_lo, y_hi = at("gy", gy, n_gy, -1), at("gy", gy, n_gy, 1)
    z_lo, z_hi = at("gz", gz, n_gz, -1), at("gz", gz, n_gz, 1)

    def remote(src, dst, send, recv, dev):
        c = pltpu.make_async_remote_copy(src_ref=src, dst_ref=dst, send_sem=send, recv_sem=recv,
                                         device_id=dev, device_id_type=MESH)
        c.start()
        return c

    loads = {}
    for i in (0, 1, 14, 15, 2, 3, 4, 5, 6, 7, 8, 9, 10, 11, 12, 13):
        c = pltpu.make_async_copy(state.at[:, i], q1.at[:, rows_of(i)], lsem.at[i])
        c.start()
        loads[i] = c
    phi_load = pltpu.make_async_copy(phi_in, phi, lsem.at[CX])
    phi_load.start()
    owner_load = pltpu.make_async_copy(owner_in, owner_ref, lsem.at[CX + 1])
    owner_load.start()

    barrier = pltpu.get_barrier_semaphore()
    peers = [x_lo, x_hi, y_lo, y_hi, z_lo, z_hi, at("gy", gy, n_gy, n_gy // 2), at("gz", gz, n_gz, n_gz // 2)]
    for dev in peers:
        pl.semaphore_signal(barrier, inc=1, device_id=dev, device_id_type=MESH)

    pending = []

    def send_x(q, r):
        cs = []
        for j in (0, 1):
            cs.append(remote(q.at[:, rows_of(14 + j)], xh.at[r, 0, j], hs.at[r, j], hr.at[r, j], x_hi))
            cs.append(remote(q.at[:, rows_of(j)], xh.at[r, 1, j], hs.at[r, 2 + j], hr.at[r, 2 + j], x_lo))
        return cs

    def pack_y(q, r):
        for k in range(NF):
            for j in (0, 1):
                ysend[r, 0, k, j] = q[k, pl.ds(BASE + j, CX, stride=PITCH), :]
                ysend[r, 1, k, j] = q[k, pl.ds(BASE + 14 + j, CX, stride=PITCH), :]

    def pack_inner(q, r):
        acc = pack_z(lambda k, i: q[k, rows_of(i), :], blank(NF), range(2, CX - 2), 6)
        for k in range(NF):
            zpack[r, k] = acc[k]

    def pack_outer(q, r):
        acc = pack_z(lambda k, i: q[k, rows_of(i), :], tuple(zpack[r, k] for k in range(NF)), (0, 1, 14, 15), 1)
        low = (lanes((8, CZ)) & 7) < 4
        for k in range(NF):
            zpack[r, k] = acc[k]
            top, bottom = acc[k][0:8], acc[k][8:16]
            zsend[r, 1, k] = jnp.where(low, top, pltpu.roll(bottom, 4, 1))
            zsend[r, 0, k] = jnp.where(low, pltpu.roll(top, CZ - 4, 1), bottom)

    def send_y(r):
        return [remote(ysend.at[r, 1], yrecv.at[r, 0], hs.at[r, 4], hr.at[r, 4], y_hi),
                remote(ysend.at[r, 0], yrecv.at[r, 1], hs.at[r, 5], hr.at[r, 5], y_lo)]

    def send_z(r):
        return [remote(zsend.at[r, 1], zrecv.at[r, 0], hs.at[r, 6], hr.at[r, 6], z_hi),
                remote(zsend.at[r, 0], zrecv.at[r, 1], hs.at[r, 7], hr.at[r, 7], z_lo)]

    def interior(q):
        def speed_body(i):
            s = speeds(lambda k: q[k, rows_of(i), :], (1, 2, 3))
            sx[i] = s[0]
            sy[rows_of(i), :] = s[1]
            sz[i] = s[2]

        each(CX, speed_body, UN)
        lane = lanes()
        inner = (lane >= 2) & (lane < CZ - 2)

        def z_body(i):
            s = sz[i]
            f = interface_flux(lambda k: z_shifted(q[k, rows_of(i), :]), s, pltpu.roll(s, CZ - 1, 1), 3)
            for k in range(NF):
                dd[k, i] = jnp.where(inner, pltpu.roll(f[k], 1, 1) - f[k], 0.0)

        each(CX, z_body, UN)

        def x_flux(i):
            return interface_flux(lambda k: tuple(q[k, rows_of(i + o), :] for o in (-1, 0, 1, 2)), sx[i], sx[i + 1], 1)

        f = x_flux(1)
        for k in range(NF):
            fb[0, k] = f[k]

        def x_body(i, prev):
            f = x_flux(i)
            for k in range(NF):
                dd[k, i] = dd[k, i] + (prev[k] - f[k])
            return tuple(f)

        f = lax.fori_loop(2, 14, x_body, tuple(f), unroll=UN)
        for k in range(NF):
            fb[1, k] = f[k]

    def y_part(q, r):
        for k in range(NF):
            for j in (0, 1):
                q[k, pl.ds(BASE - 2 + j, CX, stride=PITCH), :] = yrecv[r, 0, k, j]
                q[k, pl.ds(BASE + CY + j, CX, stride=PITCH), :] = yrecv[r, 1, k, j]
        sy[pl.ds(BASE + CY, CX, stride=PITCH), :] = speeds(lambda k: yrecv[r, 1, k, 0], (2,))[0]
        s_l, = speeds(lambda k: yrecv[r, 0, k, 1], (2,))
        s_r, = speeds(lambda k: ysend[r, 0, k, 0], (2,))
        f = interface_flux(
            lambda k: (yrecv[r, 0, k, 0], yrecv[r, 0, k, 1], ysend[r, 0, k, 0], ysend[r, 0, k, 1]), s_l, s_r, 2)
        for k in range(NF):
            fym[k] = f[k]
        first_row = lax.broadcasted_iota(jnp.int32, (CY, CZ), 0) == 0

        def y_body(i):
            at_ = i * PITCH + BASE
            f = interface_flux(lambda k: tuple(q[k, pl.ds(at_ + o, CY), :] for o in (-1, 0, 1, 2)),
                               sy[pl.ds(at_, CY), :], sy[pl.ds(at_ + 1, CY), :], 2)
            for k in range(NF):
                lower = jnp.where(first_row, fym[k, pl.ds(i, 1), :], pltpu.roll(f[k], 1, 0))
                dd[k, i] = dd[k, i] + (lower - f[k])

        each(CX, y_body, UN)

    def z_part(r):
        low = (lanes() & 7) < 4

        def z_edge(cells):
            s, = speeds(lambda k: cells[k], (3,))
            f = interface_flux(lambda k: z_shifted(cells[k]), s, pltpu.roll(s, CZ - 1, 1), 3)
            return [pltpu.roll(f[k], 1, 1) - f[k] for k in range(NF)]

        def from_left(k):
            m = zrecv[r, 0, k]
            return jnp.concatenate([m, pltpu.roll(m, CZ - 4, 1)], axis=0)

        def from_right(k):
            m = zrecv[r, 1, k]
            return jnp.concatenate([pltpu.roll(m, 4, 1), m], axis=0)

        left = z_edge([jnp.where(low, from_left(k), zpack[r, k]) for k in range(NF)])
        for k in range(NF):
            tz[k] = left[k]
        right = z_edge([jnp.where(low, zpack[r, k], from_right(k)) for k in range(NF)])
        for k in range(NF):
            tz[k] = jnp.where(low, right[k], tz[k])

    def tendency(i, k):
        lane = lanes()
        outer = (lane < 2) | (lane >= CZ - 2)
        shift = (2 * CZ - 4 - 8 * i) % CZ if isinstance(i, int) else lax.rem(2 * CZ - 4 - 8 * i, CZ)
        return dd[k, i] + jnp.where(outer, pltpu.roll(tz[k], shift, 1), 0.0)

    def x_part(q, r, finish):
        def get(i):
            if i < 0:
                return lambda k: xh[r, 0, i + 2, k]
            if i >= CX:
                return lambda k: xh[r, 1, i - CX, k]
            return lambda k: q[k, rows_of(i), :]

        def speed(i):
            return sx[i] if 0 <= i < CX else speeds(get(i), (1,))[0]

        def flux(i):
            g = [get(i + o) for o in (-1, 0, 1, 2)]
            return interface_flux(lambda k: tuple(h(k) for h in g), speed(i), speed(i + 1), 1)

        a = flux(-1)
        b = flux(0)
        finish(0, [tendency(0, k) + (a[k] - b[k]) for k in range(NF)])
        finish(1, [tendency(1, k) + (b[k] - fb[0, k]) for k in range(NF)])
        a = flux(14)
        finish(14, [tendency(14, k) + (fb[1, k] - a[k]) for k in range(NF)])
        b = flux(15)
        finish(15, [tendency(15, k) + (a[k] - b[k]) for k in range(NF)])

    def rest(finish):
        def body(j):
            finish(2 + j, [tendency(2 + j, k) for k in range(NF)])
        each(CX - 4, body, UN)

    def finish_first(i, t):
        for k in range(NF):
            q2[k, rows_of(i), :] = q1[k, rows_of(i), :] + DTH * t[k]

    def finish_new(i, t):
        for k in range(NF):
            nst[k, i] = 0.5 * q1[k, rows_of(i), :] + 0.5 * (q2[k, rows_of(i), :] + DTH * t[k])

    for i in range(CX):
        loads[i].wait()
    pack_inner(q1, 0)
    pack_outer(q1, 0)
    pl.semaphore_wait(barrier, len(peers))
    zs = send_z(0)
    xs = send_x(q1, 0)
    pack_y(q1, 0)
    ys = send_y(0)
    pending += xs + ys + zs

    phi_load.wait()
    owner_load.wait()

    def is_code(box, slot):
        return jnp.where(owner_ref[0, 0, box] == gx * SLOTS + slot, 1.0, 0.0).astype(jnp.float32)

    masks = [[[is_code(lax.rem(gx + o, n_gx) * 2 + b, s) for s in range(SLOTS)] for b in (0, 1)] for o in range(4)]

    for o in (2, 1, 3, 0):
        def phi_body(j, o=o):
            rows = [phi[s, j] for s in range(SLOTS)]
            for b in (0, 1):
                m = masks[o][b]
                v = rows[0] * m[0]
                for s in range(1, SLOTS):
                    v = v + rows[s] * m[s]
                pb[o, b, j] = v
        each(HALF, phi_body)
    interior(q1)
    for c in ys:
        c.wait_recv()
    y_part(q1, 0)
    p1 = [remote(pb.at[2, 0], pfirst.at[0], ps.at[0], pr.at[0], x_hi),
          remote(pb.at[2, 1], pfirst.at[1], ps.at[1], pr.at[1], x_lo)]
    for c in zs:
        c.wait_recv()
    z_part(0)
    rest(finish_first)
    pack_inner(q2, 1)
    for c in xs:
        c.wait_recv()
    x_part(q1, 0, finish_first)

    pack_outer(q2, 1)
    zs = send_z(1)
    xs = send_x(q2, 1)
    pack_y(q2, 1)
    ys = send_y(1)
    pending += xs + ys + zs

    interior(q2)
    for c in ys:
        c.wait_recv()
    y_part(q2, 1)
    p2 = [remote(pb.at[1, 1], pin.at[0, 1], ps.at[2], pr.at[2], x_hi),
          remote(pb.at[3, 0], pin.at[1, 0], ps.at[3], pr.at[3], x_lo)]
    for c in p1:
        c.wait_recv()

    def add_body(j):
        pb[1, 0, j] = pb[1, 0, j] + pfirst[0, j]
        pb[3, 1, j] = pb[3, 1, j] + pfirst[1, j]

    each(HALF, add_body)
    p2 += [remote(pb.at[1, 0], pin.at[0, 0], ps.at[4], pr.at[4], x_hi),
           remote(pb.at[3, 1], pin.at[1, 1], ps.at[5], pr.at[5], x_lo)]
    pending += p1 + p2
    for c in zs:
        c.wait_recv()
    z_part(1)
    rest(finish_new)
    for c in xs:
        c.wait_recv()
    x_part(q2, 1, finish_new)

    d1 = [remote(nst.at[0, pl.ds(0, HALF)], gl.at[0], ds_.at[0], dr.at[0], x_hi),
          remote(nst.at[0, pl.ds(HALF, HALF)], gr.at[1], ds_.at[1], dr.at[1], x_lo),
          remote(nst.at[0, pl.ds(HALF, HALF)], gl.at[1], ds_.at[2], dr.at[2], x_hi),
          remote(nst.at[0, pl.ds(0, HALF)], gr.at[0], ds_.at[3], dr.at[3], x_lo)]

    def mass_body(i, acc):
        return acc + nst[0, i, 0:8, :] + nst[0, i, 8:16, :]

    m0[...] = lax.fori_loop(0, CX, mass_body, jnp.zeros((8, CZ), jnp.float32), unroll=4)

    def spread(src, dst, devices, first):
        return [remote(src, dst.at[t], ms.at[first + t], mr.at[first + t], dev) for t, dev in enumerate(devices)]

    def gathered(copies, own, got, n):
        for c in copies:
            c.wait_recv()
        acc = own[...]
        for o in range(n - 1):
            acc = acc + got[o]
        return acc

    n_zy = n_gz // 2
    along_y = [{"gz": (gz // n_zy) * n_zy + lax.rem(gz + o, n_zy)} for o in range(1, n_zy)]
    along_z = [{**at("gx", gx, n_gx, o), **at("gz", gz, n_gz, h * n_zy)}
               for o in range(n_gx) for h in (0, 1) if o + h > 0]
    m_x = spread(m0, mx, [at("gy", gy, n_gy, o) for o in range(1, n_gy)], 0)

    m1[...] = gathered(m_x, m0, mx, n_gy)
    m_y = spread(m1, my, along_y, n_gy - 1)
    m2[...] = gathered(m_y, m1, my, n_zy)
    m_z = spread(m2, mz, along_z, n_gy + n_zy - 2)
    pending += m_y + m_z + m_x

    for c in p2:
        c.wait_recv()

    def pot_body(j):
        for b in (0, 1):
            pot[b * HALF + j] = pb[0, b, j] + (pin[0, b, j] + pin[1, b, j])

    each(HALF, pot_body)
    def row_body(i):
        pys[0, pl.ds(i, 1), :] = pot[i, 0:1, :]
        pys[1, pl.ds(i, 1), :] = pot[i, CY - 1:CY, :]

    each(CX, row_body)
    pzs[0] = pack_z(lambda k, i: pot[i], blank(1), range(0, CX), 4)[0]
    ph = [remote(pot.at[CX - 1], pxr.at[0], fs.at[0], fr.at[0], x_hi),
          remote(pot.at[0], pxr.at[1], fs.at[1], fr.at[1], x_lo),
          remote(pys.at[1], pyr.at[0], fs.at[2], fr.at[2], y_hi),
          remote(pys.at[0], pyr.at[1], fs.at[3], fr.at[3], y_lo),
          remote(pzs.at[0], pzr.at[0], fs.at[4], fr.at[4], z_hi),
          remote(pzs.at[0], pzr.at[1], fs.at[5], fr.at[5], z_lo)]
    pending += ph

    d1[0].wait_recv()
    d2 = [remote(gl.at[0], go.at[0], ds_.at[4], dr.at[4], x_hi)]
    d1[1].wait_recv()
    d2 += [remote(gr.at[1], go.at[1], ds_.at[5], dr.at[5], x_lo)]

    for c in ph:
        c.wait_recv()
    lane = lanes()
    row = lax.broadcasted_iota(jnp.int32, (CY, CZ), 0)
    halo = jnp.where((lane & 7) < 4, pzr[0, :, :], pzr[1, :, :])

    def lap(i, below, above):
        p = pot[i]
        h = pltpu.roll(halo, lax.rem(CZ - 4 - 8 * i + CZ, CZ), 1)
        z = pltpu.roll(jnp.where(lane == CZ - 1, h, p), 1, 1) + pltpu.roll(jnp.where(lane == 0, h, p), CZ - 1, 1)
        up = jnp.where(row == 0, pyr[0, pl.ds(i, 1), :], pltpu.roll(p, 1, 0))
        dn = jnp.where(row == CY - 1, pyr[1, pl.ds(i, 1), :], pltpu.roll(p, CY - 1, 0))
        res[i] = FOURPIG * nst[0, i] - (((below + above) + (up + dn) + z) - 6.0 * p)

    lap(0, pxr[0], pot[1])

    def lap_body(j):
        lap(j + 1, pot[j], pot[j + 2])
    each(CX - 2, lap_body, 7)
    lap(CX - 1, pot[CX - 2], pxr[1])

    total = gathered(m_z, m2, mz, len(along_z) + 1)
    cells = float(CX * CY * CZ * n_gx * n_gy * n_gz)
    mean = jnp.sum(total) * (FOURPIG / cells)

    def mean_body(i):
        res[i] = res[i] - mean
    each(CX, mean_body)

    for c in (d1[2], d1[3]):
        c.wait_recv()

    def is_box(o, b, s):
        return is_code(lax.rem(gx + o, n_gx) * 2 + b, s)

    near = [[(is_box(o, b, s)) for o in (0, 3, 1) for b in (0, 1)] for s in range(SLOTS)]

    def near_body(j):
        boxes = [nst[0, j], nst[0, HALF + j], gl[0, j], gl[1, j], gr[0, j], gr[1, j]]
        for s in range(SLOTS):
            v = boxes[0] * near[s][0]
            for t in range(1, 6):
                v = v + boxes[t] * near[s][t]
            dsol[s, j] = v
    each(HALF, near_body)
    far = [[is_box(2, b, s) for b in (0, 1)] for s in range(SLOTS)]
    for c in d2:
        c.wait_recv()

    def far_body(j):
        boxes = [go[0, j], go[1, j]]
        for s in range(SLOTS):
            dsol[s, j] = dsol[s, j] + (boxes[0] * far[s][0] + boxes[1] * far[s][1])
    each(HALF, far_body)

    pending += d1 + d2
    for c in pending:
        c.wait_send()


def solution(mesh):
    n_gx, n_gy, n_gz = mesh.shape["gx"], mesh.shape["gy"], mesh.shape["gz"]

    def on_device(state, solver_owner, phi_prev):
        f32 = jnp.float32
        V = lambda *s: pltpu.VMEM(s, f32)
        D = lambda *s: pltpu.SemaphoreType.DMA(s)
        n_mass = 2 * n_gx + n_gy + n_gz // 2 - 3
        hbm = pl.BlockSpec(memory_space=pltpu.HBM)
        vmem = pl.BlockSpec(memory_space=pltpu.VMEM)
        outs = pl.pallas_call(
            functools.partial(kernel, n_gx, n_gy, n_gz),
            out_shape=(
                jax.ShapeDtypeStruct(state.shape, f32),
                jax.ShapeDtypeStruct(phi_prev.shape, f32),
                jax.ShapeDtypeStruct(state.shape[1:], f32),
            ),
            in_specs=[hbm, hbm, hbm],
            out_specs=(vmem, vmem, vmem),
            scratch_shapes=[
                pltpu.SMEM((1, 1, 8), jnp.int32),
                V(NF, ROWS, CZ), V(NF, ROWS, CZ), V(SLOTS, HALF, CY, CZ),
                V(CX, CY, CZ), V(ROWS, CZ), V(CX, CY, CZ), V(NF, CX, CY, CZ),
                V(2, NF, CY, CZ), V(NF, CX, CZ), V(NF, CY, CZ),
                V(2, 2, 2, NF, CY, CZ), V(2, 2, NF, 2, CX, CZ), V(2, 2, NF, 2, CX, CZ),
                V(2, NF, CY, CZ), V(2, 2, NF, 8, CZ), V(2, 2, NF, 8, CZ),
                V(4, 2, HALF, CY, CZ), V(CX, CY, CZ), V(2, 2, HALF, CY, CZ), V(2, HALF, CY, CZ),
                V(2, HALF, CY, CZ), V(2, HALF, CY, CZ), V(2, HALF, CY, CZ),
                V(2, CY, CZ), V(2, CX, CZ), V(2, CX, CZ), V(1, CY, CZ), V(2, CY, CZ),
                V(8, CZ), V(8, CZ), V(8, CZ),
                V(n_gy - 1, 8, CZ), V(n_gz // 2 - 1, 8, CZ), V(2 * n_gx - 1, 8, CZ),
                D(CX + 2), D(2, 8), D(2, 8), D(6), D(6), D(6), D(6), D(6), D(6), D(n_mass), D(n_mass),
            ],
            compiler_params=pltpu.CompilerParams(
                collective_id=0, has_side_effects=True, vmem_limit_bytes=32 * 1024 * 1024
            ),
            name="gas_step",
        )(
            pltpu.with_memory_space_constraint(solver_owner, pltpu.HBM),
            pltpu.with_memory_space_constraint(state, pltpu.HBM),
            pltpu.with_memory_space_constraint(phi_prev, pltpu.HBM),
        )
        return pl.pallas_call(
            move_out,
            out_shape=tuple(jax.ShapeDtypeStruct(o.shape, f32) for o in outs),
            in_specs=[vmem] * 3,
            out_specs=(hbm,) * 3,
            scratch_shapes=[D(3)],
            compiler_params=pltpu.CompilerParams(has_side_effects=True, vmem_limit_bytes=4 * 1024 * 1024),
            name="move_out",
        )(*outs)

    return jax.shard_map(
        on_device,
        mesh=mesh,
        in_specs=(P(None, "gx", "gy", "gz"), P("gy", "gz", None), P("gx", None, "gy", "gz")),
        out_specs=(P(None, "gx", "gy", "gz"), P("gx", None, "gy", "gz"), P("gx", "gy", "gz")),
        check_vma=False,
    )
```

```python
import functools

import jax
import jax.numpy as jnp
from jax import lax
from jax.experimental import pallas as pl
from jax.experimental.pallas import tpu as pltpu
from jax.sharding import PartitionSpec as P

MESH = pl.DeviceIdType.MESH
GAMMA = 5.0 / 3.0
DTH = 0.04
FOURPIG = 2.0
NF = 7
CX, CY, CZ = 16, 16, 128
PITCH, BASE = 24, 8
ROWS = CX * PITCH + 8
HALF = 8
SLOTS = 4
UN = 2


def pressure(q5):
    return (GAMMA - 1.0) * jnp.maximum(q5, 0.1)


def speeds(get, dirs):
    inv = 1.0 / jnp.maximum(get(0), 0.25)
    sound = jnp.sqrt(GAMMA * pressure(get(5)) * inv)
    return [jnp.abs(get(d)) * inv + sound for d in dirs]


def interface_flux(get, speed_l, speed_r, d):
    def edge(k):
        a, b, c, e = get(k)
        v = 7.0 / 12.0 * (b + c) - 1.0 / 12.0 * (a + e)
        v = jnp.minimum(jnp.maximum(v, jnp.minimum(b, c)), jnp.maximum(b, c))
        return v, c - b

    half = 0.5 * jnp.maximum(speed_l, speed_r)
    e0, j0 = edge(0)
    ed, jd = edge(d)
    e5, j5 = edge(5)
    vel = ed / jnp.maximum(e0, 0.25)
    press = pressure(e5)
    out = [ed - half * j0]
    for k in (1, 2, 3):
        if k == d:
            out.append(ed * vel + press - half * jd)
        else:
            ek, jk = edge(k)
            out.append(ek * vel - half * jk)
    e4, j4 = edge(4)
    out.append((e4 + press) * vel - half * j4)
    out.append(e5 * vel - half * j5)
    e6, j6 = edge(6)
    out.append(e6 * vel - half * j6)
    return out


def lanes(shape=(CY, CZ)):
    return lax.broadcasted_iota(jnp.int32, shape, 1)


def rows_of(i):
    start = i * PITCH + BASE
    if not isinstance(i, int):
        start = pl.multiple_of(start, 8)
    return pl.ds(start, CY)


def z_shifted(q):
    return (pltpu.roll(q, 1, 1), q, pltpu.roll(q, CZ - 1, 1), pltpu.roll(q, CZ - 2, 1))


def each(n, body, unroll=1):
    def step(i, c):
        body(i)
        return c

    lax.fori_loop(0, n, step, 0, unroll=unroll)


def pack_z(load, acc, slabs, unroll):
    lane = lanes()

    def put(i, acc, shift):
        here = (lane >= 8 * i) & (lane < 8 * i + 8)
        return tuple(jnp.where(here, pltpu.roll(load(k, i), shift, 1), a) for k, a in enumerate(acc))

    if isinstance(slabs, tuple):
        for i in slabs:
            acc = put(i, acc, (8 * i + 4) % CZ)
        return acc
    return lax.fori_loop(slabs.start, slabs.stop, lambda i, a: put(i, a, lax.rem(8 * i + 4, CZ)), acc, unroll=unroll)


def blank(count):
    return tuple(jnp.zeros((CY, CZ), jnp.float32) for _ in range(count))


def move_out(*refs):
    n = (len(refs) - 1) // 2
    sem = refs[-1]
    for i in range(n):
        for p in range(refs[i].shape[0]):
            pltpu.make_async_copy(refs[i].at[p], refs[n + i].at[p], sem.at[i]).start()
    for i in range(n):
        pltpu.make_async_copy(refs[i], refs[n + i], sem.at[i]).wait()


def kernel(n_gx, n_gy, n_gz, owner_in, state, phi_in, nst, dsol, res,
           owner_ref, q1, q2, phi, sx, sy, sz, dd, fb, fym, tz,
           xh, ysend, yrecv, zpack, zsend, zrecv,
           pb, pot, pin, pfirst, gl, gr, go,
           pxr, pys, pyr, pzs, pzr,
           m0, m1, m2, mx, my, mz,
           lsem, hs, hr, ps, pr, ds_, dr, fs, fr, ms, mr):
    gx, gy, gz = lax.axis_index("gx"), lax.axis_index("gy"), lax.axis_index("gz")

    def at(axis, pos, n, off):
        return {axis: lax.rem(pos + (off + n), n)}

    x_lo, x_hi = at("gx", gx, n_gx, -1), at("gx", gx, n_gx, 1)
    y_lo, y_hi = at("gy", gy, n_gy, -1), at("gy", gy, n_gy, 1)
    z_lo, z_hi = at("gz", gz, n_gz, -1), at("gz", gz, n_gz, 1)

    def remote(src, dst, send, recv, dev):
        c = pltpu.make_async_remote_copy(src_ref=src, dst_ref=dst, send_sem=send, recv_sem=recv,
                                         device_id=dev, device_id_type=MESH)
        c.start()
        return c

    for i in range(CX):
        pltpu.make_async_copy(state.at[:, i], q1.at[:, rows_of(i)], lsem.at[0]).start()
    phi_load = pltpu.make_async_copy(phi_in, phi, lsem.at[1])
    phi_load.start()
    owner_load = pltpu.make_async_copy(owner_in, owner_ref, lsem.at[2])
    owner_load.start()

    def wait_for(ref, sem):
        pltpu.make_async_copy(ref, ref, sem).wait()

    n_zy = n_gz // 2

    def flat(h):
        return {"gz": (gz // n_zy) * n_zy + lax.rem(gz + h, n_zy)}

    barrier = pltpu.get_barrier_semaphore()
    peers = [x_lo, x_hi, y_lo, y_hi, z_lo, z_hi, at("gy", gy, n_gy, n_gy // 2), at("gz", gz, n_gz, n_zy)]
    for dev in peers:
        pl.semaphore_signal(barrier, inc=1, device_id=dev, device_id_type=MESH)

    def send_x_first():
        return [remote(state.at[:, pl.ds(CX - 2, 2)], xh.at[0, 0], hs.at[0, 0], hr.at[0, 0], x_hi),
                remote(state.at[:, pl.ds(0, 2)], xh.at[0, 1], hs.at[0, 0], hr.at[0, 0], x_lo)]

    def send_x_second():
        cs = []
        for j in (0, 1):
            cs.append(remote(q2.at[:, rows_of(14 + j)], xh.at[1, 0, :, j], hs.at[1, 0], hr.at[1, 0], x_hi))
            cs.append(remote(q2.at[:, rows_of(j)], xh.at[1, 1, :, j], hs.at[1, 0], hr.at[1, 0], x_lo))
        return cs

    def pack_y(q, r):
        for k in range(NF):
            for j in (0, 1):
                ysend[r, 0, k, j] = q[k, pl.ds(BASE + j, CX, stride=PITCH), :]
                ysend[r, 1, k, j] = q[k, pl.ds(BASE + 14 + j, CX, stride=PITCH), :]

    def pack_inner(q, r):
        acc = pack_z(lambda k, i: q[k, rows_of(i), :], blank(NF), range(2, CX - 2), 6)
        for k in range(NF):
            zpack[r, k] = acc[k]

    def pack_outer(q, r):
        acc = pack_z(lambda k, i: q[k, rows_of(i), :], tuple(zpack[r, k] for k in range(NF)), (0, 1, 14, 15), 1)
        for k in range(NF):
            zpack[r, k] = acc[k]
        slot = (lanes((8, CZ)) & 7) >> 1
        for g in range(NF // 2 + 1):
            parts = [acc[k][8 * h:8 * h + 8] for k in (2 * g, 2 * g + 1) if k < NF for h in (0, 1)]
            for side, lane in ((1, 2), (0, 4)):
                v = pltpu.roll(parts[0], CZ - lane, 1)
                for n in range(1, len(parts)):
                    shift = (CZ + 2 * n - lane) % CZ
                    v = jnp.where(slot == n, pltpu.roll(parts[n], shift, 1) if shift else parts[n], v)
                zsend[r, side, g] = v

    def send_y(r):
        return [remote(ysend.at[r, 1], yrecv.at[r, 0], hs.at[r, 1], hr.at[r, 1], y_hi),
                remote(ysend.at[r, 0], yrecv.at[r, 1], hs.at[r, 1], hr.at[r, 1], y_lo)]

    def send_z(r):
        return [remote(zsend.at[r, 1], zrecv.at[r, 0], hs.at[r, 2], hr.at[r, 2], z_hi),
                remote(zsend.at[r, 0], zrecv.at[r, 1], hs.at[r, 2], hr.at[r, 2], z_lo)]

    def interior(q):
        def speed_body(i):
            s = speeds(lambda k: q[k, rows_of(i), :], (1, 2, 3))
            sx[i] = s[0]
            sy[rows_of(i), :] = s[1]
            sz[i] = s[2]

        each(CX, speed_body, UN)
        lane = lanes()
        inner = (lane >= 2) & (lane < CZ - 2)

        def z_body(i):
            s = sz[i]
            f = interface_flux(lambda k: z_shifted(q[k, rows_of(i), :]), s, pltpu.roll(s, CZ - 1, 1), 3)
            for k in range(NF):
                dd[k, i] = jnp.where(inner, pltpu.roll(f[k], 1, 1) - f[k], 0.0)

        each(CX, z_body, UN)

        def x_flux(i):
            return interface_flux(lambda k: tuple(q[k, rows_of(i + o), :] for o in (-1, 0, 1, 2)), sx[i], sx[i + 1], 1)

        f = x_flux(1)
        for k in range(NF):
            fb[0, k] = f[k]

        def x_body(i, prev):
            f = x_flux(i)
            for k in range(NF):
                dd[k, i] = dd[k, i] + (prev[k] - f[k])
            return tuple(f)

        f = lax.fori_loop(2, 14, x_body, tuple(f), unroll=UN)
        for k in range(NF):
            fb[1, k] = f[k]

    def y_part(q, r):
        for k in range(NF):
            for j in (0, 1):
                q[k, pl.ds(BASE - 2 + j, CX, stride=PITCH), :] = yrecv[r, 0, k, j]
                q[k, pl.ds(BASE + CY + j, CX, stride=PITCH), :] = yrecv[r, 1, k, j]
        sy[pl.ds(BASE + CY, CX, stride=PITCH), :] = speeds(lambda k: yrecv[r, 1, k, 0], (2,))[0]
        s_l, = speeds(lambda k: yrecv[r, 0, k, 1], (2,))
        s_r, = speeds(lambda k: ysend[r, 0, k, 0], (2,))
        f = interface_flux(
            lambda k: (yrecv[r, 0, k, 0], yrecv[r, 0, k, 1], ysend[r, 0, k, 0], ysend[r, 0, k, 1]), s_l, s_r, 2)
        for k in range(NF):
            fym[k] = f[k]
        first_row = lax.broadcasted_iota(jnp.int32, (CY, CZ), 0) == 0

        def y_body(i):
            at_ = i * PITCH + BASE
            f = interface_flux(lambda k: tuple(q[k, pl.ds(at_ + o, CY), :] for o in (-1, 0, 1, 2)),
                               sy[pl.ds(at_, CY), :], sy[pl.ds(at_ + 1, CY), :], 2)
            for k in range(NF):
                lower = jnp.where(first_row, fym[k, pl.ds(i, 1), :], pltpu.roll(f[k], 1, 0))
                dd[k, i] = dd[k, i] + (lower - f[k])

        each(CX, y_body, UN)

    def z_part(r):
        low = (lanes() & 7) < 4

        def z_edge(cells):
            s, = speeds(lambda k: cells[k], (3,))
            f = interface_flux(lambda k: z_shifted(cells[k]), s, pltpu.roll(s, CZ - 1, 1), 3)
            return [pltpu.roll(f[k], 1, 1) - f[k] for k in range(NF)]

        def received(side, lane, k):
            m = zrecv[r, side, k // 2]
            shifts = [(2 * CZ + lane - 2 * (2 * (k % 2) + h)) % CZ for h in (0, 1)]
            return jnp.concatenate([pltpu.roll(m, t, 1) if t else m for t in shifts], axis=0)

        def from_left(k):
            return received(0, 2, k)

        def from_right(k):
            return received(1, 4, k)

        left = z_edge([jnp.where(low, from_left(k), zpack[r, k]) for k in range(NF)])
        for k in range(NF):
            tz[k] = left[k]
        right = z_edge([jnp.where(low, zpack[r, k], from_right(k)) for k in range(NF)])
        for k in range(NF):
            tz[k] = jnp.where(low, right[k], tz[k])

    def tendency(i, k):
        lane = lanes()
        outer = (lane < 2) | (lane >= CZ - 2)
        shift = (2 * CZ - 4 - 8 * i) % CZ if isinstance(i, int) else lax.rem(2 * CZ - 4 - 8 * i, CZ)
        return dd[k, i] + jnp.where(outer, pltpu.roll(tz[k], shift, 1), 0.0)

    def x_part(q, r, finish):
        def get(i):
            if i < 0:
                return lambda k: xh[r, 0, k, i + 2]
            if i >= CX:
                return lambda k: xh[r, 1, k, i - CX]
            return lambda k: q[k, rows_of(i), :]

        def speed(i):
            return sx[i] if 0 <= i < CX else speeds(get(i), (1,))[0]

        def flux(i):
            g = [get(i + o) for o in (-1, 0, 1, 2)]
            return interface_flux(lambda k: tuple(h(k) for h in g), speed(i), speed(i + 1), 1)

        a = flux(-1)
        b = flux(0)
        finish(0, [tendency(0, k) + (a[k] - b[k]) for k in range(NF)])
        finish(1, [tendency(1, k) + (b[k] - fb[0, k]) for k in range(NF)])
        a = flux(14)
        finish(14, [tendency(14, k) + (fb[1, k] - a[k]) for k in range(NF)])
        b = flux(15)
        finish(15, [tendency(15, k) + (a[k] - b[k]) for k in range(NF)])

    def rest(finish):
        def body(j):
            finish(2 + j, [tendency(2 + j, k) for k in range(NF)])
        each(CX - 4, body, UN)

    def finish_first(i, t):
        for k in range(NF):
            q2[k, rows_of(i), :] = q1[k, rows_of(i), :] + DTH * t[k]

    def finish_new(i, t):
        for k in range(NF):
            nst[k, i] = 0.5 * q1[k, rows_of(i), :] + 0.5 * (q2[k, rows_of(i), :] + DTH * t[k])

    pl.semaphore_wait(barrier, len(peers))
    send_x_first()
    wait_for(q1.at[:, pl.ds(0, CX * CY)], lsem.at[0])
    pack_inner(q1, 0)
    pack_outer(q1, 0)
    send_z(0)
    pack_y(q1, 0)
    send_y(0)

    phi_load.wait()
    owner_load.wait()

    def is_code(box, slot):
        return jnp.where(owner_ref[0, 0, box] == gx * SLOTS + slot, 1.0, 0.0).astype(jnp.float32)

    masks = [[[is_code(lax.rem(gx + o, n_gx) * 2 + b, s) for s in range(SLOTS)] for b in (0, 1)] for o in range(4)]

    for o in (2, 1, 3, 0):
        def phi_body(j, o=o):
            rows = [phi[s, j] for s in range(SLOTS)]
            for b in (0, 1):
                m = masks[o][b]
                v = rows[0] * m[0]
                for s in range(1, SLOTS):
                    v = v + rows[s] * m[s]
                pb[o, b, j] = v
        each(HALF, phi_body)
    interior(q1)
    wait_for(yrecv.at[0], hr.at[0, 1])
    y_part(q1, 0)
    remote(pb.at[2, 0], pfirst.at[0], ps.at[0], pr.at[0], x_hi)
    remote(pb.at[2, 1], pfirst.at[1], ps.at[0], pr.at[0], x_lo)
    wait_for(zrecv.at[0], hr.at[0, 2])
    z_part(0)
    rest(finish_first)
    pack_inner(q2, 1)
    wait_for(xh.at[0], hr.at[0, 0])
    x_part(q1, 0, finish_first)

    pack_outer(q2, 1)
    send_z(1)
    send_x_second()
    pack_y(q2, 1)
    send_y(1)

    interior(q2)
    wait_for(yrecv.at[1], hr.at[1, 1])
    y_part(q2, 1)
    remote(pb.at[1, 1], pin.at[0, 1], ps.at[1], pr.at[1], x_hi)
    remote(pb.at[3, 0], pin.at[1, 0], ps.at[1], pr.at[1], x_lo)
    wait_for(zrecv.at[1], hr.at[1, 2])
    z_part(1)
    rest(finish_new)
    wait_for(pfirst, pr.at[0])

    def add_body(j):
        pb[1, 0, j] = pb[1, 0, j] + pfirst[0, j]
        pb[3, 1, j] = pb[3, 1, j] + pfirst[1, j]

    each(HALF, add_body)
    wait_for(xh.at[1], hr.at[1, 0])
    x_part(q2, 1, finish_new)

    def mass_body(i, acc):
        return acc + nst[0, i, 0:8, :] + nst[0, i, 8:16, :]

    acc = lax.fori_loop(0, CX, mass_body, jnp.zeros((8, CZ), jnp.float32), unroll=4)
    m0[...] = jnp.sum(acc, axis=0, keepdims=True)

    def spread(src, dst, devices, t):
        for n, dev in enumerate(devices):
            remote(src, dst.at[n], ms.at[t], mr.at[t], dev)

    def gathered(own, got, t):
        wait_for(got, mr.at[t])
        acc = own[...]
        for n in range(got.shape[0]):
            acc = acc + got[n]
        return acc

    along_z = [{**at("gx", gx, n_gx, o), **at("gz", gz, n_gz, h * n_zy)}
               for o in range(n_gx) for h in (0, 1) if o + h > 0]
    spread(m0, mz, along_z, 0)

    remote(pb.at[1, 0], pin.at[0, 0], ps.at[1], pr.at[1], x_hi)
    remote(pb.at[3, 1], pin.at[1, 1], ps.at[1], pr.at[1], x_lo)

    remote(nst.at[0, pl.ds(0, HALF)], gl.at[0], ds_.at[0], dr.at[0], x_hi)
    remote(nst.at[0, pl.ds(HALF, HALF)], gr.at[1], ds_.at[0], dr.at[1], x_lo)
    remote(nst.at[0, pl.ds(HALF, HALF)], gl.at[1], ds_.at[0], dr.at[2], x_hi)
    remote(nst.at[0, pl.ds(0, HALF)], gr.at[0], ds_.at[0], dr.at[4], x_lo)

    m1[...] = gathered(m0, mz, 0)
    spread(m1, mx, [at("gy", gy, n_gy, o) for o in range(1, n_gy)], 1)

    wait_for(pin, pr.at[1])

    def pot_body(j):
        for b in (0, 1):
            pot[b * HALF + j] = pb[0, b, j] + (pin[0, b, j] + pin[1, b, j])

    each(HALF, pot_body)
    def row_body(i):
        pys[0, pl.ds(i, 1), :] = pot[i, 0:1, :]
        pys[1, pl.ds(i, 1), :] = pot[i, CY - 1:CY, :]

    each(CX, row_body)
    pzs[0] = pack_z(lambda k, i: pot[i], blank(1), range(0, CX), 4)[0]
    remote(pot.at[CX - 1], pxr.at[0], fs.at[0], fr.at[0], x_hi)
    remote(pot.at[0], pxr.at[1], fs.at[0], fr.at[0], x_lo)
    remote(pys.at[1], pyr.at[0], fs.at[1], fr.at[1], y_hi)
    remote(pys.at[0], pyr.at[1], fs.at[1], fr.at[1], y_lo)
    remote(pzs.at[0], pzr.at[0], fs.at[2], fr.at[2], z_hi)
    remote(pzs.at[0], pzr.at[1], fs.at[2], fr.at[2], z_lo)

    wait_for(gl.at[0], dr.at[0])
    remote(gl.at[0], go.at[0], ds_.at[1], dr.at[3], x_hi)
    wait_for(gr.at[1], dr.at[1])
    remote(gr.at[1], go.at[1], ds_.at[1], dr.at[3], x_lo)

    m2[...] = gathered(m1, mx, 1)
    spread(m2, my, [flat(h) for h in range(1, n_zy)], 2)

    wait_for(gl.at[1], dr.at[2])
    wait_for(gr.at[0], dr.at[4])

    def is_box(o, b, s):
        return is_code(lax.rem(gx + o, n_gx) * 2 + b, s)

    near = [[(is_box(o, b, s)) for o in (0, 3, 1) for b in (0, 1)] for s in range(SLOTS)]

    def near_body(j):
        boxes = [nst[0, j], nst[0, HALF + j], gl[0, j], gl[1, j], gr[0, j], gr[1, j]]
        for s in range(SLOTS):
            v = boxes[0] * near[s][0]
            for t in range(1, 6):
                v = v + boxes[t] * near[s][t]
            dsol[s, j] = v
    each(HALF, near_body)
    total = gathered(m2, my, 2)
    cells = float(CX * CY * CZ * n_gx * n_gy * n_gz)
    mean = jnp.sum(total) / cells

    for n, ref in enumerate((pxr, pyr, pzr)):
        wait_for(ref, fr.at[n])
    lane = lanes()
    row = lax.broadcasted_iota(jnp.int32, (CY, CZ), 0)
    halo = jnp.where((lane & 7) < 4, pzr[0, :, :], pzr[1, :, :])

    def lap(i, below, above):
        p = pot[i]
        h = pltpu.roll(halo, lax.rem(CZ - 4 - 8 * i + CZ, CZ), 1)
        z = pltpu.roll(jnp.where(lane == CZ - 1, h, p), 1, 1) + pltpu.roll(jnp.where(lane == 0, h, p), CZ - 1, 1)
        up = jnp.where(row == 0, pyr[0, pl.ds(i, 1), :], pltpu.roll(p, 1, 0))
        dn = jnp.where(row == CY - 1, pyr[1, pl.ds(i, 1), :], pltpu.roll(p, CY - 1, 0))
        res[i] = FOURPIG * (nst[0, i] - mean) - (((below + above) + (up + dn) + z) - 6.0 * p)

    lap(0, pxr[0], pot[1])

    def lap_body(j):
        lap(j + 1, pot[j], pot[j + 2])
    each(CX - 2, lap_body, 7)
    lap(CX - 1, pot[CX - 2], pxr[1])

    far = [[is_box(2, b, s) for b in (0, 1)] for s in range(SLOTS)]
    wait_for(go, dr.at[3])

    def far_body(j):
        boxes = [go[0, j], go[1, j]]
        for s in range(SLOTS):
            dsol[s, j] = dsol[s, j] + (boxes[0] * far[s][0] + boxes[1] * far[s][1])
    each(HALF, far_body)

    for r in (0, 1):
        for n, ref in enumerate((xh, yrecv, zrecv)):
            wait_for(ref.at[r], hs.at[r, n])
    for ref, sem in ((pfirst, ps.at[0]), (pin, ps.at[1]), (pin, ds_.at[0]), (go, ds_.at[1]), (mz, ms.at[0]), (mx, ms.at[1]), (my, ms.at[2]),
                     (pxr, fs.at[0]), (pyr, fs.at[1]), (pzr, fs.at[2])):
        wait_for(ref, sem)


def solution(mesh):
    n_gx, n_gy, n_gz = mesh.shape["gx"], mesh.shape["gy"], mesh.shape["gz"]

    def on_device(state, solver_owner, phi_prev):
        f32 = jnp.float32
        V = lambda *s: pltpu.VMEM(s, f32)
        D = lambda *s: pltpu.SemaphoreType.DMA(s)
        hbm = pl.BlockSpec(memory_space=pltpu.HBM)
        vmem = pl.BlockSpec(memory_space=pltpu.VMEM)
        outs = pl.pallas_call(
            functools.partial(kernel, n_gx, n_gy, n_gz),
            out_shape=(
                jax.ShapeDtypeStruct(state.shape, f32),
                jax.ShapeDtypeStruct(phi_prev.shape, f32),
                jax.ShapeDtypeStruct(state.shape[1:], f32),
            ),
            in_specs=[hbm, hbm, hbm],
            out_specs=(vmem, vmem, vmem),
            scratch_shapes=[
                pltpu.SMEM((1, 1, 8), jnp.int32),
                V(NF, ROWS, CZ), V(NF, ROWS, CZ), V(SLOTS, HALF, CY, CZ),
                V(CX, CY, CZ), V(ROWS, CZ), V(CX, CY, CZ), V(NF, CX, CY, CZ),
                V(2, NF, CY, CZ), V(NF, CX, CZ), V(NF, CY, CZ),
                V(2, 2, NF, 2, CY, CZ), V(2, 2, NF, 2, CX, CZ), V(2, 2, NF, 2, CX, CZ),
                V(2, NF, CY, CZ), V(2, 2, NF // 2 + 1, 8, CZ), V(2, 2, NF // 2 + 1, 8, CZ),
                V(4, 2, HALF, CY, CZ), V(CX, CY, CZ), V(2, 2, HALF, CY, CZ), V(2, HALF, CY, CZ),
                V(2, HALF, CY, CZ), V(2, HALF, CY, CZ), V(2, HALF, CY, CZ),
                V(2, CY, CZ), V(2, CX, CZ), V(2, CX, CZ), V(1, CY, CZ), V(2, CY, CZ),
                V(1, CZ), V(1, CZ), V(1, CZ),
                V(n_gy - 1, 1, CZ), V(n_gz // 2 - 1, 1, CZ), V(2 * n_gx - 1, 1, CZ),
                D(3), D(2, 3), D(2, 3), D(2), D(2), D(2), D(5), D(3), D(3), D(3), D(3),
            ],
            compiler_params=pltpu.CompilerParams(
                collective_id=0, has_side_effects=True, vmem_limit_bytes=32 * 1024 * 1024
            ),
            name="gas_step",
        )(
            pltpu.with_memory_space_constraint(solver_owner, pltpu.HBM),
            pltpu.with_memory_space_constraint(state, pltpu.HBM),
            pltpu.with_memory_space_constraint(phi_prev, pltpu.HBM),
        )
        return pl.pallas_call(
            move_out,
            out_shape=tuple(jax.ShapeDtypeStruct(o.shape, f32) for o in outs),
            in_specs=[vmem] * 3,
            out_specs=(hbm,) * 3,
            scratch_shapes=[D(3)],
            compiler_params=pltpu.CompilerParams(has_side_effects=True, vmem_limit_bytes=4 * 1024 * 1024),
            name="move_out",
        )(*outs)

    return jax.shard_map(
        on_device,
        mesh=mesh,
        in_specs=(P(None, "gx", "gy", "gz"), P("gy", "gz", None), P("gx", None, "gy", "gz")),
        out_specs=(P(None, "gx", "gy", "gz"), P("gx", None, "gy", "gz"), P("gx", "gy", "gz")),
        check_vma=False,
    )
```

```python
import functools

import jax
import jax.numpy as jnp
from jax import lax
from jax.experimental import pallas as pl
from jax.experimental.pallas import tpu as pltpu
from jax.sharding import PartitionSpec as P

MESH = pl.DeviceIdType.MESH
GAMMA = 5.0 / 3.0
DTH = 0.04
FOURPIG = 2.0
NF = 7
CX, CY, CZ = 16, 16, 128
PITCH, BASE = 24, 8
ROWS = CX * PITCH + 8
HALF = 8
SLOTS = 4
UN = 2


def pressure(q5):
    return (GAMMA - 1.0) * jnp.maximum(q5, 0.1)


def speeds(get, dirs):
    inv = 1.0 / jnp.maximum(get(0), 0.25)
    sound = jnp.sqrt(GAMMA * pressure(get(5)) * inv)
    return [jnp.abs(get(d)) * inv + sound for d in dirs]


def interface_flux(get, speed_l, speed_r, d):
    def edge(k):
        a, b, c, e = get(k)
        v = 7.0 / 12.0 * (b + c) - 1.0 / 12.0 * (a + e)
        v = jnp.minimum(jnp.maximum(v, jnp.minimum(b, c)), jnp.maximum(b, c))
        return v, c - b

    half = 0.5 * jnp.maximum(speed_l, speed_r)
    e0, j0 = edge(0)
    ed, jd = edge(d)
    e5, j5 = edge(5)
    vel = ed / jnp.maximum(e0, 0.25)
    press = pressure(e5)
    out = [ed - half * j0]
    for k in (1, 2, 3):
        if k == d:
            out.append(ed * vel + press - half * jd)
        else:
            ek, jk = edge(k)
            out.append(ek * vel - half * jk)
    e4, j4 = edge(4)
    out.append((e4 + press) * vel - half * j4)
    out.append(e5 * vel - half * j5)
    e6, j6 = edge(6)
    out.append(e6 * vel - half * j6)
    return out


def lanes(shape=(CY, CZ)):
    return lax.broadcasted_iota(jnp.int32, shape, 1)


def rows_of(i):
    start = i * PITCH + BASE
    if not isinstance(i, int):
        start = pl.multiple_of(start, 8)
    return pl.ds(start, CY)


def z_shifted(q):
    return (pltpu.roll(q, 1, 1), q, pltpu.roll(q, CZ - 1, 1), pltpu.roll(q, CZ - 2, 1))


def each(n, body, unroll=1):
    def step(i, c):
        body(i)
        return c

    lax.fori_loop(0, n, step, 0, unroll=unroll)


def pack_z(load, acc, slabs, unroll):
    lane = lanes()

    def put(i, acc, shift):
        here = (lane >= 8 * i) & (lane < 8 * i + 8)
        return tuple(jnp.where(here, pltpu.roll(load(k, i), shift, 1), a) for k, a in enumerate(acc))

    if isinstance(slabs, tuple):
        for i in slabs:
            acc = put(i, acc, (8 * i + 4) % CZ)
        return acc
    return lax.fori_loop(slabs.start, slabs.stop, lambda i, a: put(i, a, lax.rem(8 * i + 4, CZ)), acc, unroll=unroll)


def blank(count):
    return tuple(jnp.zeros((CY, CZ), jnp.float32) for _ in range(count))


def move_out(*refs):
    n = (len(refs) - 1) // 2
    sem = refs[-1]
    for i in range(n):
        for p in range(refs[i].shape[0]):
            pltpu.make_async_copy(refs[i].at[p], refs[n + i].at[p], sem.at[i]).start()
    for i in range(n):
        pltpu.make_async_copy(refs[i], refs[n + i], sem.at[i]).wait()


def kernel(n_gx, n_gy, n_gz, owner_in, state, phi_in, nst, dsol, res,
           owner_ref, q1, q2, phi, sx, sy, sz, dd, fb, fym, tz,
           xh, ysend, yrecv, zpack, zsend, zrecv,
           pb, pot, pin, pfirst, gl, gr, go,
           pxr, pys, pyr, pzs, pzr,
           m0, m1, m2, mx, my, mz,
           lsem, hs, hr, ps, pr, ds_, dr, fs, fr, ms, mr):
    gx, gy, gz = lax.axis_index("gx"), lax.axis_index("gy"), lax.axis_index("gz")

    def at(axis, pos, n, off):
        return {axis: lax.rem(pos + (off + n), n)}

    x_lo, x_hi = at("gx", gx, n_gx, -1), at("gx", gx, n_gx, 1)
    y_lo, y_hi = at("gy", gy, n_gy, -1), at("gy", gy, n_gy, 1)
    z_lo, z_hi = at("gz", gz, n_gz, -1), at("gz", gz, n_gz, 1)

    def remote(src, dst, send, recv, dev):
        c = pltpu.make_async_remote_copy(src_ref=src, dst_ref=dst, send_sem=send, recv_sem=recv,
                                         device_id=dev, device_id_type=MESH)
        c.start()
        return c

    n_zy = n_gz // 2

    def flat(h):
        return {"gz": (gz // n_zy) * n_zy + lax.rem(gz + h, n_zy)}

    barrier = pltpu.get_barrier_semaphore()
    peers = [x_lo, x_hi, y_lo, y_hi, z_lo, z_hi, at("gy", gy, n_gy, n_gy // 2), at("gz", gz, n_gz, n_zy)]
    for dev in peers:
        pl.semaphore_signal(barrier, inc=1, device_id=dev, device_id_type=MESH)

    for i in range(CX):
        pltpu.make_async_copy(state.at[:, i], q1.at[:, rows_of(i)], lsem.at[0]).start()
    phi_load = pltpu.make_async_copy(phi_in, phi, lsem.at[1])
    phi_load.start()
    owner_load = pltpu.make_async_copy(owner_in, owner_ref, lsem.at[2])
    owner_load.start()

    def wait_for(ref, sem):
        pltpu.make_async_copy(ref, ref, sem).wait()

    def send_x_first():
        return [remote(state.at[:, pl.ds(CX - 2, 2)], xh.at[0, 0], hs.at[0, 0], hr.at[0, 0], x_hi),
                remote(state.at[:, pl.ds(0, 2)], xh.at[0, 1], hs.at[0, 0], hr.at[0, 0], x_lo)]

    def send_x_second():
        cs = []
        for j in (0, 1):
            cs.append(remote(q2.at[:, rows_of(14 + j)], xh.at[1, 0, :, j], hs.at[1, 0], hr.at[1, 0], x_hi))
            cs.append(remote(q2.at[:, rows_of(j)], xh.at[1, 1, :, j], hs.at[1, 0], hr.at[1, 0], x_lo))
        return cs

    def pack_y(q, r):
        for k in range(NF):
            for j in (0, 1):
                ysend[r, 0, k, j] = q[k, pl.ds(BASE + j, CX, stride=PITCH), :]
                ysend[r, 1, k, j] = q[k, pl.ds(BASE + 14 + j, CX, stride=PITCH), :]

    def pack_inner(q, r):
        acc = pack_z(lambda k, i: q[k, rows_of(i), :], blank(NF), range(2, CX - 2), 6)
        for k in range(NF):
            zpack[r, k] = acc[k]

    def pack_outer(q, r):
        acc = pack_z(lambda k, i: q[k, rows_of(i), :], tuple(zpack[r, k] for k in range(NF)), (0, 1, 14, 15), 1)
        for k in range(NF):
            zpack[r, k] = acc[k]
        slot = (lanes((8, CZ)) & 7) >> 1
        for g in range(NF // 2 + 1):
            parts = [acc[k][8 * h:8 * h + 8] for k in (2 * g, 2 * g + 1) if k < NF for h in (0, 1)]
            for side, lane in ((1, 2), (0, 4)):
                v = pltpu.roll(parts[0], CZ - lane, 1)
                for n in range(1, len(parts)):
                    shift = (CZ + 2 * n - lane) % CZ
                    v = jnp.where(slot == n, pltpu.roll(parts[n], shift, 1) if shift else parts[n], v)
                zsend[r, side, g] = v

    def send_y(r):
        return [remote(ysend.at[r, 1], yrecv.at[r, 0], hs.at[r, 1], hr.at[r, 1], y_hi),
                remote(ysend.at[r, 0], yrecv.at[r, 1], hs.at[r, 1], hr.at[r, 1], y_lo)]

    def send_z(r):
        return [remote(zsend.at[r, 1], zrecv.at[r, 0], hs.at[r, 2], hr.at[r, 2], z_hi),
                remote(zsend.at[r, 0], zrecv.at[r, 1], hs.at[r, 2], hr.at[r, 2], z_lo)]

    def interior(q):
        def speed_body(i):
            s = speeds(lambda k: q[k, rows_of(i), :], (1, 2, 3))
            sx[i] = s[0]
            sy[rows_of(i), :] = s[1]
            sz[i] = s[2]

        each(CX, speed_body, UN)
        lane = lanes()
        inner = (lane >= 2) & (lane < CZ - 2)

        def z_body(i):
            s = sz[i]
            f = interface_flux(lambda k: z_shifted(q[k, rows_of(i), :]), s, pltpu.roll(s, CZ - 1, 1), 3)
            for k in range(NF):
                dd[k, i] = jnp.where(inner, pltpu.roll(f[k], 1, 1) - f[k], 0.0)

        each(CX, z_body, UN)

        def x_flux(i):
            return interface_flux(lambda k: tuple(q[k, rows_of(i + o), :] for o in (-1, 0, 1, 2)), sx[i], sx[i + 1], 1)

        f = x_flux(1)
        for k in range(NF):
            fb[0, k] = f[k]

        def x_body(i, prev):
            f = x_flux(i)
            for k in range(NF):
                dd[k, i] = dd[k, i] + (prev[k] - f[k])
            return tuple(f)

        f = lax.fori_loop(2, 14, x_body, tuple(f), unroll=UN)
        for k in range(NF):
            fb[1, k] = f[k]

    def y_part(q, r, finish):
        for k in range(NF):
            for j in (0, 1):
                q[k, pl.ds(BASE - 2 + j, CX, stride=PITCH), :] = yrecv[r, 0, k, j]
                q[k, pl.ds(BASE + CY + j, CX, stride=PITCH), :] = yrecv[r, 1, k, j]
        sy[pl.ds(BASE + CY, CX, stride=PITCH), :] = speeds(lambda k: yrecv[r, 1, k, 0], (2,))[0]
        s_l, = speeds(lambda k: yrecv[r, 0, k, 1], (2,))
        s_r, = speeds(lambda k: ysend[r, 0, k, 0], (2,))
        f = interface_flux(
            lambda k: (yrecv[r, 0, k, 0], yrecv[r, 0, k, 1], ysend[r, 0, k, 0], ysend[r, 0, k, 1]), s_l, s_r, 2)
        for k in range(NF):
            fym[k] = f[k]
        first_row = lax.broadcasted_iota(jnp.int32, (CY, CZ), 0) == 0

        def y_tendency(i):
            at_ = i * PITCH + BASE
            f = interface_flux(lambda k: tuple(q[k, pl.ds(at_ + o, CY), :] for o in (-1, 0, 1, 2)),
                               sy[pl.ds(at_, CY), :], sy[pl.ds(at_ + 1, CY), :], 2)
            for k in range(NF):
                lower = jnp.where(first_row, fym[k, pl.ds(i, 1), :], pltpu.roll(f[k], 1, 0))
                f[k] = dd[k, i] + (lower - f[k])
            return f

        def outer_body(j):
            i = jnp.where(j < 2, j, j + 12)
            t = y_tendency(i)
            for k in range(NF):
                dd[k, i] = t[k]

        each(4, outer_body, UN)

        def inner_body(j):
            finish(j + 2, y_tendency(j + 2))

        each(CX - 4, inner_body, UN)

    def z_part(r):
        low = (lanes() & 7) < 4

        def z_edge(cells):
            s, = speeds(lambda k: cells[k], (3,))
            f = interface_flux(lambda k: z_shifted(cells[k]), s, pltpu.roll(s, CZ - 1, 1), 3)
            return [pltpu.roll(f[k], 1, 1) - f[k] for k in range(NF)]

        def received(side, lane, k):
            m = zrecv[r, side, k // 2]
            shifts = [(2 * CZ + lane - 2 * (2 * (k % 2) + h)) % CZ for h in (0, 1)]
            return jnp.concatenate([pltpu.roll(m, t, 1) if t else m for t in shifts], axis=0)

        def from_left(k):
            return received(0, 2, k)

        def from_right(k):
            return received(1, 4, k)

        left = z_edge([jnp.where(low, from_left(k), zpack[r, k]) for k in range(NF)])
        for k in range(NF):
            tz[k] = left[k]
        right = z_edge([jnp.where(low, zpack[r, k], from_right(k)) for k in range(NF)])
        for k in range(NF):
            tz[k] = jnp.where(low, right[k], tz[k])

    def edge_tendency(i, k):
        lane = lanes()
        outer = (lane < 2) | (lane >= CZ - 2)
        shift = (2 * CZ - 4 - 8 * i) % CZ if isinstance(i, int) else lax.rem(2 * CZ - 4 - 8 * i, CZ)
        return jnp.where(outer, pltpu.roll(tz[k], shift, 1), 0.0)

    def tendency(i, k):
        return dd[k, i] + edge_tendency(i, k)

    def x_part(q, r, finish):
        def get(i):
            if i < 0:
                return lambda k: xh[r, 0, k, i + 2]
            if i >= CX:
                return lambda k: xh[r, 1, k, i - CX]
            return lambda k: q[k, rows_of(i), :]

        def speed(i):
            return sx[i] if 0 <= i < CX else speeds(get(i), (1,))[0]

        def flux(i):
            g = [get(i + o) for o in (-1, 0, 1, 2)]
            return interface_flux(lambda k: tuple(h(k) for h in g), speed(i), speed(i + 1), 1)

        a = flux(-1)
        b = flux(0)
        finish(0, [tendency(0, k) + (a[k] - b[k]) for k in range(NF)])
        finish(1, [tendency(1, k) + (b[k] - fb[0, k]) for k in range(NF)])
        a = flux(14)
        finish(14, [tendency(14, k) + (fb[1, k] - a[k]) for k in range(NF)])
        b = flux(15)
        finish(15, [tendency(15, k) + (a[k] - b[k]) for k in range(NF)])

    def edges(scale, view, fields):
        def body(j):
            for k in fields:
                ref, idx = view(j + 2, k)
                ref[idx] = ref[idx] + scale * edge_tendency(j + 2, k)
        each(CX - 4, body, UN)

    def edges_packed(r, scale):
        lane = lanes()
        here = (lane >= 16) & (lane < CZ - 16) & ((lane & 7) >= 2) & ((lane & 7) < 6)
        for k in range(NF):
            zpack[r, k] = zpack[r, k] + jnp.where(here, scale * tz[k], 0.0)

    def finish_first(i, t):
        for k in range(NF):
            q2[k, rows_of(i), :] = q1[k, rows_of(i), :] + DTH * t[k]

    def finish_new(i, t):
        for k in range(NF):
            nst[k, i] = 0.5 * q1[k, rows_of(i), :] + 0.5 * (q2[k, rows_of(i), :] + DTH * t[k])

    pl.semaphore_wait(barrier, len(peers))
    send_x_first()
    wait_for(q1.at[:, pl.ds(0, CX * CY)], lsem.at[0])
    pack_inner(q1, 0)
    pack_outer(q1, 0)
    send_z(0)
    pack_y(q1, 0)
    send_y(0)

    phi_load.wait()
    owner_load.wait()

    def is_code(box, slot):
        return jnp.where(owner_ref[0, 0, box] == gx * SLOTS + slot, 1.0, 0.0).astype(jnp.float32)

    masks = [[[is_code(lax.rem(gx + o, n_gx) * 2 + b, s) for s in range(SLOTS)] for b in (0, 1)] for o in range(4)]

    for o in (2, 1, 3, 0):
        def phi_body(j, o=o):
            rows = [phi[s, j] for s in range(SLOTS)]
            for b in (0, 1):
                m = masks[o][b]
                v = rows[0] * m[0]
                for s in range(1, SLOTS):
                    v = v + rows[s] * m[s]
                pb[o, b, j] = v
        each(HALF, phi_body)
    interior(q1)
    wait_for(yrecv.at[0], hr.at[0, 1])
    y_part(q1, 0, finish_first)
    remote(pb.at[2, 0], pfirst.at[0], ps.at[0], pr.at[0], x_hi)
    remote(pb.at[2, 1], pfirst.at[1], ps.at[0], pr.at[0], x_lo)
    pack_inner(q2, 1)
    wait_for(zrecv.at[0], hr.at[0, 2])
    z_part(0)
    edges_packed(1, DTH)
    wait_for(xh.at[0], hr.at[0, 0])
    x_part(q1, 0, finish_first)

    pack_outer(q2, 1)
    send_z(1)
    send_x_second()
    edges(DTH, lambda i, k: (q2, (k, rows_of(i), slice(None))), range(NF))
    pack_y(q2, 1)
    send_y(1)

    interior(q2)
    wait_for(yrecv.at[1], hr.at[1, 1])
    y_part(q2, 1, finish_new)
    remote(pb.at[1, 1], pin.at[0, 1], ps.at[1], pr.at[1], x_hi)
    remote(pb.at[3, 0], pin.at[1, 0], ps.at[1], pr.at[1], x_lo)
    wait_for(pfirst, pr.at[0])

    def add_body(j):
        pb[1, 0, j] = pb[1, 0, j] + pfirst[0, j]
        pb[3, 1, j] = pb[3, 1, j] + pfirst[1, j]

    each(HALF, add_body)
    wait_for(zrecv.at[1], hr.at[1, 2])
    z_part(1)
    edges(0.5 * DTH, lambda i, k: (nst, (k, i)), (0,))
    wait_for(xh.at[1], hr.at[1, 0])
    x_part(q2, 1, finish_new)

    def mass_body(i, acc):
        return acc + nst[0, i, 0:8, :] + nst[0, i, 8:16, :]

    acc = lax.fori_loop(0, CX, mass_body, jnp.zeros((8, CZ), jnp.float32), unroll=4)
    m0[...] = jnp.sum(acc, axis=0, keepdims=True)

    def spread(src, dst, devices, t):
        for n, dev in enumerate(devices):
            remote(src, dst.at[n], ms.at[t], mr.at[t], dev)

    def gathered(own, got, t):
        wait_for(got, mr.at[t])
        acc = own[...]
        for n in range(got.shape[0]):
            acc = acc + got[n]
        return acc

    along_z = [{**at("gx", gx, n_gx, o), **at("gz", gz, n_gz, h * n_zy)}
               for o in range(n_gx) for h in (0, 1) if o + h > 0]
    spread(m0, mz, along_z, 0)
    remote(pb.at[1, 0], pin.at[0, 0], ps.at[1], pr.at[1], x_hi)
    remote(pb.at[3, 1], pin.at[1, 1], ps.at[1], pr.at[1], x_lo)

    remote(nst.at[0, pl.ds(0, HALF)], gl.at[0], ds_.at[0], dr.at[0], x_hi)
    remote(nst.at[0, pl.ds(HALF, HALF)], gr.at[1], ds_.at[0], dr.at[1], x_lo)
    remote(nst.at[0, pl.ds(HALF, HALF)], gl.at[1], ds_.at[0], dr.at[2], x_hi)
    remote(nst.at[0, pl.ds(0, HALF)], gr.at[0], ds_.at[0], dr.at[4], x_lo)
    edges(0.5 * DTH, lambda i, k: (nst, (k, i)), range(1, NF))

    m1[...] = gathered(m0, mz, 0)
    spread(m1, mx, [at("gy", gy, n_gy, o) for o in range(1, n_gy)], 1)

    wait_for(pin, pr.at[1])

    def pot_body(j):
        for b in (0, 1):
            pot[b * HALF + j] = pb[0, b, j] + (pin[0, b, j] + pin[1, b, j])

    each(HALF, pot_body)
    def row_body(i):
        pys[0, pl.ds(i, 1), :] = pot[i, 0:1, :]
        pys[1, pl.ds(i, 1), :] = pot[i, CY - 1:CY, :]

    each(CX, row_body)
    pzs[0] = pack_z(lambda k, i: pot[i], blank(1), range(0, CX), 4)[0]
    remote(pot.at[CX - 1], pxr.at[0], fs.at[0], fr.at[0], x_hi)
    remote(pot.at[0], pxr.at[1], fs.at[0], fr.at[0], x_lo)
    remote(pys.at[1], pyr.at[0], fs.at[1], fr.at[1], y_hi)
    remote(pys.at[0], pyr.at[1], fs.at[1], fr.at[1], y_lo)
    remote(pzs.at[0], pzr.at[0], fs.at[2], fr.at[2], z_hi)
    remote(pzs.at[0], pzr.at[1], fs.at[2], fr.at[2], z_lo)

    wait_for(gl.at[0], dr.at[0])
    remote(gl.at[0], go.at[0], ds_.at[1], dr.at[3], x_hi)
    wait_for(gr.at[1], dr.at[1])
    remote(gr.at[1], go.at[1], ds_.at[1], dr.at[3], x_lo)

    m2[...] = gathered(m1, mx, 1)
    spread(m2, my, [flat(h) for h in range(1, n_zy)], 2)

    wait_for(gl.at[1], dr.at[2])
    wait_for(gr.at[0], dr.at[4])

    def is_box(o, b, s):
        return is_code(lax.rem(gx + o, n_gx) * 2 + b, s)

    near = [[(is_box(o, b, s)) for o in (0, 3, 1) for b in (0, 1)] for s in range(SLOTS)]

    def near_body(j):
        boxes = [nst[0, j], nst[0, HALF + j], gl[0, j], gl[1, j], gr[0, j], gr[1, j]]
        for s in range(SLOTS):
            v = boxes[0] * near[s][0]
            for t in range(1, 6):
                v = v + boxes[t] * near[s][t]
            dsol[s, j] = v
    each(HALF, near_body)
    total = gathered(m2, my, 2)
    cells = float(CX * CY * CZ * n_gx * n_gy * n_gz)
    mean = jnp.sum(total) / cells

    for n, ref in enumerate((pxr, pyr, pzr)):
        wait_for(ref, fr.at[n])
    lane = lanes()
    row = lax.broadcasted_iota(jnp.int32, (CY, CZ), 0)
    halo = jnp.where((lane & 7) < 4, pzr[0, :, :], pzr[1, :, :])

    def lap(i, below, above):
        p = pot[i]
        h = pltpu.roll(halo, lax.rem(CZ - 4 - 8 * i + CZ, CZ), 1)
        z = pltpu.roll(jnp.where(lane == CZ - 1, h, p), 1, 1) + pltpu.roll(jnp.where(lane == 0, h, p), CZ - 1, 1)
        up = jnp.where(row == 0, pyr[0, pl.ds(i, 1), :], pltpu.roll(p, 1, 0))
        dn = jnp.where(row == CY - 1, pyr[1, pl.ds(i, 1), :], pltpu.roll(p, CY - 1, 0))
        res[i] = FOURPIG * (nst[0, i] - mean) - (((below + above) + (up + dn) + z) - 6.0 * p)

    lap(0, pxr[0], pot[1])

    def lap_body(j):
        lap(j + 1, pot[j], pot[j + 2])
    each(CX - 2, lap_body, 7)
    lap(CX - 1, pot[CX - 2], pxr[1])

    far = [[is_box(2, b, s) for b in (0, 1)] for s in range(SLOTS)]
    wait_for(go, dr.at[3])

    def far_body(j):
        boxes = [go[0, j], go[1, j]]
        for s in range(SLOTS):
            dsol[s, j] = dsol[s, j] + (boxes[0] * far[s][0] + boxes[1] * far[s][1])
    each(HALF, far_body)

    for r in (0, 1):
        for n, ref in enumerate((xh, yrecv, zrecv)):
            wait_for(ref.at[r], hs.at[r, n])
    for ref, sem in ((pfirst, ps.at[0]), (pin, ps.at[1]), (pin, ds_.at[0]), (go, ds_.at[1]), (mz, ms.at[0]), (mx, ms.at[1]), (my, ms.at[2]),
                     (pxr, fs.at[0]), (pyr, fs.at[1]), (pzr, fs.at[2])):
        wait_for(ref, sem)


def solution(mesh):
    n_gx, n_gy, n_gz = mesh.shape["gx"], mesh.shape["gy"], mesh.shape["gz"]

    def on_device(state, solver_owner, phi_prev):
        f32 = jnp.float32
        V = lambda *s: pltpu.VMEM(s, f32)
        D = lambda *s: pltpu.SemaphoreType.DMA(s)
        hbm = pl.BlockSpec(memory_space=pltpu.HBM)
        vmem = pl.BlockSpec(memory_space=pltpu.VMEM)
        outs = pl.pallas_call(
            functools.partial(kernel, n_gx, n_gy, n_gz),
            out_shape=(
                jax.ShapeDtypeStruct(state.shape, f32),
                jax.ShapeDtypeStruct(phi_prev.shape, f32),
                jax.ShapeDtypeStruct(state.shape[1:], f32),
            ),
            in_specs=[hbm, hbm, hbm],
            out_specs=(vmem, vmem, vmem),
            scratch_shapes=[
                pltpu.SMEM((1, 1, 8), jnp.int32),
                V(NF, ROWS, CZ), V(NF, ROWS, CZ), V(SLOTS, HALF, CY, CZ),
                V(CX, CY, CZ), V(ROWS, CZ), V(CX, CY, CZ), V(NF, CX, CY, CZ),
                V(2, NF, CY, CZ), V(NF, CX, CZ), V(NF, CY, CZ),
                V(2, 2, NF, 2, CY, CZ), V(2, 2, NF, 2, CX, CZ), V(2, 2, NF, 2, CX, CZ),
                V(2, NF, CY, CZ), V(2, 2, NF // 2 + 1, 8, CZ), V(2, 2, NF // 2 + 1, 8, CZ),
                V(4, 2, HALF, CY, CZ), V(CX, CY, CZ), V(2, 2, HALF, CY, CZ), V(2, HALF, CY, CZ),
                V(2, HALF, CY, CZ), V(2, HALF, CY, CZ), V(2, HALF, CY, CZ),
                V(2, CY, CZ), V(2, CX, CZ), V(2, CX, CZ), V(1, CY, CZ), V(2, CY, CZ),
                V(1, CZ), V(1, CZ), V(1, CZ),
                V(n_gy - 1, 1, CZ), V(n_gz // 2 - 1, 1, CZ), V(2 * n_gx - 1, 1, CZ),
                D(3), D(2, 3), D(2, 3), D(2), D(2), D(2), D(5), D(3), D(3), D(3), D(3),
            ],
            compiler_params=pltpu.CompilerParams(
                collective_id=0, has_side_effects=True, vmem_limit_bytes=32 * 1024 * 1024
            ),
            name="gas_step",
        )(
            pltpu.with_memory_space_constraint(solver_owner, pltpu.HBM),
            pltpu.with_memory_space_constraint(state, pltpu.HBM),
            pltpu.with_memory_space_constraint(phi_prev, pltpu.HBM),
        )
        return pl.pallas_call(
            move_out,
            out_shape=tuple(jax.ShapeDtypeStruct(o.shape, f32) for o in outs),
            in_specs=[vmem] * 3,
            out_specs=(hbm,) * 3,
            scratch_shapes=[D(3)],
            compiler_params=pltpu.CompilerParams(has_side_effects=True, vmem_limit_bytes=4 * 1024 * 1024),
            name="move_out",
        )(*outs)

    return jax.shard_map(
        on_device,
        mesh=mesh,
        in_specs=(P(None, "gx", "gy", "gz"), P("gy", "gz", None), P("gx", None, "gy", "gz")),
        out_specs=(P(None, "gx", "gy", "gz"), P("gx", None, "gy", "gz"), P("gx", "gy", "gz")),
        check_vma=False,
    )
```

```python
import functools

import jax
import jax.numpy as jnp
from jax import lax
from jax.experimental import pallas as pl
from jax.experimental.pallas import tpu as pltpu
from jax.sharding import PartitionSpec as P

MESH = pl.DeviceIdType.MESH
GAMMA = 5.0 / 3.0
DTH = 0.04
FOURPIG = 2.0
NF = 7
CX, CY, CZ = 16, 16, 128
PITCH, BASE = 24, 8
ROWS = CX * PITCH + 8
HALF = 8
SLOTS = 4
UN = 2


def pressure(q5):
    return (GAMMA - 1.0) * jnp.maximum(q5, 0.1)


def speeds(get, dirs):
    inv = 1.0 / jnp.maximum(get(0), 0.25)
    sound = jnp.sqrt(GAMMA * pressure(get(5)) * inv)
    return [jnp.abs(get(d)) * inv + sound for d in dirs]


def interface_flux(get, speed_l, speed_r, d):
    def edge(k):
        a, b, c, e = get(k)
        v = 7.0 / 12.0 * (b + c) - 1.0 / 12.0 * (a + e)
        v = jnp.minimum(jnp.maximum(v, jnp.minimum(b, c)), jnp.maximum(b, c))
        return v, c - b

    half = 0.5 * jnp.maximum(speed_l, speed_r)
    e0, j0 = edge(0)
    ed, jd = edge(d)
    e5, j5 = edge(5)
    vel = ed / jnp.maximum(e0, 0.25)
    press = pressure(e5)
    out = [ed - half * j0]
    for k in (1, 2, 3):
        if k == d:
            out.append(ed * vel + press - half * jd)
        else:
            ek, jk = edge(k)
            out.append(ek * vel - half * jk)
    e4, j4 = edge(4)
    out.append((e4 + press) * vel - half * j4)
    out.append(e5 * vel - half * j5)
    e6, j6 = edge(6)
    out.append(e6 * vel - half * j6)
    return out


def lanes(shape=(CY, CZ)):
    return lax.broadcasted_iota(jnp.int32, shape, 1)


def rows_of(i):
    start = i * PITCH + BASE
    if not isinstance(i, int):
        start = pl.multiple_of(start, 8)
    return pl.ds(start, CY)


def z_shifted(q):
    return (pltpu.roll(q, 1, 1), q, pltpu.roll(q, CZ - 1, 1), pltpu.roll(q, CZ - 2, 1))


def each(n, body, unroll=1):
    def step(i, c):
        body(i)
        return c

    lax.fori_loop(0, n, step, 0, unroll=unroll)


def pack_z(load, acc, slabs, unroll):
    lane = lanes()

    def put(i, acc, shift):
        here = (lane >= CZ - 8 - 8 * i) & (lane < CZ - 8 * i)
        return tuple(jnp.where(here, pltpu.roll(load(k, i), shift, 1), a) for k, a in enumerate(acc))

    if isinstance(slabs, tuple):
        for i in slabs:
            acc = put(i, acc, CZ - 4 - 8 * i)
        return acc
    return lax.fori_loop(slabs.start, slabs.stop, lambda i, a: put(i, a, CZ - 4 - 8 * i), acc, unroll=unroll)


def blank(count):
    return tuple(jnp.zeros((CY, CZ), jnp.float32) for _ in range(count))


def move_out(*refs):
    n = (len(refs) - 1) // 2
    sem = refs[-1]
    for i in range(n):
        for p in range(refs[i].shape[0]):
            pltpu.make_async_copy(refs[i].at[p], refs[n + i].at[p], sem.at[i]).start()
    for i in range(n):
        pltpu.make_async_copy(refs[i], refs[n + i], sem.at[i]).wait()


def kernel(n_gx, n_gy, n_gz, owner_in, state, phi_in, nst, dsol, res,
           owner_ref, q1, q2, phi, sx, sy, sz, dd, fb, fym, tz,
           xh, ysend, yrecv, zpack, zsend, zrecv,
           pb, pot, pin, pfirst, gl, gr, go,
           pxr, pys, pyr, pzs, pzr,
           m0, m1, m2, mx, my, mz,
           lsem, hs, hr, ps, pr, ds_, dr, fs, fr, ms, mr):
    gx, gy, gz = lax.axis_index("gx"), lax.axis_index("gy"), lax.axis_index("gz")

    def at(axis, pos, n, off):
        return {axis: lax.rem(pos + (off + n), n)}

    x_lo, x_hi = at("gx", gx, n_gx, -1), at("gx", gx, n_gx, 1)
    y_lo, y_hi = at("gy", gy, n_gy, -1), at("gy", gy, n_gy, 1)
    z_lo, z_hi = at("gz", gz, n_gz, -1), at("gz", gz, n_gz, 1)

    def remote(src, dst, send, recv, dev):
        c = pltpu.make_async_remote_copy(src_ref=src, dst_ref=dst, send_sem=send, recv_sem=recv,
                                         device_id=dev, device_id_type=MESH)
        c.start()
        return c

    n_zy = n_gz // 2

    def flat(h):
        return {"gz": (gz // n_zy) * n_zy + lax.rem(gz + h, n_zy)}

    barrier = pltpu.get_barrier_semaphore()
    peers = [x_lo, x_hi, y_lo, y_hi, z_lo, z_hi, at("gy", gy, n_gy, n_gy // 2), at("gz", gz, n_gz, n_zy)]
    for dev in peers:
        pl.semaphore_signal(barrier, inc=1, device_id=dev, device_id_type=MESH)

    for i in range(CX):
        pltpu.make_async_copy(state.at[:, i], q1.at[:, rows_of(i)], lsem.at[0]).start()
    phi_load = pltpu.make_async_copy(phi_in, phi, lsem.at[1])
    phi_load.start()
    owner_load = pltpu.make_async_copy(owner_in, owner_ref, lsem.at[2])
    owner_load.start()

    def wait_for(ref, sem):
        pltpu.make_async_copy(ref, ref, sem).wait()

    def send_x_first():
        return [remote(state.at[:, pl.ds(CX - 2, 2)], xh.at[0, 0], hs.at[0, 0], hr.at[0, 0], x_hi),
                remote(state.at[:, pl.ds(0, 2)], xh.at[0, 1], hs.at[0, 0], hr.at[0, 0], x_lo)]

    def send_x_second():
        cs = []
        for j in (0, 1):
            cs.append(remote(q2.at[:, rows_of(14 + j)], xh.at[1, 0, :, j], hs.at[1, 0], hr.at[1, 0], x_hi))
            cs.append(remote(q2.at[:, rows_of(j)], xh.at[1, 1, :, j], hs.at[1, 0], hr.at[1, 0], x_lo))
        return cs

    def pack_y(q, r):
        for k in range(NF):
            for j in (0, 1):
                ysend[r, 0, k, j] = q[k, pl.ds(BASE + j, CX, stride=PITCH), :]
                ysend[r, 1, k, j] = q[k, pl.ds(BASE + 14 + j, CX, stride=PITCH), :]

    def pack_inner(q, r):
        acc = pack_z(lambda k, i: q[k, rows_of(i), :], blank(NF), range(2, CX - 2), 6)
        for k in range(NF):
            zpack[r, k] = acc[k]

    def pack_outer(q, r):
        acc = pack_z(lambda k, i: q[k, rows_of(i), :], tuple(zpack[r, k] for k in range(NF)), (0, 1, 14, 15), 1)
        for k in range(NF):
            zpack[r, k] = acc[k]
        slot = (lanes((8, CZ)) & 7) >> 1
        for g in range(NF // 2 + 1):
            parts = [acc[k][8 * h:8 * h + 8] for k in (2 * g, 2 * g + 1) if k < NF for h in (0, 1)]
            for side, lane in ((1, 2), (0, 4)):
                v = pltpu.roll(parts[0], CZ - lane, 1)
                for n in range(1, len(parts)):
                    shift = (CZ + 2 * n - lane) % CZ
                    v = jnp.where(slot == n, pltpu.roll(parts[n], shift, 1) if shift else parts[n], v)
                zsend[r, side, g] = v

    def send_y(r):
        return [remote(ysend.at[r, 1], yrecv.at[r, 0], hs.at[r, 1], hr.at[r, 1], y_hi),
                remote(ysend.at[r, 0], yrecv.at[r, 1], hs.at[r, 1], hr.at[r, 1], y_lo)]

    def send_z(r):
        return [remote(zsend.at[r, 1], zrecv.at[r, 0], hs.at[r, 2], hr.at[r, 2], z_hi),
                remote(zsend.at[r, 0], zrecv.at[r, 1], hs.at[r, 2], hr.at[r, 2], z_lo)]

    def interior(q):
        def speed_body(i):
            s = speeds(lambda k: q[k, rows_of(i), :], (1, 2, 3))
            sx[i] = s[0]
            sy[rows_of(i), :] = s[1]
            sz[i] = s[2]

        each(CX, speed_body, UN)
        lane = lanes()
        inner = (lane >= 2) & (lane < CZ - 2)

        def z_body(i):
            s = sz[i]
            f = interface_flux(lambda k: z_shifted(q[k, rows_of(i), :]), s, pltpu.roll(s, CZ - 1, 1), 3)
            for k in range(NF):
                dd[k, i] = jnp.where(inner, pltpu.roll(f[k], 1, 1) - f[k], 0.0)

        each(CX, z_body, UN)

        def x_flux(i):
            return interface_flux(lambda k: tuple(q[k, rows_of(i + o), :] for o in (-1, 0, 1, 2)), sx[i], sx[i + 1], 1)

        f = x_flux(1)
        for k in range(NF):
            fb[0, k] = f[k]

        def x_body(i, prev):
            f = x_flux(i)
            for k in range(NF):
                dd[k, i] = dd[k, i] + (prev[k] - f[k])
            return tuple(f)

        f = lax.fori_loop(2, 14, x_body, tuple(f), unroll=UN)
        for k in range(NF):
            fb[1, k] = f[k]

    def y_part(q, r, finish):
        for k in range(NF):
            for j in (0, 1):
                q[k, pl.ds(BASE - 2 + j, CX, stride=PITCH), :] = yrecv[r, 0, k, j]
                q[k, pl.ds(BASE + CY + j, CX, stride=PITCH), :] = yrecv[r, 1, k, j]
        sy[pl.ds(BASE + CY, CX, stride=PITCH), :] = speeds(lambda k: yrecv[r, 1, k, 0], (2,))[0]
        s_l, = speeds(lambda k: yrecv[r, 0, k, 1], (2,))
        s_r, = speeds(lambda k: ysend[r, 0, k, 0], (2,))
        f = interface_flux(
            lambda k: (yrecv[r, 0, k, 0], yrecv[r, 0, k, 1], ysend[r, 0, k, 0], ysend[r, 0, k, 1]), s_l, s_r, 2)
        for k in range(NF):
            fym[k] = f[k]
        first_row = lax.broadcasted_iota(jnp.int32, (CY, CZ), 0) == 0

        def y_tendency(i):
            at_ = i * PITCH + BASE
            f = interface_flux(lambda k: tuple(q[k, pl.ds(at_ + o, CY), :] for o in (-1, 0, 1, 2)),
                               sy[pl.ds(at_, CY), :], sy[pl.ds(at_ + 1, CY), :], 2)
            for k in range(NF):
                lower = jnp.where(first_row, fym[k, pl.ds(i, 1), :], pltpu.roll(f[k], 1, 0))
                f[k] = dd[k, i] + (lower - f[k])
            return f

        def outer_body(j):
            i = jnp.where(j < 2, j, j + 12)
            t = y_tendency(i)
            for k in range(NF):
                dd[k, i] = t[k]

        each(4, outer_body, UN)

        def inner_body(j):
            finish(j + 2, y_tendency(j + 2))

        each(CX - 4, inner_body, UN)

    def z_part(r):
        low = (lanes() & 7) < 4

        def z_edge(cells):
            s, = speeds(lambda k: cells[k], (3,))
            f = interface_flux(lambda k: z_shifted(cells[k]), s, pltpu.roll(s, CZ - 1, 1), 3)
            return [pltpu.roll(f[k], 1, 1) - f[k] for k in range(NF)]

        def received(side, lane, k):
            m = zrecv[r, side, k // 2]
            shifts = [(2 * CZ + lane - 2 * (2 * (k % 2) + h)) % CZ for h in (0, 1)]
            return jnp.concatenate([pltpu.roll(m, t, 1) if t else m for t in shifts], axis=0)

        def from_left(k):
            return received(0, 2, k)

        def from_right(k):
            return received(1, 4, k)

        left = z_edge([jnp.where(low, from_left(k), zpack[r, k]) for k in range(NF)])
        for k in range(NF):
            tz[k] = left[k]
        right = z_edge([jnp.where(low, zpack[r, k], from_right(k)) for k in range(NF)])
        for k in range(NF):
            tz[k] = jnp.where(low, right[k], tz[k])

    def edge_tendency(i, k):
        lane = lanes()
        outer = (lane < 2) | (lane >= CZ - 2)
        return jnp.where(outer, pltpu.roll(tz[k], 4 + 8 * i, 1), 0.0)

    def tendency(i, k):
        return dd[k, i] + edge_tendency(i, k)

    def edges_rows(scale):
        lane = lanes((CX, CZ))
        x = lax.broadcasted_iota(jnp.int32, (CX, CZ), 0)
        here = ((lane < 2) | (lane >= CZ - 2)) & (x >= 2) & (x < CX - 2)
        for k in range(NF):
            for side, j in ((0, 0), (0, 1), (1, 0), (1, 1)):
                row = jnp.broadcast_to(tz[k, 14 * side + j:14 * side + j + 1, :], (CX, CZ))
                part = pltpu.roll(row, 4, 1, stride=8, stride_axis=0)
                ysend[1, side, k, j] = ysend[1, side, k, j] + jnp.where(here, scale * part, 0.0)

    def x_part(q, r, finish):
        def get(i):
            if i < 0:
                return lambda k: xh[r, 0, k, i + 2]
            if i >= CX:
                return lambda k: xh[r, 1, k, i - CX]
            return lambda k: q[k, rows_of(i), :]

        def speed(i):
            return sx[i] if 0 <= i < CX else speeds(get(i), (1,))[0]

        def flux(i):
            g = [get(i + o) for o in (-1, 0, 1, 2)]
            return interface_flux(lambda k: tuple(h(k) for h in g), speed(i), speed(i + 1), 1)

        a = flux(-1)
        b = flux(0)
        finish(0, [tendency(0, k) + (a[k] - b[k]) for k in range(NF)])
        finish(1, [tendency(1, k) + (b[k] - fb[0, k]) for k in range(NF)])
        a = flux(14)
        finish(14, [tendency(14, k) + (fb[1, k] - a[k]) for k in range(NF)])
        b = flux(15)
        finish(15, [tendency(15, k) + (a[k] - b[k]) for k in range(NF)])

    def edges(scale, view, fields):
        def body(j):
            for k in fields:
                ref, idx = view(j + 2, k)
                ref[idx] = ref[idx] + scale * edge_tendency(j + 2, k)
        each(CX - 4, body, 6)

    def edges_packed(r, scale):
        lane = lanes()
        here = (lane >= 16) & (lane < CZ - 16) & ((lane & 7) >= 2) & ((lane & 7) < 6)
        for k in range(NF):
            zpack[r, k] = zpack[r, k] + jnp.where(here, scale * tz[k], 0.0)

    def finish_first(i, t):
        for k in range(NF):
            q2[k, rows_of(i), :] = q1[k, rows_of(i), :] + DTH * t[k]

    def finish_new(i, t):
        for k in range(NF):
            nst[k, i] = 0.5 * q1[k, rows_of(i), :] + 0.5 * (q2[k, rows_of(i), :] + DTH * t[k])

    pl.semaphore_wait(barrier, len(peers))
    send_x_first()
    wait_for(q1.at[:, pl.ds(0, CX * CY)], lsem.at[0])
    pack_inner(q1, 0)
    pack_outer(q1, 0)
    send_z(0)
    pack_y(q1, 0)
    send_y(0)

    phi_load.wait()
    owner_load.wait()

    def is_code(box, slot):
        return jnp.where(owner_ref[0, 0, box] == gx * SLOTS + slot, 1.0, 0.0).astype(jnp.float32)

    masks = [[[is_code(lax.rem(gx + o, n_gx) * 2 + b, s) for s in range(SLOTS)] for b in (0, 1)] for o in range(4)]

    for o in (2, 1, 3, 0):
        def phi_body(j, o=o):
            rows = [phi[s, j] for s in range(SLOTS)]
            for b in (0, 1):
                m = masks[o][b]
                v = rows[0] * m[0]
                for s in range(1, SLOTS):
                    v = v + rows[s] * m[s]
                pb[o, b, j] = v
        each(HALF, phi_body)
    interior(q1)
    wait_for(yrecv.at[0], hr.at[0, 1])
    y_part(q1, 0, finish_first)
    remote(pb.at[2, 0], pfirst.at[0], ps.at[0], pr.at[0], x_hi)
    remote(pb.at[2, 1], pfirst.at[1], ps.at[0], pr.at[0], x_lo)
    pack_inner(q2, 1)
    wait_for(zrecv.at[0], hr.at[0, 2])
    z_part(0)
    edges_packed(1, DTH)
    wait_for(xh.at[0], hr.at[0, 0])
    x_part(q1, 0, finish_first)

    pack_outer(q2, 1)
    send_z(1)
    send_x_second()
    pack_y(q2, 1)
    edges_rows(DTH)
    send_y(1)
    edges(DTH, lambda i, k: (q2, (k, rows_of(i), slice(None))), range(NF))

    interior(q2)
    wait_for(yrecv.at[1], hr.at[1, 1])
    y_part(q2, 1, finish_new)
    remote(pb.at[1, 1], pin.at[0, 1], ps.at[1], pr.at[1], x_hi)
    remote(pb.at[3, 0], pin.at[1, 0], ps.at[1], pr.at[1], x_lo)
    wait_for(pfirst, pr.at[0])

    def add_body(j):
        pb[1, 0, j] = pb[1, 0, j] + pfirst[0, j]
        pb[3, 1, j] = pb[3, 1, j] + pfirst[1, j]

    each(HALF, add_body)
    wait_for(zrecv.at[1], hr.at[1, 2])
    z_part(1)
    edges(0.5 * DTH, lambda i, k: (nst, (k, i)), (0,))
    wait_for(xh.at[1], hr.at[1, 0])
    x_part(q2, 1, finish_new)

    def mass_body(i, acc):
        return acc + nst[0, i, 0:8, :] + nst[0, i, 8:16, :]

    acc = lax.fori_loop(0, CX, mass_body, jnp.zeros((8, CZ), jnp.float32), unroll=4)
    m0[...] = jnp.sum(acc, axis=0, keepdims=True)

    def spread(src, dst, devices, t):
        for n, dev in enumerate(devices):
            remote(src, dst.at[n], ms.at[t], mr.at[t], dev)

    def gathered(own, got, t):
        wait_for(got, mr.at[t])
        acc = own[...]
        for n in range(got.shape[0]):
            acc = acc + got[n]
        return acc

    along_z = [{**at("gx", gx, n_gx, o), **at("gz", gz, n_gz, h * n_zy)}
               for o in range(n_gx) for h in (0, 1) if o + h > 0]
    spread(m0, mz, along_z, 0)
    remote(pb.at[1, 0], pin.at[0, 0], ps.at[1], pr.at[1], x_hi)
    remote(pb.at[3, 1], pin.at[1, 1], ps.at[1], pr.at[1], x_lo)

    remote(nst.at[0, pl.ds(0, HALF)], gl.at[0], ds_.at[0], dr.at[0], x_hi)
    remote(nst.at[0, pl.ds(HALF, HALF)], gr.at[1], ds_.at[0], dr.at[1], x_lo)
    remote(nst.at[0, pl.ds(HALF, HALF)], gl.at[1], ds_.at[0], dr.at[2], x_hi)
    remote(nst.at[0, pl.ds(0, HALF)], gr.at[0], ds_.at[0], dr.at[4], x_lo)
    edges(0.5 * DTH, lambda i, k: (nst, (k, i)), range(1, NF))

    m1[...] = gathered(m0, mz, 0)
    spread(m1, mx, [at("gy", gy, n_gy, o) for o in range(1, n_gy)], 1)

    wait_for(pin, pr.at[1])

    def pot_body(j):
        for b in (0, 1):
            pot[b * HALF + j] = pb[0, b, j] + (pin[0, b, j] + pin[1, b, j])

    each(HALF, pot_body)
    def row_body(i):
        pys[0, pl.ds(i, 1), :] = pot[i, 0:1, :]
        pys[1, pl.ds(i, 1), :] = pot[i, CY - 1:CY, :]

    each(CX, row_body)
    pzs[0] = pack_z(lambda k, i: pot[i], blank(1), range(0, CX), 16)[0]
    remote(pot.at[CX - 1], pxr.at[0], fs.at[0], fr.at[0], x_hi)
    remote(pot.at[0], pxr.at[1], fs.at[0], fr.at[0], x_lo)
    remote(pys.at[1], pyr.at[0], fs.at[1], fr.at[1], y_hi)
    remote(pys.at[0], pyr.at[1], fs.at[1], fr.at[1], y_lo)
    remote(pzs.at[0], pzr.at[0], fs.at[2], fr.at[2], z_hi)
    remote(pzs.at[0], pzr.at[1], fs.at[2], fr.at[2], z_lo)

    wait_for(gl.at[0], dr.at[0])
    remote(gl.at[0], go.at[0], ds_.at[1], dr.at[3], x_hi)
    wait_for(gr.at[1], dr.at[1])
    remote(gr.at[1], go.at[1], ds_.at[1], dr.at[3], x_lo)

    m2[...] = gathered(m1, mx, 1)
    spread(m2, my, [flat(h) for h in range(1, n_zy)], 2)

    wait_for(gl.at[1], dr.at[2])
    wait_for(gr.at[0], dr.at[4])

    def is_box(o, b, s):
        return is_code(lax.rem(gx + o, n_gx) * 2 + b, s)

    near = [[(is_box(o, b, s)) for o in (0, 3, 1) for b in (0, 1)] for s in range(SLOTS)]

    def near_body(j):
        boxes = [nst[0, j], nst[0, HALF + j], gl[0, j], gl[1, j], gr[0, j], gr[1, j]]
        for s in range(SLOTS):
            v = boxes[0] * near[s][0]
            for t in range(1, 6):
                v = v + boxes[t] * near[s][t]
            dsol[s, j] = v
    each(HALF, near_body)
    total = gathered(m2, my, 2)
    cells = float(CX * CY * CZ * n_gx * n_gy * n_gz)
    mean = jnp.sum(total) / cells

    for n, ref in enumerate((pxr, pyr, pzr)):
        wait_for(ref, fr.at[n])
    lane = lanes()
    row = lax.broadcasted_iota(jnp.int32, (CY, CZ), 0)
    halo = jnp.where((lane & 7) < 4, pzr[0, :, :], pzr[1, :, :])

    def lap(i, below, above):
        p = pot[i]
        h = pltpu.roll(halo, 4 + 8 * i, 1)
        z = pltpu.roll(jnp.where(lane == CZ - 1, h, p), 1, 1) + pltpu.roll(jnp.where(lane == 0, h, p), CZ - 1, 1)
        up = jnp.where(row == 0, pyr[0, pl.ds(i, 1), :], pltpu.roll(p, 1, 0))
        dn = jnp.where(row == CY - 1, pyr[1, pl.ds(i, 1), :], pltpu.roll(p, CY - 1, 0))
        res[i] = FOURPIG * (nst[0, i] - mean) - (((below + above) + (up + dn) + z) - 6.0 * p)

    lap(0, pxr[0], pot[1])

    def lap_body(j):
        lap(j + 1, pot[j], pot[j + 2])
    each(CX - 2, lap_body, 7)
    lap(CX - 1, pot[CX - 2], pxr[1])

    far = [[is_box(2, b, s) for b in (0, 1)] for s in range(SLOTS)]
    wait_for(go, dr.at[3])

    def far_body(j):
        boxes = [go[0, j], go[1, j]]
        for s in range(SLOTS):
            dsol[s, j] = dsol[s, j] + (boxes[0] * far[s][0] + boxes[1] * far[s][1])
    each(HALF, far_body)

    for r in (0, 1):
        for n, ref in enumerate((xh, yrecv, zrecv)):
            wait_for(ref.at[r], hs.at[r, n])
    for ref, sem in ((pfirst, ps.at[0]), (pin, ps.at[1]), (pin, ds_.at[0]), (go, ds_.at[1]), (mz, ms.at[0]), (mx, ms.at[1]), (my, ms.at[2]),
                     (pxr, fs.at[0]), (pyr, fs.at[1]), (pzr, fs.at[2])):
        wait_for(ref, sem)


def solution(mesh):
    n_gx, n_gy, n_gz = mesh.shape["gx"], mesh.shape["gy"], mesh.shape["gz"]

    def on_device(state, solver_owner, phi_prev):
        f32 = jnp.float32
        V = lambda *s: pltpu.VMEM(s, f32)
        D = lambda *s: pltpu.SemaphoreType.DMA(s)
        hbm = pl.BlockSpec(memory_space=pltpu.HBM)
        vmem = pl.BlockSpec(memory_space=pltpu.VMEM)
        outs = pl.pallas_call(
            functools.partial(kernel, n_gx, n_gy, n_gz),
            out_shape=(
                jax.ShapeDtypeStruct(state.shape, f32),
                jax.ShapeDtypeStruct(phi_prev.shape, f32),
                jax.ShapeDtypeStruct(state.shape[1:], f32),
            ),
            in_specs=[hbm, hbm, hbm],
            out_specs=(vmem, vmem, vmem),
            scratch_shapes=[
                pltpu.SMEM((1, 1, 8), jnp.int32),
                V(NF, ROWS, CZ), V(NF, ROWS, CZ), V(SLOTS, HALF, CY, CZ),
                V(CX, CY, CZ), V(ROWS, CZ), V(CX, CY, CZ), V(NF, CX, CY, CZ),
                V(2, NF, CY, CZ), V(NF, CX, CZ), V(NF, CY, CZ),
                V(2, 2, NF, 2, CY, CZ), V(2, 2, NF, 2, CX, CZ), V(2, 2, NF, 2, CX, CZ),
                V(2, NF, CY, CZ), V(2, 2, NF // 2 + 1, 8, CZ), V(2, 2, NF // 2 + 1, 8, CZ),
                V(4, 2, HALF, CY, CZ), V(CX, CY, CZ), V(2, 2, HALF, CY, CZ), V(2, HALF, CY, CZ),
                V(2, HALF, CY, CZ), V(2, HALF, CY, CZ), V(2, HALF, CY, CZ),
                V(2, CY, CZ), V(2, CX, CZ), V(2, CX, CZ), V(1, CY, CZ), V(2, CY, CZ),
                V(1, CZ), V(1, CZ), V(1, CZ),
                V(n_gy - 1, 1, CZ), V(n_gz // 2 - 1, 1, CZ), V(2 * n_gx - 1, 1, CZ),
                D(3), D(2, 3), D(2, 3), D(2), D(2), D(2), D(5), D(3), D(3), D(3), D(3),
            ],
            compiler_params=pltpu.CompilerParams(
                collective_id=0, has_side_effects=True, vmem_limit_bytes=32 * 1024 * 1024
            ),
            name="gas_step",
        )(
            pltpu.with_memory_space_constraint(solver_owner, pltpu.HBM),
            pltpu.with_memory_space_constraint(state, pltpu.HBM),
            pltpu.with_memory_space_constraint(phi_prev, pltpu.HBM),
        )
        return pl.pallas_call(
            move_out,
            out_shape=tuple(jax.ShapeDtypeStruct(o.shape, f32) for o in outs),
            in_specs=[vmem] * 3,
            out_specs=(hbm,) * 3,
            scratch_shapes=[D(3)],
            compiler_params=pltpu.CompilerParams(has_side_effects=True, vmem_limit_bytes=4 * 1024 * 1024),
            name="move_out",
        )(*outs)

    return jax.shard_map(
        on_device,
        mesh=mesh,
        in_specs=(P(None, "gx", "gy", "gz"), P("gy", "gz", None), P("gx", None, "gy", "gz")),
        out_specs=(P(None, "gx", "gy", "gz"), P("gx", None, "gy", "gz"), P("gx", "gy", "gz")),
        check_vma=False,
    )
```

```python
import functools

import jax
import jax.numpy as jnp
from jax import lax
from jax.experimental import pallas as pl
from jax.experimental.pallas import tpu as pltpu
from jax.sharding import PartitionSpec as P

MESH = pl.DeviceIdType.MESH
GAMMA = 5.0 / 3.0
DTH = 0.04
FOURPIG = 2.0
NF = 7
CX, CY, CZ = 16, 16, 128
PITCH, BASE = 24, 8
ROWS = CX * PITCH + 8
HALF = 8
SLOTS = 4
UN = 4


def pressure(q5):
    return (GAMMA - 1.0) * jnp.maximum(q5, 0.1)


def speeds(get, dirs):
    inv = 1.0 / jnp.maximum(get(0), 0.25)
    sound = jnp.sqrt(GAMMA * pressure(get(5)) * inv)
    return [jnp.abs(get(d)) * inv + sound for d in dirs]


def interface_flux(get, speed_l, speed_r, d):
    def edge(k):
        a, b, c, e = get(k)
        v = 7.0 / 12.0 * (b + c) - 1.0 / 12.0 * (a + e)
        v = jnp.minimum(jnp.maximum(v, jnp.minimum(b, c)), jnp.maximum(b, c))
        return v, c - b

    half = 0.5 * jnp.maximum(speed_l, speed_r)
    e0, j0 = edge(0)
    ed, jd = edge(d)
    e5, j5 = edge(5)
    vel = ed / jnp.maximum(e0, 0.25)
    press = pressure(e5)
    out = [ed - half * j0]
    for k in (1, 2, 3):
        if k == d:
            out.append(ed * vel + press - half * jd)
        else:
            ek, jk = edge(k)
            out.append(ek * vel - half * jk)
    e4, j4 = edge(4)
    out.append((e4 + press) * vel - half * j4)
    out.append(e5 * vel - half * j5)
    e6, j6 = edge(6)
    out.append(e6 * vel - half * j6)
    return out


def lanes(shape=(CY, CZ)):
    return lax.broadcasted_iota(jnp.int32, shape, 1)


def rows_of(i):
    start = i * PITCH + BASE
    if not isinstance(i, int):
        start = pl.multiple_of(start, 8)
    return pl.ds(start, CY)


def z_shifted(q):
    return (pltpu.roll(q, 1, 1), q, pltpu.roll(q, CZ - 1, 1), pltpu.roll(q, CZ - 2, 1))


def each(n, body, unroll=1):
    def step(i, c):
        body(i)
        return c

    lax.fori_loop(0, n, step, 0, unroll=unroll)


def pack_z(load, acc, slabs, unroll):
    lane = lanes()

    def put(i, acc, shift):
        here = (lane >= CZ - 8 - 8 * i) & (lane < CZ - 8 * i)
        return tuple(jnp.where(here, pltpu.roll(load(k, i), shift, 1), a) for k, a in enumerate(acc))

    if isinstance(slabs, tuple):
        for i in slabs:
            acc = put(i, acc, CZ - 4 - 8 * i)
        return acc
    return lax.fori_loop(slabs.start, slabs.stop, lambda i, a: put(i, a, CZ - 4 - 8 * i), acc, unroll=unroll)


def blank(count):
    return tuple(jnp.zeros((CY, CZ), jnp.float32) for _ in range(count))


def move_out(*refs):
    n = (len(refs) - 1) // 2
    sem = refs[-1]
    for i in range(n):
        for p in range(refs[i].shape[0]):
            pltpu.make_async_copy(refs[i].at[p], refs[n + i].at[p], sem.at[i]).start()
    for i in range(n):
        pltpu.make_async_copy(refs[i], refs[n + i], sem.at[i]).wait()


def kernel(n_gx, n_gy, n_gz, owner_in, state, phi_in, nst, dsol, res,
           owner_ref, q1, q2, phi, sx, sy, sz, dd, fb, fym, tz,
           xh, ysend, yrecv, zpack, zsend, zrecv,
           pb, pot, pin, pfirst, gl, gr, go,
           pxr, pys, pyr, pzs, pzr,
           m0, m1, m2, mx, my, mz,
           lsem, hs, hr, ps, pr, ds_, dr, fs, fr, ms, mr):
    gx, gy, gz = lax.axis_index("gx"), lax.axis_index("gy"), lax.axis_index("gz")

    def at(axis, pos, n, off):
        return {axis: lax.rem(pos + (off + n), n)}

    x_lo, x_hi = at("gx", gx, n_gx, -1), at("gx", gx, n_gx, 1)
    y_lo, y_hi = at("gy", gy, n_gy, -1), at("gy", gy, n_gy, 1)
    z_lo, z_hi = at("gz", gz, n_gz, -1), at("gz", gz, n_gz, 1)

    def remote(src, dst, send, recv, dev):
        c = pltpu.make_async_remote_copy(src_ref=src, dst_ref=dst, send_sem=send, recv_sem=recv,
                                         device_id=dev, device_id_type=MESH)
        c.start()
        return c

    n_zy = n_gz // 2

    def flat(h):
        return {"gz": (gz // n_zy) * n_zy + lax.rem(gz + h, n_zy)}

    barrier = pltpu.get_barrier_semaphore()
    peers = [x_lo, x_hi, y_lo, y_hi, z_lo, z_hi, at("gy", gy, n_gy, n_gy // 2), at("gz", gz, n_gz, n_zy)]
    for dev in peers:
        pl.semaphore_signal(barrier, inc=1, device_id=dev, device_id_type=MESH)

    for i in range(CX):
        pltpu.make_async_copy(state.at[:, i], q1.at[:, rows_of(i)], lsem.at[0]).start()
    phi_load = pltpu.make_async_copy(phi_in, phi, lsem.at[1])
    phi_load.start()
    owner_load = pltpu.make_async_copy(owner_in, owner_ref, lsem.at[2])
    owner_load.start()

    def wait_for(ref, sem):
        pltpu.make_async_copy(ref, ref, sem).wait()

    def send_x_first():
        return [remote(state.at[:, pl.ds(CX - 2, 2)], xh.at[0, 0], hs.at[0, 0], hr.at[0, 0], x_hi),
                remote(state.at[:, pl.ds(0, 2)], xh.at[0, 1], hs.at[0, 0], hr.at[0, 0], x_lo)]

    def send_x_second():
        cs = []
        for j in (0, 1):
            cs.append(remote(q2.at[:, rows_of(14 + j)], xh.at[1, 0, :, j], hs.at[1, 0], hr.at[1, 0], x_hi))
            cs.append(remote(q2.at[:, rows_of(j)], xh.at[1, 1, :, j], hs.at[1, 0], hr.at[1, 0], x_lo))
        return cs

    def pack_y(q, r):
        for k in range(NF):
            for j in (0, 1):
                ysend[r, 0, k, j] = q[k, pl.ds(BASE + j, CX, stride=PITCH), :]
                ysend[r, 1, k, j] = q[k, pl.ds(BASE + 14 + j, CX, stride=PITCH), :]

    def pack_inner(q, r):
        acc = pack_z(lambda k, i: q[k, rows_of(i), :], blank(NF), range(2, CX - 2), 6)
        for k in range(NF):
            zpack[r, k] = acc[k]

    def pack_outer(q, r):
        acc = pack_z(lambda k, i: q[k, rows_of(i), :], tuple(zpack[r, k] for k in range(NF)), (0, 1, 14, 15), 1)
        for k in range(NF):
            zpack[r, k] = acc[k]
        slot = (lanes((8, CZ)) & 7) >> 1
        for g in range(NF // 2 + 1):
            parts = [acc[k][8 * h:8 * h + 8] for k in (2 * g, 2 * g + 1) if k < NF for h in (0, 1)]
            for side, lane in ((1, 2), (0, 4)):
                v = pltpu.roll(parts[0], CZ - lane, 1)
                for n in range(1, len(parts)):
                    shift = (CZ + 2 * n - lane) % CZ
                    v = jnp.where(slot == n, pltpu.roll(parts[n], shift, 1) if shift else parts[n], v)
                zsend[r, side, g] = v

    def send_y(r):
        return [remote(ysend.at[r, 1], yrecv.at[r, 0], hs.at[r, 1], hr.at[r, 1], y_hi),
                remote(ysend.at[r, 0], yrecv.at[r, 1], hs.at[r, 1], hr.at[r, 1], y_lo)]

    def send_z(r):
        return [remote(zsend.at[r, 1], zrecv.at[r, 0], hs.at[r, 2], hr.at[r, 2], z_hi),
                remote(zsend.at[r, 0], zrecv.at[r, 1], hs.at[r, 2], hr.at[r, 2], z_lo)]

    def interior(q):
        def speed_body(i):
            s = speeds(lambda k: q[k, rows_of(i), :], (1, 2, 3))
            sx[i] = s[0]
            sy[rows_of(i), :] = s[1]
            sz[i] = s[2]

        each(CX, speed_body, UN)
        lane = lanes()
        inner = (lane >= 2) & (lane < CZ - 2)

        def z_body(i):
            s = sz[i]
            f = interface_flux(lambda k: z_shifted(q[k, rows_of(i), :]), s, pltpu.roll(s, CZ - 1, 1), 3)
            for k in range(NF):
                dd[k, i] = jnp.where(inner, pltpu.roll(f[k], 1, 1) - f[k], 0.0)

        each(CX, z_body, UN)

        def x_flux(i):
            return interface_flux(lambda k: tuple(q[k, rows_of(i + o), :] for o in (-1, 0, 1, 2)), sx[i], sx[i + 1], 1)

        f = x_flux(1)
        for k in range(NF):
            fb[0, k] = f[k]

        def x_body(i, prev):
            f = x_flux(i)
            for k in range(NF):
                dd[k, i] = dd[k, i] + (prev[k] - f[k])
            return tuple(f)

        f = lax.fori_loop(2, 14, x_body, tuple(f), unroll=UN)
        for k in range(NF):
            fb[1, k] = f[k]

    def y_part(q, r, finish):
        for k in range(NF):
            for j in (0, 1):
                q[k, pl.ds(BASE - 2 + j, CX, stride=PITCH), :] = yrecv[r, 0, k, j]
                q[k, pl.ds(BASE + CY + j, CX, stride=PITCH), :] = yrecv[r, 1, k, j]
        sy[pl.ds(BASE + CY, CX, stride=PITCH), :] = speeds(lambda k: yrecv[r, 1, k, 0], (2,))[0]
        s_l, = speeds(lambda k: yrecv[r, 0, k, 1], (2,))
        s_r, = speeds(lambda k: ysend[r, 0, k, 0], (2,))
        f = interface_flux(
            lambda k: (yrecv[r, 0, k, 0], yrecv[r, 0, k, 1], ysend[r, 0, k, 0], ysend[r, 0, k, 1]), s_l, s_r, 2)
        for k in range(NF):
            fym[k] = f[k]
        first_row = lax.broadcasted_iota(jnp.int32, (CY, CZ), 0) == 0

        def y_tendency(i):
            at_ = i * PITCH + BASE
            f = interface_flux(lambda k: tuple(q[k, pl.ds(at_ + o, CY), :] for o in (-1, 0, 1, 2)),
                               sy[pl.ds(at_, CY), :], sy[pl.ds(at_ + 1, CY), :], 2)
            for k in range(NF):
                lower = jnp.where(first_row, fym[k, pl.ds(i, 1), :], pltpu.roll(f[k], 1, 0))
                f[k] = dd[k, i] + (lower - f[k])
            return f

        def outer_body(j):
            i = jnp.where(j < 2, j, j + 12)
            t = y_tendency(i)
            for k in range(NF):
                dd[k, i] = t[k]

        each(4, outer_body, UN)

        def inner_body(j):
            finish(j + 2, y_tendency(j + 2))

        each(CX - 4, inner_body, UN)

    def z_part(r):
        low = (lanes() & 7) < 4

        def z_edge(cells):
            s, = speeds(lambda k: cells[k], (3,))
            f = interface_flux(lambda k: z_shifted(cells[k]), s, pltpu.roll(s, CZ - 1, 1), 3)
            return [pltpu.roll(f[k], 1, 1) - f[k] for k in range(NF)]

        def received(side, lane, k):
            m = zrecv[r, side, k // 2]
            shifts = [(2 * CZ + lane - 2 * (2 * (k % 2) + h)) % CZ for h in (0, 1)]
            return jnp.concatenate([pltpu.roll(m, t, 1) if t else m for t in shifts], axis=0)

        def from_left(k):
            return received(0, 2, k)

        def from_right(k):
            return received(1, 4, k)

        left = z_edge([jnp.where(low, from_left(k), zpack[r, k]) for k in range(NF)])
        for k in range(NF):
            tz[k] = left[k]
        right = z_edge([jnp.where(low, zpack[r, k], from_right(k)) for k in range(NF)])
        for k in range(NF):
            tz[k] = jnp.where(low, right[k], tz[k])

    def edge_tendency(i, k):
        lane = lanes()
        outer = (lane < 2) | (lane >= CZ - 2)
        return jnp.where(outer, pltpu.roll(tz[k], 4 + 8 * i, 1), 0.0)

    def tendency(i, k):
        return dd[k, i] + edge_tendency(i, k)

    def edges_rows(scale):
        lane = lanes((CX, CZ))
        x = lax.broadcasted_iota(jnp.int32, (CX, CZ), 0)
        here = ((lane < 2) | (lane >= CZ - 2)) & (x >= 2) & (x < CX - 2)
        for k in range(NF):
            for side, j in ((0, 0), (0, 1), (1, 0), (1, 1)):
                row = jnp.broadcast_to(tz[k, 14 * side + j:14 * side + j + 1, :], (CX, CZ))
                part = pltpu.roll(row, 4, 1, stride=8, stride_axis=0)
                ysend[1, side, k, j] = ysend[1, side, k, j] + jnp.where(here, scale * part, 0.0)

    def x_part(q, r, finish):
        def get(i):
            if i < 0:
                return lambda k: xh[r, 0, k, i + 2]
            if i >= CX:
                return lambda k: xh[r, 1, k, i - CX]
            return lambda k: q[k, rows_of(i), :]

        def speed(i):
            return sx[i] if 0 <= i < CX else speeds(get(i), (1,))[0]

        def flux(i):
            g = [get(i + o) for o in (-1, 0, 1, 2)]
            return interface_flux(lambda k: tuple(h(k) for h in g), speed(i), speed(i + 1), 1)

        a = flux(-1)
        b = flux(0)
        finish(0, [tendency(0, k) + (a[k] - b[k]) for k in range(NF)])
        finish(1, [tendency(1, k) + (b[k] - fb[0, k]) for k in range(NF)])
        a = flux(14)
        finish(14, [tendency(14, k) + (fb[1, k] - a[k]) for k in range(NF)])
        b = flux(15)
        finish(15, [tendency(15, k) + (a[k] - b[k]) for k in range(NF)])

    def edges(scale, view, fields):
        def body(j):
            for k in fields:
                ref, idx = view(j + 2, k)
                ref[idx] = ref[idx] + scale * edge_tendency(j + 2, k)
        each(CX - 4, body, 6)

    def edges_packed(r, scale):
        lane = lanes()
        here = (lane >= 16) & (lane < CZ - 16) & ((lane & 7) >= 2) & ((lane & 7) < 6)
        for k in range(NF):
            zpack[r, k] = zpack[r, k] + jnp.where(here, scale * tz[k], 0.0)

    def finish_first(i, t):
        for k in range(NF):
            q2[k, rows_of(i), :] = q1[k, rows_of(i), :] + DTH * t[k]

    def finish_new(i, t):
        for k in range(NF):
            nst[k, i] = 0.5 * q1[k, rows_of(i), :] + 0.5 * (q2[k, rows_of(i), :] + DTH * t[k])

    pl.semaphore_wait(barrier, len(peers))
    send_x_first()
    wait_for(q1.at[:, pl.ds(0, CX * CY)], lsem.at[0])
    pack_inner(q1, 0)
    pack_outer(q1, 0)
    send_z(0)
    pack_y(q1, 0)
    send_y(0)

    phi_load.wait()
    owner_load.wait()

    def is_code(box, slot):
        return jnp.where(owner_ref[0, 0, box] == gx * SLOTS + slot, 1.0, 0.0).astype(jnp.float32)

    masks = [[[is_code(lax.rem(gx + o, n_gx) * 2 + b, s) for s in range(SLOTS)] for b in (0, 1)] for o in range(4)]

    for o in (2, 1, 3, 0):
        def phi_body(j, o=o):
            rows = [phi[s, j] for s in range(SLOTS)]
            for b in (0, 1):
                m = masks[o][b]
                v = rows[0] * m[0]
                for s in range(1, SLOTS):
                    v = v + rows[s] * m[s]
                pb[o, b, j] = v
        each(HALF, phi_body)
    interior(q1)
    wait_for(yrecv.at[0], hr.at[0, 1])
    y_part(q1, 0, finish_first)
    remote(pb.at[2, 0], pfirst.at[0], ps.at[0], pr.at[0], x_hi)
    remote(pb.at[2, 1], pfirst.at[1], ps.at[0], pr.at[0], x_lo)
    pack_inner(q2, 1)
    wait_for(zrecv.at[0], hr.at[0, 2])
    z_part(0)
    edges_packed(1, DTH)
    wait_for(xh.at[0], hr.at[0, 0])
    x_part(q1, 0, finish_first)

    pack_outer(q2, 1)
    send_z(1)
    send_x_second()
    pack_y(q2, 1)
    edges_rows(DTH)
    send_y(1)
    edges(DTH, lambda i, k: (q2, (k, rows_of(i), slice(None))), range(NF))

    interior(q2)
    wait_for(yrecv.at[1], hr.at[1, 1])
    y_part(q2, 1, finish_new)
    remote(pb.at[1, 1], pin.at[0, 1], ps.at[1], pr.at[1], x_hi)
    remote(pb.at[3, 0], pin.at[1, 0], ps.at[1], pr.at[1], x_lo)
    wait_for(pfirst, pr.at[0])

    def add_body(j):
        pb[1, 0, j] = pb[1, 0, j] + pfirst[0, j]
        pb[3, 1, j] = pb[3, 1, j] + pfirst[1, j]

    each(HALF, add_body)
    wait_for(zrecv.at[1], hr.at[1, 2])
    z_part(1)
    edges(0.5 * DTH, lambda i, k: (nst, (k, i)), (0,))
    wait_for(xh.at[1], hr.at[1, 0])
    x_part(q2, 1, finish_new)

    def mass_body(i, acc):
        return acc + nst[0, i, 0:8, :] + nst[0, i, 8:16, :]

    acc = lax.fori_loop(0, CX, mass_body, jnp.zeros((8, CZ), jnp.float32), unroll=4)
    m0[...] = jnp.sum(acc, axis=0, keepdims=True)

    def spread(src, dst, devices, t):
        for n, dev in enumerate(devices):
            remote(src, dst.at[n], ms.at[t], mr.at[t], dev)

    def gathered(own, got, t):
        wait_for(got, mr.at[t])
        acc = own[...]
        for n in range(got.shape[0]):
            acc = acc + got[n]
        return acc

    along_z = [{**at("gx", gx, n_gx, o), **at("gz", gz, n_gz, h * n_zy)}
               for o in range(n_gx) for h in (0, 1) if o + h > 0]
    spread(m0, mz, along_z, 0)
    remote(pb.at[1, 0], pin.at[0, 0], ps.at[1], pr.at[1], x_hi)
    remote(pb.at[3, 1], pin.at[1, 1], ps.at[1], pr.at[1], x_lo)

    remote(nst.at[0, pl.ds(0, HALF)], gl.at[0], ds_.at[0], dr.at[0], x_hi)
    remote(nst.at[0, pl.ds(HALF, HALF)], gr.at[1], ds_.at[0], dr.at[1], x_lo)
    remote(nst.at[0, pl.ds(HALF, HALF)], gl.at[1], ds_.at[0], dr.at[2], x_hi)
    remote(nst.at[0, pl.ds(0, HALF)], gr.at[0], ds_.at[0], dr.at[4], x_lo)
    edges(0.5 * DTH, lambda i, k: (nst, (k, i)), range(1, NF))

    m1[...] = gathered(m0, mz, 0)
    spread(m1, mx, [at("gy", gy, n_gy, o) for o in range(1, n_gy)], 1)

    wait_for(pin, pr.at[1])

    def pot_body(j):
        for b in (0, 1):
            pot[b * HALF + j] = pb[0, b, j] + (pin[0, b, j] + pin[1, b, j])

    each(HALF, pot_body)
    def row_body(i):
        pys[0, pl.ds(i, 1), :] = pot[i, 0:1, :]
        pys[1, pl.ds(i, 1), :] = pot[i, CY - 1:CY, :]

    each(CX, row_body)
    pzs[0] = pack_z(lambda k, i: pot[i], blank(1), range(0, CX), 16)[0]
    remote(pot.at[CX - 1], pxr.at[0], fs.at[0], fr.at[0], x_hi)
    remote(pot.at[0], pxr.at[1], fs.at[0], fr.at[0], x_lo)
    remote(pys.at[1], pyr.at[0], fs.at[1], fr.at[1], y_hi)
    remote(pys.at[0], pyr.at[1], fs.at[1], fr.at[1], y_lo)
    remote(pzs.at[0], pzr.at[0], fs.at[2], fr.at[2], z_hi)
    remote(pzs.at[0], pzr.at[1], fs.at[2], fr.at[2], z_lo)

    wait_for(gl.at[0], dr.at[0])
    remote(gl.at[0], go.at[0], ds_.at[1], dr.at[3], x_hi)
    wait_for(gr.at[1], dr.at[1])
    remote(gr.at[1], go.at[1], ds_.at[1], dr.at[3], x_lo)

    m2[...] = gathered(m1, mx, 1)
    spread(m2, my, [flat(h) for h in range(1, n_zy)], 2)

    wait_for(gl.at[1], dr.at[2])
    wait_for(gr.at[0], dr.at[4])

    def is_box(o, b, s):
        return is_code(lax.rem(gx + o, n_gx) * 2 + b, s)

    near = [[(is_box(o, b, s)) for o in (0, 3, 1) for b in (0, 1)] for s in range(SLOTS)]

    def near_body(j):
        boxes = [nst[0, j], nst[0, HALF + j], gl[0, j], gl[1, j], gr[0, j], gr[1, j]]
        for s in range(SLOTS):
            v = boxes[0] * near[s][0]
            for t in range(1, 6):
                v = v + boxes[t] * near[s][t]
            dsol[s, j] = v
    each(HALF, near_body)
    for n, ref in enumerate((pxr, pyr, pzr)):
        wait_for(ref, fr.at[n])
    lane = lanes()
    row = lax.broadcasted_iota(jnp.int32, (CY, CZ), 0)
    halo = jnp.where((lane & 7) < 4, pzr[0, :, :], pzr[1, :, :])

    def lap(i, below, above):
        p = pot[i]
        h = pltpu.roll(halo, 4 + 8 * i, 1)
        z = pltpu.roll(jnp.where(lane == CZ - 1, h, p), 1, 1) + pltpu.roll(jnp.where(lane == 0, h, p), CZ - 1, 1)
        up = jnp.where(row == 0, pyr[0, pl.ds(i, 1), :], pltpu.roll(p, 1, 0))
        dn = jnp.where(row == CY - 1, pyr[1, pl.ds(i, 1), :], pltpu.roll(p, CY - 1, 0))
        res[i] = FOURPIG * nst[0, i] - (((below + above) + (up + dn) + z) - 6.0 * p)

    lap(0, pxr[0], pot[1])

    def lap_body(j):
        lap(j + 1, pot[j], pot[j + 2])
    each(CX - 2, lap_body, 7)
    lap(CX - 1, pot[CX - 2], pxr[1])

    total = gathered(m2, my, 2)
    cells = float(CX * CY * CZ * n_gx * n_gy * n_gz)
    mean = jnp.sum(total) / cells

    def mean_body(i):
        res[i] = res[i] - FOURPIG * mean
    each(CX, mean_body, 8)

    far = [[is_box(2, b, s) for b in (0, 1)] for s in range(SLOTS)]
    wait_for(go, dr.at[3])

    def far_body(j):
        boxes = [go[0, j], go[1, j]]
        for s in range(SLOTS):
            dsol[s, j] = dsol[s, j] + (boxes[0] * far[s][0] + boxes[1] * far[s][1])
    each(HALF, far_body)

    for r in (0, 1):
        for n, ref in enumerate((xh, yrecv, zrecv)):
            wait_for(ref.at[r], hs.at[r, n])
    for ref, sem in ((pfirst, ps.at[0]), (pin, ps.at[1]), (pin, ds_.at[0]), (go, ds_.at[1]), (mz, ms.at[0]), (mx, ms.at[1]), (my, ms.at[2]),
                     (pxr, fs.at[0]), (pyr, fs.at[1]), (pzr, fs.at[2])):
        wait_for(ref, sem)


def solution(mesh):
    n_gx, n_gy, n_gz = mesh.shape["gx"], mesh.shape["gy"], mesh.shape["gz"]

    def on_device(state, solver_owner, phi_prev):
        f32 = jnp.float32
        V = lambda *s: pltpu.VMEM(s, f32)
        D = lambda *s: pltpu.SemaphoreType.DMA(s)
        hbm = pl.BlockSpec(memory_space=pltpu.HBM)
        vmem = pl.BlockSpec(memory_space=pltpu.VMEM)
        outs = pl.pallas_call(
            functools.partial(kernel, n_gx, n_gy, n_gz),
            out_shape=(
                jax.ShapeDtypeStruct(state.shape, f32),
                jax.ShapeDtypeStruct(phi_prev.shape, f32),
                jax.ShapeDtypeStruct(state.shape[1:], f32),
            ),
            in_specs=[hbm, hbm, hbm],
            out_specs=(vmem, vmem, vmem),
            scratch_shapes=[
                pltpu.SMEM((1, 1, 8), jnp.int32),
                V(NF, ROWS, CZ), V(NF, ROWS, CZ), V(SLOTS, HALF, CY, CZ),
                V(CX, CY, CZ), V(ROWS, CZ), V(CX, CY, CZ), V(NF, CX, CY, CZ),
                V(2, NF, CY, CZ), V(NF, CX, CZ), V(NF, CY, CZ),
                V(2, 2, NF, 2, CY, CZ), V(2, 2, NF, 2, CX, CZ), V(2, 2, NF, 2, CX, CZ),
                V(2, NF, CY, CZ), V(2, 2, NF // 2 + 1, 8, CZ), V(2, 2, NF // 2 + 1, 8, CZ),
                V(4, 2, HALF, CY, CZ), V(CX, CY, CZ), V(2, 2, HALF, CY, CZ), V(2, HALF, CY, CZ),
                V(2, HALF, CY, CZ), V(2, HALF, CY, CZ), V(2, HALF, CY, CZ),
                V(2, CY, CZ), V(2, CX, CZ), V(2, CX, CZ), V(1, CY, CZ), V(2, CY, CZ),
                V(1, CZ), V(1, CZ), V(1, CZ),
                V(n_gy - 1, 1, CZ), V(n_gz // 2 - 1, 1, CZ), V(2 * n_gx - 1, 1, CZ),
                D(3), D(2, 3), D(2, 3), D(2), D(2), D(2), D(5), D(3), D(3), D(3), D(3),
            ],
            compiler_params=pltpu.CompilerParams(
                collective_id=0, has_side_effects=True, vmem_limit_bytes=32 * 1024 * 1024
            ),
            name="gas_step",
        )(
            pltpu.with_memory_space_constraint(solver_owner, pltpu.HBM),
            pltpu.with_memory_space_constraint(state, pltpu.HBM),
            pltpu.with_memory_space_constraint(phi_prev, pltpu.HBM),
        )
        return pl.pallas_call(
            move_out,
            out_shape=tuple(jax.ShapeDtypeStruct(o.shape, f32) for o in outs),
            in_specs=[vmem] * 3,
            out_specs=(hbm,) * 3,
            scratch_shapes=[D(3)],
            compiler_params=pltpu.CompilerParams(has_side_effects=True, vmem_limit_bytes=4 * 1024 * 1024),
            name="move_out",
        )(*outs)

    return jax.shard_map(
        on_device,
        mesh=mesh,
        in_specs=(P(None, "gx", "gy", "gz"), P("gy", "gz", None), P("gx", None, "gy", "gz")),
        out_specs=(P(None, "gx", "gy", "gz"), P("gx", None, "gy", "gz"), P("gx", "gy", "gz")),
        check_vma=False,
    )
```

```python
import functools

import jax
import jax.numpy as jnp
from jax import lax
from jax.experimental import pallas as pl
from jax.experimental.pallas import tpu as pltpu
from jax.sharding import PartitionSpec as P

MESH = pl.DeviceIdType.MESH
GAMMA = 5.0 / 3.0
DTH = 0.04
FOURPIG = 2.0
NF = 7
CX, CY, CZ = 16, 16, 128
PITCH, BASE = 24, 8
ROWS = CX * PITCH + 32
HALF = 8
SLOTS = 4
UN = 4


def pressure(q5):
    return (GAMMA - 1.0) * jnp.maximum(q5, 0.1)


def speeds(get, dirs):
    inv = 1.0 / jnp.maximum(get(0), 0.25)
    sound = jnp.sqrt(GAMMA * pressure(get(5)) * inv)
    return [jnp.abs(get(d)) * inv + sound for d in dirs]


def interface_flux(get, speed_l, speed_r, d):
    def edge(k):
        a, b, c, e = get(k)
        v = 7.0 / 12.0 * (b + c) - 1.0 / 12.0 * (a + e)
        v = jnp.minimum(jnp.maximum(v, jnp.minimum(b, c)), jnp.maximum(b, c))
        return v, c - b

    half = 0.5 * jnp.maximum(speed_l, speed_r)
    e0, j0 = edge(0)
    ed, jd = edge(d)
    e5, j5 = edge(5)
    vel = ed / jnp.maximum(e0, 0.25)
    press = pressure(e5)
    out = [ed - half * j0]
    for k in (1, 2, 3):
        if k == d:
            out.append(ed * vel + press - half * jd)
        else:
            ek, jk = edge(k)
            out.append(ek * vel - half * jk)
    e4, j4 = edge(4)
    out.append((e4 + press) * vel - half * j4)
    out.append(e5 * vel - half * j5)
    e6, j6 = edge(6)
    out.append(e6 * vel - half * j6)
    return out


def lanes(shape=(CY, CZ)):
    return lax.broadcasted_iota(jnp.int32, shape, 1)


def rows_of(i):
    start = i * PITCH + BASE
    if not isinstance(i, int):
        start = pl.multiple_of(start, 8)
    return pl.ds(start, CY)


def z_shifted(q):
    return (pltpu.roll(q, 1, 1), q, pltpu.roll(q, CZ - 1, 1), pltpu.roll(q, CZ - 2, 1))


def each(n, body, unroll=1):
    def step(i, c):
        body(i)
        return c

    lax.fori_loop(0, n, step, 0, unroll=unroll)


def pack_z(load, acc, slabs, unroll):
    lane = lanes()

    def put(i, acc, shift):
        here = (lane >= CZ - 8 - 8 * i) & (lane < CZ - 8 * i)
        return tuple(jnp.where(here, pltpu.roll(load(k, i), shift, 1), a) for k, a in enumerate(acc))

    if isinstance(slabs, tuple):
        for i in slabs:
            acc = put(i, acc, CZ - 4 - 8 * i)
        return acc
    return lax.fori_loop(slabs.start, slabs.stop, lambda i, a: put(i, a, CZ - 4 - 8 * i), acc, unroll=unroll)


def blank(count):
    return tuple(jnp.zeros((CY, CZ), jnp.float32) for _ in range(count))


def move_out(*refs):
    n = (len(refs) - 1) // 2
    sem = refs[-1]
    for i in range(n):
        for p in range(refs[i].shape[0]):
            pltpu.make_async_copy(refs[i].at[p], refs[n + i].at[p], sem.at[i]).start()
    for i in range(n):
        pltpu.make_async_copy(refs[i], refs[n + i], sem.at[i]).wait()


def kernel(n_gx, n_gy, n_gz, owner_in, state, phi_in, nst, dsol, res,
           owner_ref, q1, q2, phi, sx, sy, sz, dd, fb, fym, tz,
           xh, ysend, yrecv, zpack, zsend, zrecv,
           pb, pot, pin, pfirst, gl, gr, go,
           pxr, pys, pyr, pzs, pzr,
           m0, m1, m2, mx, my, mz,
           lsem, hs, hr, ps, pr, ds_, dr, fs, fr, ms, mr):
    gx, gy, gz = lax.axis_index("gx"), lax.axis_index("gy"), lax.axis_index("gz")

    def at(axis, pos, n, off):
        return {axis: lax.rem(pos + (off + n), n)}

    x_lo, x_hi = at("gx", gx, n_gx, -1), at("gx", gx, n_gx, 1)
    y_lo, y_hi = at("gy", gy, n_gy, -1), at("gy", gy, n_gy, 1)
    z_lo, z_hi = at("gz", gz, n_gz, -1), at("gz", gz, n_gz, 1)

    def remote(src, dst, send, recv, dev):
        c = pltpu.make_async_remote_copy(src_ref=src, dst_ref=dst, send_sem=send, recv_sem=recv,
                                         device_id=dev, device_id_type=MESH)
        c.start()
        return c

    n_zy = n_gz // 2

    def flat(h):
        return {"gz": (gz // n_zy) * n_zy + lax.rem(gz + h, n_zy)}

    barrier = pltpu.get_barrier_semaphore()
    peers = [x_lo, x_hi, y_lo, y_hi, z_lo, z_hi, at("gy", gy, n_gy, n_gy // 2), at("gz", gz, n_gz, n_zy)]
    for dev in peers:
        pl.semaphore_signal(barrier, inc=1, device_id=dev, device_id_type=MESH)

    for i in range(CX):
        pltpu.make_async_copy(state.at[:, i], q1.at[:, rows_of(i)], lsem.at[0]).start()
    phi_load = pltpu.make_async_copy(phi_in, phi, lsem.at[1])
    phi_load.start()
    owner_load = pltpu.make_async_copy(owner_in, owner_ref, lsem.at[2])
    owner_load.start()

    def wait_for(ref, sem):
        pltpu.make_async_copy(ref, ref, sem).wait()

    def send_x_first():
        return [remote(state.at[:, pl.ds(CX - 2, 2)], xh.at[0, 0], hs.at[0, 0], hr.at[0, 0], x_hi),
                remote(state.at[:, pl.ds(0, 2)], xh.at[0, 1], hs.at[0, 0], hr.at[0, 0], x_lo)]

    def send_x_second():
        cs = []
        for j in (0, 1):
            cs.append(remote(q2.at[:, rows_of(14 + j)], xh.at[1, 0, :, j], hs.at[1, 0], hr.at[1, 0], x_hi))
            cs.append(remote(q2.at[:, rows_of(j)], xh.at[1, 1, :, j], hs.at[1, 0], hr.at[1, 0], x_lo))
        return cs

    def pack_y(q, r):
        for k in range(NF):
            for j in (0, 1):
                ysend[r, 0, k, j] = q[k, pl.ds(BASE + j, CX, stride=PITCH), :]
                ysend[r, 1, k, j] = q[k, pl.ds(BASE + 14 + j, CX, stride=PITCH), :]

    def pack_inner(q, r):
        acc = pack_z(lambda k, i: q[k, rows_of(i), :], blank(NF), range(2, CX - 2), 6)
        for k in range(NF):
            zpack[r, k] = acc[k]

    def pack_outer(q, r):
        acc = pack_z(lambda k, i: q[k, rows_of(i), :], tuple(zpack[r, k] for k in range(NF)), (0, 1, 14, 15), 1)
        for k in range(NF):
            zpack[r, k] = acc[k]
        slot = (lanes((8, CZ)) & 7) >> 1
        for g in range(NF // 2 + 1):
            parts = [acc[k][8 * h:8 * h + 8] for k in (2 * g, 2 * g + 1) if k < NF for h in (0, 1)]
            for side, lane in ((1, 2), (0, 4)):
                v = pltpu.roll(parts[0], CZ - lane, 1)
                for n in range(1, len(parts)):
                    shift = (CZ + 2 * n - lane) % CZ
                    v = jnp.where(slot == n, pltpu.roll(parts[n], shift, 1) if shift else parts[n], v)
                zsend[r, side, g] = v

    def send_y(r):
        return [remote(ysend.at[r, 1], yrecv.at[r, 0], hs.at[r, 1], hr.at[r, 1], y_hi),
                remote(ysend.at[r, 0], yrecv.at[r, 1], hs.at[r, 1], hr.at[r, 1], y_lo)]

    def send_z(r):
        return [remote(zsend.at[r, 1], zrecv.at[r, 0], hs.at[r, 2], hr.at[r, 2], z_hi),
                remote(zsend.at[r, 0], zrecv.at[r, 1], hs.at[r, 2], hr.at[r, 2], z_lo)]

    def interior(q):
        def speed_body(i):
            s = speeds(lambda k: q[k, rows_of(i), :], (1, 2, 3))
            sx[i] = s[0]
            sy[rows_of(i), :] = s[1]
            sz[i] = s[2]

        each(CX, speed_body, UN)
        lane = lanes()
        inner = (lane >= 2) & (lane < CZ - 2)

        def z_body(i):
            s = sz[i]
            f = interface_flux(lambda k: z_shifted(q[k, rows_of(i), :]), s, pltpu.roll(s, CZ - 1, 1), 3)
            for k in range(NF):
                dd[k, i] = jnp.where(inner, pltpu.roll(f[k], 1, 1) - f[k], 0.0)

        each(CX, z_body, UN)

        def x_flux(i):
            return interface_flux(lambda k: tuple(q[k, rows_of(i + o), :] for o in (-1, 0, 1, 2)), sx[i], sx[i + 1], 1)

        f = x_flux(1)
        for k in range(NF):
            fb[0, k] = f[k]

        def x_body(i, prev):
            f = x_flux(i)
            for k in range(NF):
                dd[k, i] = dd[k, i] + (prev[k] - f[k])
            return tuple(f)

        f = lax.fori_loop(2, 14, x_body, tuple(f), unroll=UN)
        for k in range(NF):
            fb[1, k] = f[k]

    def y_part(q, r, finish):
        for k in range(NF):
            for j in (0, 1):
                q[k, pl.ds(BASE - 2 + j, CX, stride=PITCH), :] = yrecv[r, 0, k, j]
                q[k, pl.ds(BASE + CY + j, CX, stride=PITCH), :] = yrecv[r, 1, k, j]
        sy[pl.ds(BASE + CY, CX, stride=PITCH), :] = speeds(lambda k: yrecv[r, 1, k, 0], (2,))[0]
        s_l, = speeds(lambda k: yrecv[r, 0, k, 1], (2,))
        s_r, = speeds(lambda k: ysend[r, 0, k, 0], (2,))
        f = interface_flux(
            lambda k: (yrecv[r, 0, k, 0], yrecv[r, 0, k, 1], ysend[r, 0, k, 0], ysend[r, 0, k, 1]), s_l, s_r, 2)
        for k in range(NF):
            fym[k] = f[k]
        first_row = lax.broadcasted_iota(jnp.int32, (CY, CZ), 0) == 0

        def y_tendency(i):
            at_ = i * PITCH + BASE
            f = interface_flux(lambda k: tuple(q[k, pl.ds(at_ + o, CY), :] for o in (-1, 0, 1, 2)),
                               sy[pl.ds(at_, CY), :], sy[pl.ds(at_ + 1, CY), :], 2)
            for k in range(NF):
                lower = jnp.where(first_row, fym[k, pl.ds(i, 1), :], pltpu.roll(f[k], 1, 0))
                f[k] = dd[k, i] + (lower - f[k])
            return f

        def outer_body(j):
            i = jnp.where(j < 2, j, j + 12)
            t = y_tendency(i)
            for k in range(NF):
                dd[k, i] = t[k]

        each(4, outer_body, UN)

        def inner_body(j):
            finish(j + 2, y_tendency(j + 2))

        each(CX - 4, inner_body, UN)

    def z_part(r):
        low = (lanes() & 7) < 4

        def z_edge(cells):
            s, = speeds(lambda k: cells[k], (3,))
            f = interface_flux(lambda k: z_shifted(cells[k]), s, pltpu.roll(s, CZ - 1, 1), 3)
            return [pltpu.roll(f[k], 1, 1) - f[k] for k in range(NF)]

        def received(side, lane, k):
            m = zrecv[r, side, k // 2]
            shifts = [(2 * CZ + lane - 2 * (2 * (k % 2) + h)) % CZ for h in (0, 1)]
            return jnp.concatenate([pltpu.roll(m, t, 1) if t else m for t in shifts], axis=0)

        def from_left(k):
            return received(0, 2, k)

        def from_right(k):
            return received(1, 4, k)

        left = z_edge([jnp.where(low, from_left(k), zpack[r, k]) for k in range(NF)])
        for k in range(NF):
            tz[k] = left[k]
        right = z_edge([jnp.where(low, zpack[r, k], from_right(k)) for k in range(NF)])
        for k in range(NF):
            tz[k] = jnp.where(low, right[k], tz[k])

    def edge_tendency(i, k):
        lane = lanes()
        outer = (lane < 2) | (lane >= CZ - 2)
        return jnp.where(outer, pltpu.roll(tz[k], 4 + 8 * i, 1), 0.0)

    def tendency(i, k):
        return dd[k, i] + edge_tendency(i, k)

    def edges_rows(scale):
        lane = lanes((CX, CZ))
        x = lax.broadcasted_iota(jnp.int32, (CX, CZ), 0)
        here = ((lane < 2) | (lane >= CZ - 2)) & (x >= 2) & (x < CX - 2)
        for k in range(NF):
            for side, j in ((0, 0), (0, 1), (1, 0), (1, 1)):
                row = jnp.broadcast_to(tz[k, 14 * side + j:14 * side + j + 1, :], (CX, CZ))
                part = pltpu.roll(row, 4, 1, stride=8, stride_axis=0)
                ysend[1, side, k, j] = ysend[1, side, k, j] + jnp.where(here, scale * part, 0.0)

    def x_part(q, r, finish):
        def get(i):
            if i < 0:
                return lambda k: xh[r, 0, k, i + 2]
            if i >= CX:
                return lambda k: xh[r, 1, k, i - CX]
            return lambda k: q[k, rows_of(i), :]

        def speed(i):
            return sx[i] if 0 <= i < CX else speeds(get(i), (1,))[0]

        def flux(i):
            g = [get(i + o) for o in (-1, 0, 1, 2)]
            return interface_flux(lambda k: tuple(h(k) for h in g), speed(i), speed(i + 1), 1)

        a = flux(-1)
        b = flux(0)
        finish(0, [tendency(0, k) + (a[k] - b[k]) for k in range(NF)])
        finish(1, [tendency(1, k) + (b[k] - fb[0, k]) for k in range(NF)])
        a = flux(14)
        finish(14, [tendency(14, k) + (fb[1, k] - a[k]) for k in range(NF)])
        b = flux(15)
        finish(15, [tendency(15, k) + (a[k] - b[k]) for k in range(NF)])

    def edges(scale, view, fields):
        def body(j):
            for k in fields:
                ref, idx = view(j + 2, k)
                ref[idx] = ref[idx] + scale * edge_tendency(j + 2, k)
        each(CX - 4, body, 6)

    def edges_packed(r, scale):
        lane = lanes()
        here = (lane >= 16) & (lane < CZ - 16) & ((lane & 7) >= 2) & ((lane & 7) < 6)
        for k in range(NF):
            zpack[r, k] = zpack[r, k] + jnp.where(here, scale * tz[k], 0.0)

    def finish_first(i, t):
        for k in range(NF):
            q2[k, rows_of(i), :] = q1[k, rows_of(i), :] + DTH * t[k]

    def finish_new(i, t):
        for k in range(NF):
            nst[k, i] = 0.5 * q1[k, rows_of(i), :] + 0.5 * (q2[k, rows_of(i), :] + DTH * t[k])

    pl.semaphore_wait(barrier, len(peers))
    send_x_first()
    wait_for(q1.at[:, pl.ds(0, CX * CY)], lsem.at[0])
    pack_inner(q1, 0)
    pack_outer(q1, 0)
    send_z(0)
    pack_y(q1, 0)
    send_y(0)

    phi_load.wait()
    owner_load.wait()

    def is_code(box, slot):
        return jnp.where(owner_ref[0, 0, box] == gx * SLOTS + slot, 1.0, 0.0).astype(jnp.float32)

    masks = [[[is_code(lax.rem(gx + o, n_gx) * 2 + b, s) for s in range(SLOTS)] for b in (0, 1)] for o in range(4)]

    for o in (2, 1, 3, 0):
        def phi_body(j, o=o):
            rows = [phi[s, j] for s in range(SLOTS)]
            for b in (0, 1):
                m = masks[o][b]
                v = rows[0] * m[0]
                for s in range(1, SLOTS):
                    v = v + rows[s] * m[s]
                pb[o, b, j] = v
        each(HALF, phi_body)
    interior(q1)
    wait_for(yrecv.at[0], hr.at[0, 1])
    y_part(q1, 0, finish_first)
    remote(pb.at[2, 0], pfirst.at[0], ps.at[0], pr.at[0], x_hi)
    remote(pb.at[2, 1], pfirst.at[1], ps.at[0], pr.at[0], x_lo)
    pack_inner(q2, 1)
    wait_for(zrecv.at[0], hr.at[0, 2])
    z_part(0)
    edges_packed(1, DTH)
    wait_for(xh.at[0], hr.at[0, 0])
    x_part(q1, 0, finish_first)

    pack_outer(q2, 1)
    send_z(1)
    send_x_second()
    pack_y(q2, 1)
    edges_rows(DTH)
    send_y(1)
    edges(DTH, lambda i, k: (q2, (k, rows_of(i), slice(None))), range(NF))

    interior(q2)
    wait_for(yrecv.at[1], hr.at[1, 1])
    y_part(q2, 1, finish_new)
    remote(pb.at[1, 1], pin.at[0, 1], ps.at[1], pr.at[1], x_hi)
    remote(pb.at[3, 0], pin.at[1, 0], ps.at[1], pr.at[1], x_lo)
    wait_for(pfirst, pr.at[0])

    def add_body(j):
        pb[1, 0, j] = pb[1, 0, j] + pfirst[0, j]
        pb[3, 1, j] = pb[3, 1, j] + pfirst[1, j]

    each(HALF, add_body, 4)
    wait_for(zrecv.at[1], hr.at[1, 2])
    z_part(1)
    edges(0.5 * DTH, lambda i, k: (nst, (k, i)), (0,))
    wait_for(xh.at[1], hr.at[1, 0])
    x_part(q2, 1, finish_new)

    def mass_body(i, acc):
        return acc + nst[0, i, 0:8, :] + nst[0, i, 8:16, :]

    acc = lax.fori_loop(0, CX, mass_body, jnp.zeros((8, CZ), jnp.float32), unroll=4)
    m0[...] = jnp.sum(acc, axis=0, keepdims=True)

    def spread(src, dst, devices, t):
        for n, dev in enumerate(devices):
            remote(src, dst.at[n], ms.at[t], mr.at[t], dev)

    def gathered(own, got, t):
        wait_for(got, mr.at[t])
        acc = own[...]
        for n in range(got.shape[0]):
            acc = acc + got[n]
        return acc

    along_z = [{**at("gx", gx, n_gx, o), **at("gz", gz, n_gz, h * n_zy)}
               for o in range(n_gx) for h in (0, 1) if o + h > 0]
    spread(m0, mz, along_z, 0)
    remote(pb.at[1, 0], pin.at[0, 0], ps.at[1], pr.at[1], x_hi)
    remote(pb.at[3, 1], pin.at[1, 1], ps.at[1], pr.at[1], x_lo)

    remote(nst.at[0, pl.ds(0, HALF)], gl.at[0], ds_.at[0], dr.at[0], x_hi)
    remote(nst.at[0, pl.ds(HALF, HALF)], gr.at[1], ds_.at[0], dr.at[1], x_lo)
    remote(nst.at[0, pl.ds(HALF, HALF)], gl.at[1], ds_.at[0], dr.at[2], x_hi)
    remote(nst.at[0, pl.ds(0, HALF)], gr.at[0], ds_.at[0], dr.at[4], x_lo)
    edges(0.5 * DTH, lambda i, k: (nst, (k, i)), range(1, NF))

    m1[...] = gathered(m0, mz, 0)
    spread(m1, mx, [at("gy", gy, n_gy, o) for o in range(1, n_gy)], 1)

    wait_for(pin, pr.at[1])

    def pot_body(j):
        for b in (0, 1):
            pot[b * HALF + j] = pb[0, b, j] + (pin[0, b, j] + pin[1, b, j])

    each(HALF, pot_body, 4)
    def row_body(i):
        pys[0, pl.ds(i, 1), :] = pot[i, 0:1, :]
        pys[1, pl.ds(i, 1), :] = pot[i, CY - 1:CY, :]

    each(CX, row_body, 8)
    pzs[0] = pack_z(lambda k, i: pot[i], blank(1), range(0, CX), 16)[0]
    remote(pot.at[CX - 1], pxr.at[0], fs.at[0], fr.at[0], x_hi)
    remote(pot.at[0], pxr.at[1], fs.at[0], fr.at[0], x_lo)
    remote(pys.at[1], pyr.at[0], fs.at[1], fr.at[1], y_hi)
    remote(pys.at[0], pyr.at[1], fs.at[1], fr.at[1], y_lo)
    remote(pzs.at[0], pzr.at[0], fs.at[2], fr.at[2], z_hi)
    remote(pzs.at[0], pzr.at[1], fs.at[2], fr.at[2], z_lo)

    wait_for(gl.at[0], dr.at[0])
    remote(gl.at[0], go.at[0], ds_.at[1], dr.at[3], x_hi)
    wait_for(gr.at[1], dr.at[1])
    remote(gr.at[1], go.at[1], ds_.at[1], dr.at[3], x_lo)

    m2[...] = gathered(m1, mx, 1)
    spread(m2, my, [flat(h) for h in range(1, n_zy)], 2)

    wait_for(gl.at[1], dr.at[2])
    wait_for(gr.at[0], dr.at[4])

    def is_box(o, b, s):
        return is_code(lax.rem(gx + o, n_gx) * 2 + b, s)

    near = [[(is_box(o, b, s)) for o in (0, 3, 1) for b in (0, 1)] for s in range(SLOTS)]

    def near_body(j):
        boxes = [nst[0, j], nst[0, HALF + j], gl[0, j], gl[1, j], gr[0, j], gr[1, j]]
        for s in range(SLOTS):
            v = boxes[0] * near[s][0]
            for t in range(1, 6):
                v = v + boxes[t] * near[s][t]
            dsol[s, j] = v
    each(HALF, near_body, 2)
    for n, ref in enumerate((pxr, pyr, pzr)):
        wait_for(ref, fr.at[n])
    lane = lanes()
    row = lax.broadcasted_iota(jnp.int32, (CY, CZ), 0)
    halo = jnp.where((lane & 7) < 4, pzr[0, :, :], pzr[1, :, :])

    def lap(i, below, above):
        p = pot[i]
        h = pltpu.roll(halo, 4 + 8 * i, 1)
        z = pltpu.roll(jnp.where(lane == CZ - 1, h, p), 1, 1) + pltpu.roll(jnp.where(lane == 0, h, p), CZ - 1, 1)
        up = jnp.where(row == 0, pyr[0, pl.ds(i, 1), :], pltpu.roll(p, 1, 0))
        dn = jnp.where(row == CY - 1, pyr[1, pl.ds(i, 1), :], pltpu.roll(p, CY - 1, 0))
        res[i] = FOURPIG * nst[0, i] - (((below + above) + (up + dn) + z) - 6.0 * p)

    lap(0, pxr[0], pot[1])

    def lap_body(j):
        lap(j + 1, pot[j], pot[j + 2])
    each(CX - 2, lap_body, 7)
    lap(CX - 1, pot[CX - 2], pxr[1])

    total = gathered(m2, my, 2)
    cells = float(CX * CY * CZ * n_gx * n_gy * n_gz)
    mean = jnp.sum(total) / cells

    def mean_body(i):
        res[i] = res[i] - FOURPIG * mean
    each(CX, mean_body, 8)

    far = [[is_box(2, b, s) for b in (0, 1)] for s in range(SLOTS)]
    wait_for(go, dr.at[3])

    def far_body(j):
        boxes = [go[0, j], go[1, j]]
        for s in range(SLOTS):
            dsol[s, j] = dsol[s, j] + (boxes[0] * far[s][0] + boxes[1] * far[s][1])
    each(HALF, far_body, 4)

    for r in (0, 1):
        for n, ref in enumerate((xh, yrecv, zrecv)):
            wait_for(ref.at[r], hs.at[r, n])
    for ref, sem in ((pfirst, ps.at[0]), (pin, ps.at[1]), (pin, ds_.at[0]), (go, ds_.at[1]), (mz, ms.at[0]), (mx, ms.at[1]), (my, ms.at[2]),
                     (pxr, fs.at[0]), (pyr, fs.at[1]), (pzr, fs.at[2])):
        wait_for(ref, sem)


def solution(mesh):
    n_gx, n_gy, n_gz = mesh.shape["gx"], mesh.shape["gy"], mesh.shape["gz"]

    def on_device(state, solver_owner, phi_prev):
        f32 = jnp.float32
        V = lambda *s: pltpu.VMEM(s, f32)
        D = lambda *s: pltpu.SemaphoreType.DMA(s)
        hbm = pl.BlockSpec(memory_space=pltpu.HBM)
        vmem = pl.BlockSpec(memory_space=pltpu.VMEM)
        outs = pl.pallas_call(
            functools.partial(kernel, n_gx, n_gy, n_gz),
            out_shape=(
                jax.ShapeDtypeStruct(state.shape, f32),
                jax.ShapeDtypeStruct(phi_prev.shape, f32),
                jax.ShapeDtypeStruct(state.shape[1:], f32),
            ),
            in_specs=[hbm, hbm, hbm],
            out_specs=(vmem, vmem, vmem),
            scratch_shapes=[
                pltpu.SMEM((1, 1, 8), jnp.int32),
                V(NF, ROWS, CZ), V(NF, ROWS, CZ), V(SLOTS, HALF, CY, CZ),
                V(CX, CY, CZ), V(ROWS, CZ), V(CX, CY, CZ), V(NF, CX, CY, CZ),
                V(2, NF, CY, CZ), V(NF, CX, CZ), V(NF, CY, CZ),
                V(2, 2, NF, 2, CY, CZ), V(2, 2, NF, 2, CX, CZ), V(2, 2, NF, 2, CX, CZ),
                V(2, NF, CY, CZ), V(2, 2, NF // 2 + 1, 8, CZ), V(2, 2, NF // 2 + 1, 8, CZ),
                V(4, 2, HALF, CY, CZ), V(CX, CY, CZ), V(2, 2, HALF, CY, CZ), V(2, HALF, CY, CZ),
                V(2, HALF, CY, CZ), V(2, HALF, CY, CZ), V(2, HALF, CY, CZ),
                V(2, CY, CZ), V(2, CX, CZ), V(2, CX, CZ), V(1, CY, CZ), V(2, CY, CZ),
                V(1, CZ), V(1, CZ), V(1, CZ),
                V(n_gy - 1, 1, CZ), V(n_gz // 2 - 1, 1, CZ), V(2 * n_gx - 1, 1, CZ),
                D(3), D(2, 3), D(2, 3), D(2), D(2), D(2), D(5), D(3), D(3), D(3), D(3),
            ],
            compiler_params=pltpu.CompilerParams(
                collective_id=0, has_side_effects=True, vmem_limit_bytes=32 * 1024 * 1024
            ),
            name="gas_step",
        )(
            pltpu.with_memory_space_constraint(solver_owner, pltpu.HBM),
            pltpu.with_memory_space_constraint(state, pltpu.HBM),
            pltpu.with_memory_space_constraint(phi_prev, pltpu.HBM),
        )
        return pl.pallas_call(
            move_out,
            out_shape=tuple(jax.ShapeDtypeStruct(o.shape, f32) for o in outs),
            in_specs=[vmem] * 3,
            out_specs=(hbm,) * 3,
            scratch_shapes=[D(3)],
            compiler_params=pltpu.CompilerParams(has_side_effects=True, vmem_limit_bytes=4 * 1024 * 1024),
            name="move_out",
        )(*outs)

    return jax.shard_map(
        on_device,
        mesh=mesh,
        in_specs=(P(None, "gx", "gy", "gz"), P("gy", "gz", None), P("gx", None, "gy", "gz")),
        out_specs=(P(None, "gx", "gy", "gz"), P("gx", None, "gy", "gz"), P("gx", "gy", "gz")),
        check_vma=False,
    )
```

```python
import functools

import jax
import jax.numpy as jnp
from jax import lax
from jax.experimental import pallas as pl
from jax.experimental.pallas import tpu as pltpu
from jax.sharding import PartitionSpec as P

MESH = pl.DeviceIdType.MESH
GAMMA = 5.0 / 3.0
DTH = 0.04
FOURPIG = 2.0
NF = 7
CX, CY, CZ = 16, 16, 128
PITCH, BASE = 24, 8
ROWS = CX * PITCH + 8
HALF = 8
SLOTS = 4
UN = 4


def pressure(q5):
    return (GAMMA - 1.0) * jnp.maximum(q5, 0.1)


def speeds(get, dirs):
    inv = 1.0 / jnp.maximum(get(0), 0.25)
    sound = jnp.sqrt(GAMMA * pressure(get(5)) * inv)
    return [jnp.abs(get(d)) * inv + sound for d in dirs]


def interface_flux(get, speed_l, speed_r, d):
    def edge(k):
        a, b, c, e = get(k)
        v = 7.0 / 12.0 * (b + c) - 1.0 / 12.0 * (a + e)
        v = jnp.minimum(jnp.maximum(v, jnp.minimum(b, c)), jnp.maximum(b, c))
        return v, c - b

    half = 0.5 * jnp.maximum(speed_l, speed_r)
    e0, j0 = edge(0)
    ed, jd = edge(d)
    e5, j5 = edge(5)
    vel = ed / jnp.maximum(e0, 0.25)
    press = pressure(e5)
    out = [ed - half * j0]
    for k in (1, 2, 3):
        if k == d:
            out.append(ed * vel + press - half * jd)
        else:
            ek, jk = edge(k)
            out.append(ek * vel - half * jk)
    e4, j4 = edge(4)
    out.append((e4 + press) * vel - half * j4)
    out.append(e5 * vel - half * j5)
    e6, j6 = edge(6)
    out.append(e6 * vel - half * j6)
    return out


def lanes(shape=(CY, CZ)):
    return lax.broadcasted_iota(jnp.int32, shape, 1)


def rows_of(i):
    start = i * PITCH + BASE
    if not isinstance(i, int):
        start = pl.multiple_of(start, 8)
    return pl.ds(start, CY)


def z_shifted(q):
    return (pltpu.roll(q, 1, 1), q, pltpu.roll(q, CZ - 1, 1), pltpu.roll(q, CZ - 2, 1))


def each(n, body, unroll=1):
    def step(i, c):
        body(i)
        return c

    lax.fori_loop(0, n, step, 0, unroll=unroll)


def pack_z(load, acc, slabs, unroll):
    lane = lanes()

    def put(i, acc, shift):
        here = (lane >= CZ - 8 - 8 * i) & (lane < CZ - 8 * i)
        return tuple(jnp.where(here, pltpu.roll(load(k, i), shift, 1), a) for k, a in enumerate(acc))

    if isinstance(slabs, tuple):
        for i in slabs:
            acc = put(i, acc, CZ - 4 - 8 * i)
        return acc
    return lax.fori_loop(slabs.start, slabs.stop, lambda i, a: put(i, a, CZ - 4 - 8 * i), acc, unroll=unroll)


def blank(count):
    return tuple(jnp.zeros((CY, CZ), jnp.float32) for _ in range(count))


def move_out(*refs):
    n = (len(refs) - 1) // 2
    sem = refs[-1]
    for i in range(n):
        for p in range(refs[i].shape[0]):
            pltpu.make_async_copy(refs[i].at[p], refs[n + i].at[p], sem.at[i]).start()
    for i in range(n):
        pltpu.make_async_copy(refs[i], refs[n + i], sem.at[i]).wait()


def kernel(n_gx, n_gy, n_gz, owner_in, state, phi_in, nst, dsol, res,
           owner_ref, q1, q2, phi, sx, sy, sz, dd, fb, fym, tz,
           xh, ysend, yrecv, zpack, zsend, zrecv,
           pb, pot, pin, pfirst, gl, gr, go,
           pxr, pys, pyr, pzs, pzr,
           m0, m1, m2, mx, my, mz,
           lsem, hs, hr, ps, pr, ds_, dr, fs, fr, ms, mr):
    gx, gy, gz = lax.axis_index("gx"), lax.axis_index("gy"), lax.axis_index("gz")

    def at(axis, pos, n, off):
        return {axis: lax.rem(pos + (off + n), n)}

    x_lo, x_hi = at("gx", gx, n_gx, -1), at("gx", gx, n_gx, 1)
    y_lo, y_hi = at("gy", gy, n_gy, -1), at("gy", gy, n_gy, 1)
    z_lo, z_hi = at("gz", gz, n_gz, -1), at("gz", gz, n_gz, 1)

    def remote(src, dst, send, recv, dev):
        c = pltpu.make_async_remote_copy(src_ref=src, dst_ref=dst, send_sem=send, recv_sem=recv,
                                         device_id=dev, device_id_type=MESH)
        c.start()
        return c

    n_zy = n_gz // 2

    def flat(h):
        return {"gz": (gz // n_zy) * n_zy + lax.rem(gz + h, n_zy)}

    barrier = pltpu.get_barrier_semaphore()
    peers = [x_lo, x_hi, y_lo, y_hi, z_lo, z_hi, at("gy", gy, n_gy, n_gy // 2), at("gz", gz, n_gz, n_zy)]
    for dev in peers:
        pl.semaphore_signal(barrier, inc=1, device_id=dev, device_id_type=MESH)

    for i in range(CX):
        pltpu.make_async_copy(state.at[:, i], q1.at[:, rows_of(i)], lsem.at[0]).start()
    phi_load = pltpu.make_async_copy(phi_in, phi, lsem.at[1])
    phi_load.start()
    owner_load = pltpu.make_async_copy(owner_in, owner_ref, lsem.at[2])
    owner_load.start()

    def wait_for(ref, sem):
        pltpu.make_async_copy(ref, ref, sem).wait()

    def send_x_first():
        return [remote(state.at[:, pl.ds(CX - 2, 2)], xh.at[0, 0], hs.at[0, 0], hr.at[0, 0], x_hi),
                remote(state.at[:, pl.ds(0, 2)], xh.at[0, 1], hs.at[0, 0], hr.at[0, 0], x_lo)]

    def send_x_second():
        cs = []
        for j in (0, 1):
            cs.append(remote(q2.at[:, rows_of(14 + j)], xh.at[1, 0, :, j], hs.at[1, 0], hr.at[1, 0], x_hi))
            cs.append(remote(q2.at[:, rows_of(j)], xh.at[1, 1, :, j], hs.at[1, 0], hr.at[1, 0], x_lo))
        return cs

    def pack_y(q, r):
        for k in range(NF):
            for j in (0, 1):
                ysend[r, 0, k, j] = q[k, pl.ds(BASE + j, CX, stride=PITCH), :]
                ysend[r, 1, k, j] = q[k, pl.ds(BASE + 14 + j, CX, stride=PITCH), :]

    def pack_inner(q, r):
        acc = pack_z(lambda k, i: q[k, rows_of(i), :], blank(NF), range(2, CX - 2), 6)
        for k in range(NF):
            zpack[r, k] = acc[k]

    def pack_outer(q, r):
        acc = pack_z(lambda k, i: q[k, rows_of(i), :], tuple(zpack[r, k] for k in range(NF)), (0, 1, 14, 15), 1)
        for k in range(NF):
            zpack[r, k] = acc[k]
        slot = (lanes((8, CZ)) & 7) >> 1
        for g in range(NF // 2 + 1):
            parts = [acc[k][8 * h:8 * h + 8] for k in (2 * g, 2 * g + 1) if k < NF for h in (0, 1)]
            for side, lane in ((1, 2), (0, 4)):
                v = pltpu.roll(parts[0], CZ - lane, 1)
                for n in range(1, len(parts)):
                    shift = (CZ + 2 * n - lane) % CZ
                    v = jnp.where(slot == n, pltpu.roll(parts[n], shift, 1) if shift else parts[n], v)
                zsend[r, side, g] = v

    def send_y(r):
        return [remote(ysend.at[r, 1], yrecv.at[r, 0], hs.at[r, 1], hr.at[r, 1], y_hi),
                remote(ysend.at[r, 0], yrecv.at[r, 1], hs.at[r, 1], hr.at[r, 1], y_lo)]

    def send_z(r):
        return [remote(zsend.at[r, 1], zrecv.at[r, 0], hs.at[r, 2], hr.at[r, 2], z_hi),
                remote(zsend.at[r, 0], zrecv.at[r, 1], hs.at[r, 2], hr.at[r, 2], z_lo)]

    def interior(q):
        def speed_body(i):
            s = speeds(lambda k: q[k, rows_of(i), :], (1, 2, 3))
            sx[i] = s[0]
            sy[rows_of(i), :] = s[1]
            sz[i] = s[2]

        each(CX, speed_body, UN)
        lane = lanes()
        inner = (lane >= 2) & (lane < CZ - 2)

        def z_body(i):
            s = sz[i]
            f = interface_flux(lambda k: z_shifted(q[k, rows_of(i), :]), s, pltpu.roll(s, CZ - 1, 1), 3)
            for k in range(NF):
                dd[k, i] = jnp.where(inner, pltpu.roll(f[k], 1, 1) - f[k], 0.0)

        each(CX, z_body, UN)

        def x_flux(i):
            return interface_flux(lambda k: tuple(q[k, rows_of(i + o), :] for o in (-1, 0, 1, 2)), sx[i], sx[i + 1], 1)

        f = x_flux(1)
        for k in range(NF):
            fb[0, k] = f[k]

        def x_body(i, prev):
            f = x_flux(i)
            for k in range(NF):
                dd[k, i] = dd[k, i] + (prev[k] - f[k])
            return tuple(f)

        f = lax.fori_loop(2, 14, x_body, tuple(f), unroll=UN)
        for k in range(NF):
            fb[1, k] = f[k]

    def y_part(q, r, finish):
        for k in range(NF):
            for j in (0, 1):
                q[k, pl.ds(BASE - 2 + j, CX, stride=PITCH), :] = yrecv[r, 0, k, j]
                q[k, pl.ds(BASE + CY + j, CX, stride=PITCH), :] = yrecv[r, 1, k, j]
        sy[pl.ds(BASE + CY, CX, stride=PITCH), :] = speeds(lambda k: yrecv[r, 1, k, 0], (2,))[0]
        s_l, = speeds(lambda k: yrecv[r, 0, k, 1], (2,))
        s_r, = speeds(lambda k: ysend[r, 0, k, 0], (2,))
        f = interface_flux(
            lambda k: (yrecv[r, 0, k, 0], yrecv[r, 0, k, 1], ysend[r, 0, k, 0], ysend[r, 0, k, 1]), s_l, s_r, 2)
        for k in range(NF):
            fym[k] = f[k]
        first_row = lax.broadcasted_iota(jnp.int32, (CY, CZ), 0) == 0

        def y_tendency(i):
            at_ = i * PITCH + BASE
            f = interface_flux(lambda k: tuple(q[k, pl.ds(at_ + o, CY), :] for o in (-1, 0, 1, 2)),
                               sy[pl.ds(at_, CY), :], sy[pl.ds(at_ + 1, CY), :], 2)
            for k in range(NF):
                lower = jnp.where(first_row, fym[k, pl.ds(i, 1), :], pltpu.roll(f[k], 1, 0))
                f[k] = dd[k, i] + (lower - f[k])
            return f

        def outer_body(j):
            i = jnp.where(j < 2, j, j + 12)
            t = y_tendency(i)
            for k in range(NF):
                dd[k, i] = t[k]

        each(4, outer_body, UN)

        def inner_body(j):
            finish(j + 2, y_tendency(j + 2))

        each(CX - 4, inner_body, UN)

    def z_part(r):
        low = (lanes() & 7) < 4

        def z_edge(cells):
            s, = speeds(lambda k: cells[k], (3,))
            f = interface_flux(lambda k: z_shifted(cells[k]), s, pltpu.roll(s, CZ - 1, 1), 3)
            return [pltpu.roll(f[k], 1, 1) - f[k] for k in range(NF)]

        def received(side, lane, k):
            m = zrecv[r, side, k // 2]
            shifts = [(2 * CZ + lane - 2 * (2 * (k % 2) + h)) % CZ for h in (0, 1)]
            return jnp.concatenate([pltpu.roll(m, t, 1) if t else m for t in shifts], axis=0)

        def from_left(k):
            return received(0, 2, k)

        def from_right(k):
            return received(1, 4, k)

        left = z_edge([jnp.where(low, from_left(k), zpack[r, k]) for k in range(NF)])
        for k in range(NF):
            tz[k] = left[k]
        right = z_edge([jnp.where(low, zpack[r, k], from_right(k)) for k in range(NF)])
        for k in range(NF):
            tz[k] = jnp.where(low, right[k], tz[k])

    def edge_tendency(i, k):
        lane = lanes()
        outer = (lane < 2) | (lane >= CZ - 2)
        return jnp.where(outer, pltpu.roll(tz[k], 4 + 8 * i, 1), 0.0)

    def tendency(i, k):
        return dd[k, i] + edge_tendency(i, k)

    def edges_rows(scale):
        lane = lanes((CX, CZ))
        x = lax.broadcasted_iota(jnp.int32, (CX, CZ), 0)
        here = ((lane < 2) | (lane >= CZ - 2)) & (x >= 2) & (x < CX - 2)
        for k in range(NF):
            for side, j in ((0, 0), (0, 1), (1, 0), (1, 1)):
                row = jnp.broadcast_to(tz[k, 14 * side + j:14 * side + j + 1, :], (CX, CZ))
                part = pltpu.roll(row, 4, 1, stride=8, stride_axis=0)
                ysend[1, side, k, j] = ysend[1, side, k, j] + jnp.where(here, scale * part, 0.0)

    def x_part(q, r, finish):
        def get(i):
            if i < 0:
                return lambda k: xh[r, 0, k, i + 2]
            if i >= CX:
                return lambda k: xh[r, 1, k, i - CX]
            return lambda k: q[k, rows_of(i), :]

        def speed(i):
            return sx[i] if 0 <= i < CX else speeds(get(i), (1,))[0]

        def flux(i):
            g = [get(i + o) for o in (-1, 0, 1, 2)]
            return interface_flux(lambda k: tuple(h(k) for h in g), speed(i), speed(i + 1), 1)

        a = flux(-1)
        b = flux(0)
        finish(0, [tendency(0, k) + (a[k] - b[k]) for k in range(NF)])
        finish(1, [tendency(1, k) + (b[k] - fb[0, k]) for k in range(NF)])
        a = flux(14)
        finish(14, [tendency(14, k) + (fb[1, k] - a[k]) for k in range(NF)])
        b = flux(15)
        finish(15, [tendency(15, k) + (a[k] - b[k]) for k in range(NF)])

    def edges(scale, view, fields):
        def body(j):
            for k in fields:
                ref, idx = view(j + 2, k)
                ref[idx] = ref[idx] + scale * edge_tendency(j + 2, k)
        each(CX - 4, body, 6)

    def edges_packed(r, scale):
        lane = lanes()
        here = (lane >= 16) & (lane < CZ - 16) & ((lane & 7) >= 2) & ((lane & 7) < 6)
        for k in range(NF):
            zpack[r, k] = zpack[r, k] + jnp.where(here, scale * tz[k], 0.0)

    def finish_first(i, t):
        for k in range(NF):
            q2[k, rows_of(i), :] = q1[k, rows_of(i), :] + DTH * t[k]

    def finish_new(i, t):
        for k in range(NF):
            nst[k, i] = 0.5 * q1[k, rows_of(i), :] + 0.5 * (q2[k, rows_of(i), :] + DTH * t[k])

    pl.semaphore_wait(barrier, len(peers))
    send_x_first()
    wait_for(q1.at[:, pl.ds(0, CX * CY)], lsem.at[0])
    pack_y(q1, 0)
    send_y(0)
    pack_inner(q1, 0)
    pack_outer(q1, 0)
    send_z(0)

    phi_load.wait()
    owner_load.wait()

    def is_code(box, slot):
        return jnp.where(owner_ref[0, 0, box] == gx * SLOTS + slot, 1.0, 0.0).astype(jnp.float32)

    masks = [[[is_code(lax.rem(gx + o, n_gx) * 2 + b, s) for s in range(SLOTS)] for b in (0, 1)] for o in range(4)]

    for o in (2, 1, 3, 0):
        def phi_body(j, o=o):
            rows = [phi[s, j] for s in range(SLOTS)]
            for b in (0, 1):
                m = masks[o][b]
                v = rows[0] * m[0]
                for s in range(1, SLOTS):
                    v = v + rows[s] * m[s]
                pb[o, b, j] = v
        each(HALF, phi_body)
    interior(q1)
    wait_for(yrecv.at[0], hr.at[0, 1])
    y_part(q1, 0, finish_first)
    remote(pb.at[2, 0], pfirst.at[0], ps.at[0], pr.at[0], x_hi)
    remote(pb.at[2, 1], pfirst.at[1], ps.at[0], pr.at[0], x_lo)
    pack_inner(q2, 1)
    wait_for(zrecv.at[0], hr.at[0, 2])
    z_part(0)
    edges_packed(1, DTH)
    wait_for(xh.at[0], hr.at[0, 0])
    x_part(q1, 0, finish_first)

    pack_outer(q2, 1)
    send_z(1)
    send_x_second()
    pack_y(q2, 1)
    edges_rows(DTH)
    send_y(1)
    edges(DTH, lambda i, k: (q2, (k, rows_of(i), slice(None))), range(NF))

    interior(q2)
    wait_for(yrecv.at[1], hr.at[1, 1])
    y_part(q2, 1, finish_new)
    remote(pb.at[1, 1], pin.at[0, 1], ps.at[1], pr.at[1], x_hi)
    remote(pb.at[3, 0], pin.at[1, 0], ps.at[1], pr.at[1], x_lo)
    wait_for(pfirst, pr.at[0])

    def add_body(j):
        pb[1, 0, j] = pb[1, 0, j] + pfirst[0, j]
        pb[3, 1, j] = pb[3, 1, j] + pfirst[1, j]

    each(HALF, add_body)
    wait_for(zrecv.at[1], hr.at[1, 2])
    z_part(1)
    edges(0.5 * DTH, lambda i, k: (nst, (k, i)), (0,))
    wait_for(xh.at[1], hr.at[1, 0])
    x_part(q2, 1, finish_new)

    def mass_body(i, acc):
        return acc + nst[0, i, 0:8, :] + nst[0, i, 8:16, :]

    acc = lax.fori_loop(0, CX, mass_body, jnp.zeros((8, CZ), jnp.float32), unroll=4)
    m0[...] = jnp.sum(acc, axis=0, keepdims=True)

    def spread(src, dst, devices, t):
        for n, dev in enumerate(devices):
            remote(src, dst.at[n], ms.at[t], mr.at[t], dev)

    def gathered(own, got, t):
        wait_for(got, mr.at[t])
        acc = own[...]
        for n in range(got.shape[0]):
            acc = acc + got[n]
        return acc

    along_z = [{**at("gx", gx, n_gx, o), **at("gz", gz, n_gz, h * n_zy)}
               for o in range(n_gx) for h in (0, 1) if o + h > 0]
    spread(m0, mz, along_z, 0)
    remote(pb.at[1, 0], pin.at[0, 0], ps.at[1], pr.at[1], x_hi)
    remote(pb.at[3, 1], pin.at[1, 1], ps.at[1], pr.at[1], x_lo)

    remote(nst.at[0, pl.ds(0, HALF)], gl.at[0], ds_.at[0], dr.at[0], x_hi)
    remote(nst.at[0, pl.ds(HALF, HALF)], gr.at[1], ds_.at[0], dr.at[1], x_lo)
    remote(nst.at[0, pl.ds(HALF, HALF)], gl.at[1], ds_.at[0], dr.at[2], x_hi)
    remote(nst.at[0, pl.ds(0, HALF)], gr.at[0], ds_.at[0], dr.at[4], x_lo)
    edges(0.5 * DTH, lambda i, k: (nst, (k, i)), range(1, NF))

    m1[...] = gathered(m0, mz, 0)
    spread(m1, mx, [at("gy", gy, n_gy, o) for o in range(1, n_gy)], 1)

    wait_for(pin, pr.at[1])

    def pot_body(j):
        for b in (0, 1):
            pot[b * HALF + j] = pb[0, b, j] + (pin[0, b, j] + pin[1, b, j])

    each(HALF, pot_body)
    def row_body(i):
        pys[0, pl.ds(i, 1), :] = pot[i, 0:1, :]
        pys[1, pl.ds(i, 1), :] = pot[i, CY - 1:CY, :]

    each(CX, row_body)
    pzs[0] = pack_z(lambda k, i: pot[i], blank(1), range(0, CX), 16)[0]
    remote(pot.at[CX - 1], pxr.at[0], fs.at[0], fr.at[0], x_hi)
    remote(pot.at[0], pxr.at[1], fs.at[0], fr.at[0], x_lo)
    remote(pys.at[1], pyr.at[0], fs.at[1], fr.at[1], y_hi)
    remote(pys.at[0], pyr.at[1], fs.at[1], fr.at[1], y_lo)
    remote(pzs.at[0], pzr.at[0], fs.at[2], fr.at[2], z_hi)
    remote(pzs.at[0], pzr.at[1], fs.at[2], fr.at[2], z_lo)

    wait_for(gl.at[0], dr.at[0])
    remote(gl.at[0], go.at[0], ds_.at[1], dr.at[3], x_hi)
    wait_for(gr.at[1], dr.at[1])
    remote(gr.at[1], go.at[1], ds_.at[1], dr.at[3], x_lo)

    m2[...] = gathered(m1, mx, 1)
    spread(m2, my, [flat(h) for h in range(1, n_zy)], 2)

    wait_for(gl.at[1], dr.at[2])
    wait_for(gr.at[0], dr.at[4])

    def is_box(o, b, s):
        return is_code(lax.rem(gx + o, n_gx) * 2 + b, s)

    near = [[(is_box(o, b, s)) for o in (0, 3, 1) for b in (0, 1)] for s in range(SLOTS)]

    def near_body(j):
        boxes = [nst[0, j], nst[0, HALF + j], gl[0, j], gl[1, j], gr[0, j], gr[1, j]]
        for s in range(SLOTS):
            v = boxes[0] * near[s][0]
            for t in range(1, 6):
                v = v + boxes[t] * near[s][t]
            dsol[s, j] = v
    each(HALF, near_body)
    for n, ref in enumerate((pxr, pyr, pzr)):
        wait_for(ref, fr.at[n])
    lane = lanes()
    row = lax.broadcasted_iota(jnp.int32, (CY, CZ), 0)
    halo = jnp.where((lane & 7) < 4, pzr[0, :, :], pzr[1, :, :])

    def lap(i, below, above):
        p = pot[i]
        h = pltpu.roll(halo, 4 + 8 * i, 1)
        z = pltpu.roll(jnp.where(lane == CZ - 1, h, p), 1, 1) + pltpu.roll(jnp.where(lane == 0, h, p), CZ - 1, 1)
        up = jnp.where(row == 0, pyr[0, pl.ds(i, 1), :], pltpu.roll(p, 1, 0))
        dn = jnp.where(row == CY - 1, pyr[1, pl.ds(i, 1), :], pltpu.roll(p, CY - 1, 0))
        res[i] = FOURPIG * nst[0, i] - (((below + above) + (up + dn) + z) - 6.0 * p)

    lap(0, pxr[0], pot[1])

    def lap_body(j):
        lap(j + 1, pot[j], pot[j + 2])
    each(CX - 2, lap_body, 7)
    lap(CX - 1, pot[CX - 2], pxr[1])

    total = gathered(m2, my, 2)
    cells = float(CX * CY * CZ * n_gx * n_gy * n_gz)
    mean = jnp.sum(total) / cells

    def mean_body(i):
        res[i] = res[i] - FOURPIG * mean
    each(CX, mean_body, 8)

    far = [[is_box(2, b, s) for b in (0, 1)] for s in range(SLOTS)]
    wait_for(go, dr.at[3])

    def far_body(j):
        boxes = [go[0, j], go[1, j]]
        for s in range(SLOTS):
            dsol[s, j] = dsol[s, j] + (boxes[0] * far[s][0] + boxes[1] * far[s][1])
    each(HALF, far_body)

    for r in (0, 1):
        for n, ref in enumerate((xh, yrecv, zrecv)):
            wait_for(ref.at[r], hs.at[r, n])
    for ref, sem in ((pfirst, ps.at[0]), (pin, ps.at[1]), (pin, ds_.at[0]), (go, ds_.at[1]), (mz, ms.at[0]), (mx, ms.at[1]), (my, ms.at[2]),
                     (pxr, fs.at[0]), (pyr, fs.at[1]), (pzr, fs.at[2])):
        wait_for(ref, sem)


def solution(mesh):
    n_gx, n_gy, n_gz = mesh.shape["gx"], mesh.shape["gy"], mesh.shape["gz"]

    def on_device(state, solver_owner, phi_prev):
        f32 = jnp.float32
        V = lambda *s: pltpu.VMEM(s, f32)
        D = lambda *s: pltpu.SemaphoreType.DMA(s)
        hbm = pl.BlockSpec(memory_space=pltpu.HBM)
        vmem = pl.BlockSpec(memory_space=pltpu.VMEM)
        outs = pl.pallas_call(
            functools.partial(kernel, n_gx, n_gy, n_gz),
            out_shape=(
                jax.ShapeDtypeStruct(state.shape, f32),
                jax.ShapeDtypeStruct(phi_prev.shape, f32),
                jax.ShapeDtypeStruct(state.shape[1:], f32),
            ),
            in_specs=[hbm, hbm, hbm],
            out_specs=(vmem, vmem, vmem),
            scratch_shapes=[
                pltpu.SMEM((1, 1, 8), jnp.int32),
                V(NF, ROWS, CZ), V(NF, ROWS, CZ), V(SLOTS, HALF, CY, CZ),
                V(CX, CY, CZ), V(ROWS, CZ), V(CX, CY, CZ), V(NF, CX, CY, CZ),
                V(2, NF, CY, CZ), V(NF, CX, CZ), V(NF, CY, CZ),
                V(2, 2, NF, 2, CY, CZ), V(2, 2, NF, 2, CX, CZ), V(2, 2, NF, 2, CX, CZ),
                V(2, NF, CY, CZ), V(2, 2, NF // 2 + 1, 8, CZ), V(2, 2, NF // 2 + 1, 8, CZ),
                V(4, 2, HALF, CY, CZ), V(CX, CY, CZ), V(2, 2, HALF, CY, CZ), V(2, HALF, CY, CZ),
                V(2, HALF, CY, CZ), V(2, HALF, CY, CZ), V(2, HALF, CY, CZ),
                V(2, CY, CZ), V(2, CX, CZ), V(2, CX, CZ), V(1, CY, CZ), V(2, CY, CZ),
                V(1, CZ), V(1, CZ), V(1, CZ),
                V(n_gy - 1, 1, CZ), V(n_gz // 2 - 1, 1, CZ), V(2 * n_gx - 1, 1, CZ),
                D(3), D(2, 3), D(2, 3), D(2), D(2), D(2), D(5), D(3), D(3), D(3), D(3),
            ],
            compiler_params=pltpu.CompilerParams(
                collective_id=0, has_side_effects=True, vmem_limit_bytes=32 * 1024 * 1024
            ),
            name="gas_step",
        )(
            pltpu.with_memory_space_constraint(solver_owner, pltpu.HBM),
            pltpu.with_memory_space_constraint(state, pltpu.HBM),
            pltpu.with_memory_space_constraint(phi_prev, pltpu.HBM),
        )
        return pl.pallas_call(
            move_out,
            out_shape=tuple(jax.ShapeDtypeStruct(o.shape, f32) for o in outs),
            in_specs=[vmem] * 3,
            out_specs=(hbm,) * 3,
            scratch_shapes=[D(3)],
            compiler_params=pltpu.CompilerParams(has_side_effects=True, vmem_limit_bytes=4 * 1024 * 1024),
            name="move_out",
        )(*outs)

    return jax.shard_map(
        on_device,
        mesh=mesh,
        in_specs=(P(None, "gx", "gy", "gz"), P("gy", "gz", None), P("gx", None, "gy", "gz")),
        out_specs=(P(None, "gx", "gy", "gz"), P("gx", None, "gy", "gz"), P("gx", "gy", "gz")),
        check_vma=False,
    )
```

```python
import functools

import jax
import jax.numpy as jnp
from jax import lax
from jax.experimental import pallas as pl
from jax.experimental.pallas import tpu as pltpu
from jax.sharding import PartitionSpec as P

MESH = pl.DeviceIdType.MESH
GAMMA = 5.0 / 3.0
DTH = 0.04
FOURPIG = 2.0
NF = 7
CX, CY, CZ = 16, 16, 128
PITCH, BASE = 24, 8
ROWS = CX * PITCH + 32
HALF = 8
SLOTS = 4
UN = 4


def pressure(q5):
    return (GAMMA - 1.0) * jnp.maximum(q5, 0.1)


def speeds(get, dirs):
    inv = 1.0 / jnp.maximum(get(0), 0.25)
    sound = jnp.sqrt(GAMMA * pressure(get(5)) * inv)
    return [jnp.abs(get(d)) * inv + sound for d in dirs]


def interface_flux(get, speed_l, speed_r, d):
    def edge(k):
        a, b, c, e = get(k)
        v = 7.0 / 12.0 * (b + c) - 1.0 / 12.0 * (a + e)
        v = jnp.minimum(jnp.maximum(v, jnp.minimum(b, c)), jnp.maximum(b, c))
        return v, c - b

    half = 0.5 * jnp.maximum(speed_l, speed_r)
    e0, j0 = edge(0)
    ed, jd = edge(d)
    e5, j5 = edge(5)
    vel = ed / jnp.maximum(e0, 0.25)
    press = pressure(e5)
    out = [ed - half * j0]
    for k in (1, 2, 3):
        if k == d:
            out.append(ed * vel + press - half * jd)
        else:
            ek, jk = edge(k)
            out.append(ek * vel - half * jk)
    e4, j4 = edge(4)
    out.append((e4 + press) * vel - half * j4)
    out.append(e5 * vel - half * j5)
    e6, j6 = edge(6)
    out.append(e6 * vel - half * j6)
    return out


def lanes(shape=(CY, CZ)):
    return lax.broadcasted_iota(jnp.int32, shape, 1)


def rows_of(i):
    start = i * PITCH + BASE
    if not isinstance(i, int):
        start = pl.multiple_of(start, 8)
    return pl.ds(start, CY)


def z_shifted(q):
    return (pltpu.roll(q, 1, 1), q, pltpu.roll(q, CZ - 1, 1), pltpu.roll(q, CZ - 2, 1))


def each(n, body, unroll=1):
    def step(i, c):
        body(i)
        return c

    lax.fori_loop(0, n, step, 0, unroll=unroll)


def pack_z(load, acc, slabs, unroll):
    lane = lanes()

    def put(i, acc, shift):
        here = (lane >= CZ - 8 - 8 * i) & (lane < CZ - 8 * i)
        return tuple(jnp.where(here, pltpu.roll(load(k, i), shift, 1), a) for k, a in enumerate(acc))

    if isinstance(slabs, tuple):
        for i in slabs:
            acc = put(i, acc, CZ - 4 - 8 * i)
        return acc
    return lax.fori_loop(slabs.start, slabs.stop, lambda i, a: put(i, a, CZ - 4 - 8 * i), acc, unroll=unroll)


def blank(count):
    return tuple(jnp.zeros((CY, CZ), jnp.float32) for _ in range(count))


def move_out(*refs):
    n = (len(refs) - 1) // 2
    sem = refs[-1]
    for i in range(n):
        for p in range(refs[i].shape[0]):
            pltpu.make_async_copy(refs[i].at[p], refs[n + i].at[p], sem.at[i]).start()
    for i in range(n):
        pltpu.make_async_copy(refs[i], refs[n + i], sem.at[i]).wait()


def kernel(n_gx, n_gy, n_gz, owner_in, state, phi_in, nst, dsol, res,
           owner_ref, q1, q2, phi, sx, sy, sz, dd, fb, fym, tz,
           xh, ysend, yrecv, zpack, zsend, zrecv,
           pb, pot, pin, pfirst, gl, gr, go,
           pxr, pys, pyr, pzs, pzr,
           m0, m1, m2, mx, my, mz,
           lsem, hs, hr, ps, pr, ds_, dr, fs, fr, ms, mr):
    gx, gy, gz = lax.axis_index("gx"), lax.axis_index("gy"), lax.axis_index("gz")

    def at(axis, pos, n, off):
        return {axis: lax.rem(pos + (off + n), n)}

    x_lo, x_hi = at("gx", gx, n_gx, -1), at("gx", gx, n_gx, 1)
    y_lo, y_hi = at("gy", gy, n_gy, -1), at("gy", gy, n_gy, 1)
    z_lo, z_hi = at("gz", gz, n_gz, -1), at("gz", gz, n_gz, 1)

    def remote(src, dst, send, recv, dev):
        c = pltpu.make_async_remote_copy(src_ref=src, dst_ref=dst, send_sem=send, recv_sem=recv,
                                         device_id=dev, device_id_type=MESH)
        c.start()
        return c

    n_zy = n_gz // 2

    def flat(h):
        return {"gz": (gz // n_zy) * n_zy + lax.rem(gz + h, n_zy)}

    barrier = pltpu.get_barrier_semaphore()
    peers = [x_lo, x_hi, y_lo, y_hi, z_lo, z_hi, at("gy", gy, n_gy, n_gy // 2), at("gz", gz, n_gz, n_zy)]
    for dev in peers:
        pl.semaphore_signal(barrier, inc=1, device_id=dev, device_id_type=MESH)

    for i in range(CX):
        pltpu.make_async_copy(state.at[:, i], q1.at[:, rows_of(i)], lsem.at[0]).start()
    phi_load = pltpu.make_async_copy(phi_in, phi, lsem.at[1])
    phi_load.start()
    owner_load = pltpu.make_async_copy(owner_in, owner_ref, lsem.at[2])
    owner_load.start()

    def wait_for(ref, sem):
        pltpu.make_async_copy(ref, ref, sem).wait()

    def send_x_first():
        return [remote(state.at[:, pl.ds(CX - 2, 2)], xh.at[0, 0], hs.at[0, 0], hr.at[0, 0], x_hi),
                remote(state.at[:, pl.ds(0, 2)], xh.at[0, 1], hs.at[0, 0], hr.at[0, 0], x_lo)]

    def send_x_second():
        cs = []
        for j in (0, 1):
            cs.append(remote(q2.at[:, rows_of(14 + j)], xh.at[1, 0, :, j], hs.at[1, 0], hr.at[1, 0], x_hi))
            cs.append(remote(q2.at[:, rows_of(j)], xh.at[1, 1, :, j], hs.at[1, 0], hr.at[1, 0], x_lo))
        return cs

    def pack_y(q, r):
        for k in range(NF):
            for j in (0, 1):
                ysend[r, 0, k, j] = q[k, pl.ds(BASE + j, CX, stride=PITCH), :]
                ysend[r, 1, k, j] = q[k, pl.ds(BASE + 14 + j, CX, stride=PITCH), :]

    def pack_inner(q, r):
        acc = pack_z(lambda k, i: q[k, rows_of(i), :], blank(NF), range(2, CX - 2), 6)
        for k in range(NF):
            zpack[r, k] = acc[k]

    def pack_outer(q, r):
        acc = pack_z(lambda k, i: q[k, rows_of(i), :], tuple(zpack[r, k] for k in range(NF)), (0, 1, 14, 15), 1)
        for k in range(NF):
            zpack[r, k] = acc[k]
        slot = (lanes((8, CZ)) & 7) >> 1
        for g in range(NF // 2 + 1):
            parts = [acc[k][8 * h:8 * h + 8] for k in (2 * g, 2 * g + 1) if k < NF for h in (0, 1)]
            for side, lane in ((1, 2), (0, 4)):
                v = pltpu.roll(parts[0], CZ - lane, 1)
                for n in range(1, len(parts)):
                    shift = (CZ + 2 * n - lane) % CZ
                    v = jnp.where(slot == n, pltpu.roll(parts[n], shift, 1) if shift else parts[n], v)
                zsend[r, side, g] = v

    def send_y(r):
        return [remote(ysend.at[r, 1], yrecv.at[r, 0], hs.at[r, 1], hr.at[r, 1], y_hi),
                remote(ysend.at[r, 0], yrecv.at[r, 1], hs.at[r, 1], hr.at[r, 1], y_lo)]

    def send_z(r):
        return [remote(zsend.at[r, 1], zrecv.at[r, 0], hs.at[r, 2], hr.at[r, 2], z_hi),
                remote(zsend.at[r, 0], zrecv.at[r, 1], hs.at[r, 2], hr.at[r, 2], z_lo)]

    def interior(q):
        def speed_body(i):
            s = speeds(lambda k: q[k, rows_of(i), :], (1, 2, 3))
            sx[i] = s[0]
            sy[rows_of(i), :] = s[1]
            sz[i] = s[2]

        each(CX, speed_body, UN)
        lane = lanes()
        inner = (lane >= 2) & (lane < CZ - 2)

        def z_body(i):
            s = sz[i]
            f = interface_flux(lambda k: z_shifted(q[k, rows_of(i), :]), s, pltpu.roll(s, CZ - 1, 1), 3)
            for k in range(NF):
                dd[k, i] = jnp.where(inner, pltpu.roll(f[k], 1, 1) - f[k], 0.0)

        each(CX, z_body, UN)

        def x_flux(i):
            return interface_flux(lambda k: tuple(q[k, rows_of(i + o), :] for o in (-1, 0, 1, 2)), sx[i], sx[i + 1], 1)

        f = x_flux(1)
        for k in range(NF):
            fb[0, k] = f[k]

        def x_body(i, prev):
            f = x_flux(i)
            for k in range(NF):
                dd[k, i] = dd[k, i] + (prev[k] - f[k])
            return tuple(f)

        f = lax.fori_loop(2, 14, x_body, tuple(f), unroll=UN)
        for k in range(NF):
            fb[1, k] = f[k]

    def y_part(q, r, finish):
        for k in range(NF):
            for j in (0, 1):
                q[k, pl.ds(BASE - 2 + j, CX, stride=PITCH), :] = yrecv[r, 0, k, j]
                q[k, pl.ds(BASE + CY + j, CX, stride=PITCH), :] = yrecv[r, 1, k, j]
        sy[pl.ds(BASE + CY, CX, stride=PITCH), :] = speeds(lambda k: yrecv[r, 1, k, 0], (2,))[0]
        s_l, = speeds(lambda k: yrecv[r, 0, k, 1], (2,))
        s_r, = speeds(lambda k: ysend[r, 0, k, 0], (2,))
        f = interface_flux(
            lambda k: (yrecv[r, 0, k, 0], yrecv[r, 0, k, 1], ysend[r, 0, k, 0], ysend[r, 0, k, 1]), s_l, s_r, 2)
        for k in range(NF):
            fym[k] = f[k]
        first_row = lax.broadcasted_iota(jnp.int32, (CY, CZ), 0) == 0

        def y_tendency(i):
            at_ = i * PITCH + BASE
            f = interface_flux(lambda k: tuple(q[k, pl.ds(at_ + o, CY), :] for o in (-1, 0, 1, 2)),
                               sy[pl.ds(at_, CY), :], sy[pl.ds(at_ + 1, CY), :], 2)
            for k in range(NF):
                lower = jnp.where(first_row, fym[k, pl.ds(i, 1), :], pltpu.roll(f[k], 1, 0))
                f[k] = dd[k, i] + (lower - f[k])
            return f

        def outer_body(j):
            i = jnp.where(j < 2, j, j + 12)
            t = y_tendency(i)
            for k in range(NF):
                dd[k, i] = t[k]

        each(4, outer_body, UN)

        def inner_body(j):
            finish(j + 2, y_tendency(j + 2))

        each(CX - 4, inner_body, UN)

    def z_part(r):
        low = (lanes() & 7) < 4

        def z_edge(cells):
            s, = speeds(lambda k: cells[k], (3,))
            f = interface_flux(lambda k: z_shifted(cells[k]), s, pltpu.roll(s, CZ - 1, 1), 3)
            return [pltpu.roll(f[k], 1, 1) - f[k] for k in range(NF)]

        def received(side, lane, k):
            m = zrecv[r, side, k // 2]
            shifts = [(2 * CZ + lane - 2 * (2 * (k % 2) + h)) % CZ for h in (0, 1)]
            return jnp.concatenate([pltpu.roll(m, t, 1) if t else m for t in shifts], axis=0)

        def from_left(k):
            return received(0, 2, k)

        def from_right(k):
            return received(1, 4, k)

        left = z_edge([jnp.where(low, from_left(k), zpack[r, k]) for k in range(NF)])
        for k in range(NF):
            tz[k] = left[k]
        right = z_edge([jnp.where(low, zpack[r, k], from_right(k)) for k in range(NF)])
        for k in range(NF):
            tz[k] = jnp.where(low, right[k], tz[k])

    def edge_tendency(i, k):
        lane = lanes()
        outer = (lane < 2) | (lane >= CZ - 2)
        return jnp.where(outer, pltpu.roll(tz[k], 4 + 8 * i, 1), 0.0)

    def tendency(i, k):
        return dd[k, i] + edge_tendency(i, k)

    def edges_rows(scale):
        lane = lanes((CX, CZ))
        x = lax.broadcasted_iota(jnp.int32, (CX, CZ), 0)
        here = ((lane < 2) | (lane >= CZ - 2)) & (x >= 2) & (x < CX - 2)
        for k in range(NF):
            for side, j in ((0, 0), (0, 1), (1, 0), (1, 1)):
                row = jnp.broadcast_to(tz[k, 14 * side + j:14 * side + j + 1, :], (CX, CZ))
                part = pltpu.roll(row, 4, 1, stride=8, stride_axis=0)
                ysend[1, side, k, j] = ysend[1, side, k, j] + jnp.where(here, scale * part, 0.0)

    def x_part(q, r, finish):
        def get(i):
            if i < 0:
                return lambda k: xh[r, 0, k, i + 2]
            if i >= CX:
                return lambda k: xh[r, 1, k, i - CX]
            return lambda k: q[k, rows_of(i), :]

        def speed(i):
            return sx[i] if 0 <= i < CX else speeds(get(i), (1,))[0]

        def flux(i):
            g = [get(i + o) for o in (-1, 0, 1, 2)]
            return interface_flux(lambda k: tuple(h(k) for h in g), speed(i), speed(i + 1), 1)

        a = flux(-1)
        b = flux(0)
        finish(0, [tendency(0, k) + (a[k] - b[k]) for k in range(NF)])
        finish(1, [tendency(1, k) + (b[k] - fb[0, k]) for k in range(NF)])
        a = flux(14)
        finish(14, [tendency(14, k) + (fb[1, k] - a[k]) for k in range(NF)])
        b = flux(15)
        finish(15, [tendency(15, k) + (a[k] - b[k]) for k in range(NF)])

    def edges(scale, view, fields):
        def body(j):
            for k in fields:
                ref, idx = view(j + 2, k)
                ref[idx] = ref[idx] + scale * edge_tendency(j + 2, k)
        each(CX - 4, body, 6)

    def edges_packed(r, scale):
        lane = lanes()
        here = (lane >= 16) & (lane < CZ - 16) & ((lane & 7) >= 2) & ((lane & 7) < 6)
        for k in range(NF):
            zpack[r, k] = zpack[r, k] + jnp.where(here, scale * tz[k], 0.0)

    def finish_first(i, t):
        for k in range(NF):
            q2[k, rows_of(i), :] = q1[k, rows_of(i), :] + DTH * t[k]

    def finish_new(i, t):
        for k in range(NF):
            nst[k, i] = 0.5 * q1[k, rows_of(i), :] + 0.5 * (q2[k, rows_of(i), :] + DTH * t[k])

    pl.semaphore_wait(barrier, len(peers))
    send_x_first()
    wait_for(q1.at[:, pl.ds(0, CX * CY)], lsem.at[0])
    pack_inner(q1, 0)
    pack_outer(q1, 0)
    send_z(0)
    pack_y(q1, 0)
    send_y(0)

    phi_load.wait()
    owner_load.wait()

    def is_code(box, slot):
        return jnp.where(owner_ref[0, 0, box] == gx * SLOTS + slot, 1.0, 0.0).astype(jnp.float32)

    masks = [[[is_code(lax.rem(gx + o, n_gx) * 2 + b, s) for s in range(SLOTS)] for b in (0, 1)] for o in range(4)]

    for o in (2, 1, 3, 0):
        def phi_body(j, o=o):
            rows = [phi[s, j] for s in range(SLOTS)]
            for b in (0, 1):
                m = masks[o][b]
                v = rows[0] * m[0]
                for s in range(1, SLOTS):
                    v = v + rows[s] * m[s]
                pb[o, b, j] = v
        each(HALF, phi_body)
    interior(q1)
    wait_for(yrecv.at[0], hr.at[0, 1])
    y_part(q1, 0, finish_first)
    remote(pb.at[2, 0], pfirst.at[0], ps.at[0], pr.at[0], x_hi)
    remote(pb.at[2, 1], pfirst.at[1], ps.at[0], pr.at[0], x_lo)
    pack_inner(q2, 1)
    wait_for(zrecv.at[0], hr.at[0, 2])
    z_part(0)
    edges_packed(1, DTH)
    wait_for(xh.at[0], hr.at[0, 0])
    x_part(q1, 0, finish_first)

    pack_outer(q2, 1)
    send_z(1)
    send_x_second()
    pack_y(q2, 1)
    edges_rows(DTH)
    send_y(1)
    edges(DTH, lambda i, k: (q2, (k, rows_of(i), slice(None))), range(NF))

    interior(q2)
    wait_for(yrecv.at[1], hr.at[1, 1])
    y_part(q2, 1, finish_new)
    remote(pb.at[1, 1], pin.at[0, 1], ps.at[1], pr.at[1], x_hi)
    remote(pb.at[3, 0], pin.at[1, 0], ps.at[1], pr.at[1], x_lo)
    wait_for(pfirst, pr.at[0])

    def add_body(j):
        pb[1, 0, j] = pb[1, 0, j] + pfirst[0, j]
        pb[3, 1, j] = pb[3, 1, j] + pfirst[1, j]

    each(HALF, add_body, 4)
    remote(pb.at[1, 0, pl.ds(0, 4)], pin.at[0, 0, pl.ds(0, 4)], ps.at[1], pr.at[1], x_hi)
    remote(pb.at[3, 1, pl.ds(0, 4)], pin.at[1, 1, pl.ds(0, 4)], ps.at[1], pr.at[1], x_lo)
    wait_for(zrecv.at[1], hr.at[1, 2])
    z_part(1)
    edges(0.5 * DTH, lambda i, k: (nst, (k, i)), (0,))
    wait_for(xh.at[1], hr.at[1, 0])
    x_part(q2, 1, finish_new)

    def mass_body(i, acc):
        return acc + nst[0, i, 0:8, :] + nst[0, i, 8:16, :]

    acc = lax.fori_loop(0, CX, mass_body, jnp.zeros((8, CZ), jnp.float32), unroll=4)
    m0[...] = jnp.sum(acc, axis=0, keepdims=True)

    def spread(src, dst, devices, t):
        for n, dev in enumerate(devices):
            remote(src, dst.at[n], ms.at[t], mr.at[t], dev)

    def gathered(own, got, t):
        wait_for(got, mr.at[t])
        acc = own[...]
        for n in range(got.shape[0]):
            acc = acc + got[n]
        return acc

    along_z = [{**at("gx", gx, n_gx, o), **at("gz", gz, n_gz, h * n_zy)}
               for o in range(n_gx) for h in (0, 1) if o + h > 0]
    spread(m0, mz, along_z, 0)
    remote(pb.at[1, 0, pl.ds(4, 4)], pin.at[0, 0, pl.ds(4, 4)], ps.at[1], pr.at[1], x_hi)
    remote(pb.at[3, 1, pl.ds(4, 4)], pin.at[1, 1, pl.ds(4, 4)], ps.at[1], pr.at[1], x_lo)

    remote(nst.at[0, pl.ds(0, HALF)], gl.at[0], ds_.at[0], dr.at[0], x_hi)
    remote(nst.at[0, pl.ds(HALF, HALF)], gr.at[1], ds_.at[0], dr.at[1], x_lo)
    remote(nst.at[0, pl.ds(HALF, HALF)], gl.at[1], ds_.at[0], dr.at[2], x_hi)
    remote(nst.at[0, pl.ds(0, HALF)], gr.at[0], ds_.at[0], dr.at[4], x_lo)
    edges(0.5 * DTH, lambda i, k: (nst, (k, i)), range(1, NF))

    m1[...] = gathered(m0, mz, 0)
    spread(m1, mx, [at("gy", gy, n_gy, o) for o in range(1, n_gy)], 1)

    wait_for(pin, pr.at[1])

    def pot_body(j):
        for b in (0, 1):
            pot[b * HALF + j] = pb[0, b, j] + (pin[0, b, j] + pin[1, b, j])

    each(HALF, pot_body, 4)
    def row_body(i):
        pys[0, pl.ds(i, 1), :] = pot[i, 0:1, :]
        pys[1, pl.ds(i, 1), :] = pot[i, CY - 1:CY, :]

    each(CX, row_body, 8)
    pzs[0] = pack_z(lambda k, i: pot[i], blank(1), range(0, CX), 16)[0]
    remote(pot.at[CX - 1], pxr.at[0], fs.at[0], fr.at[0], x_hi)
    remote(pot.at[0], pxr.at[1], fs.at[0], fr.at[0], x_lo)
    remote(pys.at[1], pyr.at[0], fs.at[1], fr.at[1], y_hi)
    remote(pys.at[0], pyr.at[1], fs.at[1], fr.at[1], y_lo)
    remote(pzs.at[0], pzr.at[0], fs.at[2], fr.at[2], z_hi)
    remote(pzs.at[0], pzr.at[1], fs.at[2], fr.at[2], z_lo)

    wait_for(gl.at[0], dr.at[0])
    remote(gl.at[0], go.at[0], ds_.at[1], dr.at[3], x_hi)
    wait_for(gr.at[1], dr.at[1])
    remote(gr.at[1], go.at[1], ds_.at[1], dr.at[3], x_lo)

    m2[...] = gathered(m1, mx, 1)
    spread(m2, my, [flat(h) for h in range(1, n_zy)], 2)

    wait_for(gl.at[1], dr.at[2])
    wait_for(gr.at[0], dr.at[4])

    def is_box(o, b, s):
        return is_code(lax.rem(gx + o, n_gx) * 2 + b, s)

    near = [[(is_box(o, b, s)) for o in (0, 3, 1) for b in (0, 1)] for s in range(SLOTS)]

    def near_body(j):
        boxes = [nst[0, j], nst[0, HALF + j], gl[0, j], gl[1, j], gr[0, j], gr[1, j]]
        for s in range(SLOTS):
            v = boxes[0] * near[s][0]
            for t in range(1, 6):
                v = v + boxes[t] * near[s][t]
            dsol[s, j] = v
    each(HALF, near_body, 2)
    for n, ref in enumerate((pxr, pyr, pzr)):
        wait_for(ref, fr.at[n])
    lane = lanes()
    row = lax.broadcasted_iota(jnp.int32, (CY, CZ), 0)
    halo = jnp.where((lane & 7) < 4, pzr[0, :, :], pzr[1, :, :])

    def lap(i, below, above):
        p = pot[i]
        h = pltpu.roll(halo, 4 + 8 * i, 1)
        z = pltpu.roll(jnp.where(lane == CZ - 1, h, p), 1, 1) + pltpu.roll(jnp.where(lane == 0, h, p), CZ - 1, 1)
        up = jnp.where(row == 0, pyr[0, pl.ds(i, 1), :], pltpu.roll(p, 1, 0))
        dn = jnp.where(row == CY - 1, pyr[1, pl.ds(i, 1), :], pltpu.roll(p, CY - 1, 0))
        res[i] = FOURPIG * nst[0, i] - (((below + above) + (up + dn) + z) - 6.0 * p)

    lap(0, pxr[0], pot[1])

    def lap_body(j):
        lap(j + 1, pot[j], pot[j + 2])
    each(CX - 2, lap_body, 7)
    lap(CX - 1, pot[CX - 2], pxr[1])

    total = gathered(m2, my, 2)
    cells = float(CX * CY * CZ * n_gx * n_gy * n_gz)
    mean = jnp.sum(total) / cells

    def mean_body(i):
        res[i] = res[i] - FOURPIG * mean
    each(CX, mean_body, 8)

    far = [[is_box(2, b, s) for b in (0, 1)] for s in range(SLOTS)]
    wait_for(go, dr.at[3])

    def far_body(j):
        boxes = [go[0, j], go[1, j]]
        for s in range(SLOTS):
            dsol[s, j] = dsol[s, j] + (boxes[0] * far[s][0] + boxes[1] * far[s][1])
    each(HALF, far_body, 4)

    for r in (0, 1):
        for n, ref in enumerate((xh, yrecv, zrecv)):
            wait_for(ref.at[r], hs.at[r, n])
    for ref, sem in ((pfirst, ps.at[0]), (pin, ps.at[1]), (pin, ds_.at[0]), (go, ds_.at[1]), (mz, ms.at[0]), (mx, ms.at[1]), (my, ms.at[2]),
                     (pxr, fs.at[0]), (pyr, fs.at[1]), (pzr, fs.at[2])):
        wait_for(ref, sem)


def solution(mesh):
    n_gx, n_gy, n_gz = mesh.shape["gx"], mesh.shape["gy"], mesh.shape["gz"]

    def on_device(state, solver_owner, phi_prev):
        f32 = jnp.float32
        V = lambda *s: pltpu.VMEM(s, f32)
        D = lambda *s: pltpu.SemaphoreType.DMA(s)
        hbm = pl.BlockSpec(memory_space=pltpu.HBM)
        vmem = pl.BlockSpec(memory_space=pltpu.VMEM)
        outs = pl.pallas_call(
            functools.partial(kernel, n_gx, n_gy, n_gz),
            out_shape=(
                jax.ShapeDtypeStruct(state.shape, f32),
                jax.ShapeDtypeStruct(phi_prev.shape, f32),
                jax.ShapeDtypeStruct(state.shape[1:], f32),
            ),
            in_specs=[hbm, hbm, hbm],
            out_specs=(vmem, vmem, vmem),
            scratch_shapes=[
                pltpu.SMEM((1, 1, 8), jnp.int32),
                V(NF, ROWS, CZ), V(NF, ROWS, CZ), V(SLOTS, HALF, CY, CZ),
                V(CX, CY, CZ), V(ROWS, CZ), V(CX, CY, CZ), V(NF, CX, CY, CZ),
                V(2, NF, CY, CZ), V(NF, CX, CZ), V(NF, CY, CZ),
                V(2, 2, NF, 2, CY, CZ), V(2, 2, NF, 2, CX, CZ), V(2, 2, NF, 2, CX, CZ),
                V(2, NF, CY, CZ), V(2, 2, NF // 2 + 1, 8, CZ), V(2, 2, NF // 2 + 1, 8, CZ),
                V(4, 2, HALF, CY, CZ), V(CX, CY, CZ), V(2, 2, HALF, CY, CZ), V(2, HALF, CY, CZ),
                V(2, HALF, CY, CZ), V(2, HALF, CY, CZ), V(2, HALF, CY, CZ),
                V(2, CY, CZ), V(2, CX, CZ), V(2, CX, CZ), V(1, CY, CZ), V(2, CY, CZ),
                V(1, CZ), V(1, CZ), V(1, CZ),
                V(n_gy - 1, 1, CZ), V(n_gz // 2 - 1, 1, CZ), V(2 * n_gx - 1, 1, CZ),
                D(3), D(2, 3), D(2, 3), D(2), D(2), D(2), D(5), D(3), D(3), D(3), D(3),
            ],
            compiler_params=pltpu.CompilerParams(
                collective_id=0, has_side_effects=True, vmem_limit_bytes=32 * 1024 * 1024
            ),
            name="gas_step",
        )(
            pltpu.with_memory_space_constraint(solver_owner, pltpu.HBM),
            pltpu.with_memory_space_constraint(state, pltpu.HBM),
            pltpu.with_memory_space_constraint(phi_prev, pltpu.HBM),
        )
        return pl.pallas_call(
            move_out,
            out_shape=tuple(jax.ShapeDtypeStruct(o.shape, f32) for o in outs),
            in_specs=[vmem] * 3,
            out_specs=(hbm,) * 3,
            scratch_shapes=[D(3)],
            compiler_params=pltpu.CompilerParams(has_side_effects=True, vmem_limit_bytes=4 * 1024 * 1024),
            name="move_out",
        )(*outs)

    return jax.shard_map(
        on_device,
        mesh=mesh,
        in_specs=(P(None, "gx", "gy", "gz"), P("gy", "gz", None), P("gx", None, "gy", "gz")),
        out_specs=(P(None, "gx", "gy", "gz"), P("gx", None, "gy", "gz"), P("gx", "gy", "gz")),
        check_vma=False,
    )
```
